128 devices in a mesh: mp: 2 (over core), dp: 64 (over z, y, x).
Axes of the slice: x: 4, y: 4, z: 4, core: 2. Of those that a mesh axis runs over, the one named last changes fastest.
Arguments:
- a: bfloat16 [131072, 768], P('dp')
- g: bfloat16 [131072, 2304], P('dp')
- w: float32 [2304, 6, 128], P(None, 'mp')
- a_old: float32 [768, 6, 128], P(None, 'mp')
- s_old: float32 [2304, 18, 128], P(None, 'mp')
Outputs:
- output 1: float32 [2304, 6, 128], P(None, 'mp')
- output 2: float32 [768, 6, 128], P(None, 'mp')
- output 3: float32 [2304, 18, 128], P(None, 'mp')
All inputs are finite; a program needn't handle non-finite values.
Results may differ from the reference program's by a relative error of at most 0.001.
Values sent between devices are 32-bit elements.
A program may use at most 1 GiB of HBM per device.

```python
import math
import jax
import jax.numpy as jnp
from jax import lax

D_IN = 768
D_OUT = 2304
BLOCK_W = 128
N_LOC = 2048
N_DP = 64
N_MP = 2
TEACH_RANK = 32

FACTOR_DECAY = 0.95
DAMPING = 0.001
DAMP_SHIFT = math.sqrt(DAMPING)
LEARN_RATE = 1.0


def to_natural(stored):
    n_rows, n_blocks, blk_width = stored.shape
    return stored.reshape(n_rows, N_MP, n_blocks // N_MP, blk_width).transpose(0, 2, 1, 3).reshape(n_rows, n_blocks * blk_width)


def to_cyclic(matrix):
    n_rows, n_cols = matrix.shape
    n_blocks = n_cols // BLOCK_W
    return matrix.reshape(n_rows, n_blocks // N_MP, N_MP, BLOCK_W).transpose(0, 2, 1, 3).reshape(n_rows, n_blocks, BLOCK_W)


def spd_factor(key_a, key_b, dim_size):
    diag_vals = 0.2 + jax.random.uniform(key_a, (dim_size,))
    low_rank = jax.random.normal(key_b, (TEACH_RANK, dim_size)) * math.sqrt(2.0 / dim_size)
    return jnp.diag(diag_vals) + jnp.dot(low_rank.T, low_rank)


def setup_inputs(seed: int = 0) -> dict:
    key_list = jax.random.split(jax.random.key(seed), 12)
    n_all = N_DP * N_LOC
    col_scale = 0.3 + 1.2 * jax.random.uniform(key_list[0], (D_IN,))
    shared_dir = jax.random.normal(key_list[1], (TEACH_RANK, D_IN)) * math.sqrt(4.0 / D_IN)
    latent = jax.random.normal(key_list[2], (n_all, TEACH_RANK))
    act_f32 = jax.random.normal(key_list[3], (n_all, D_IN)) * col_scale + jnp.dot(latent, shared_dir)
    teach_in = jax.random.normal(key_list[4], (N_DP, D_IN, TEACH_RANK)) * (1.0 / math.sqrt(D_IN))
    teach_out = jax.random.normal(key_list[5], (N_DP, D_OUT, TEACH_RANK)) * (0.5 * math.sqrt(N_DP / TEACH_RANK))
    hidden = jnp.einsum('snd,sdr->snr', act_f32.reshape(N_DP, N_LOC, D_IN), teach_in)
    out_grad = jnp.einsum('snr,sor->sno', hidden, teach_out).reshape(n_all, D_OUT) + 0.5 * jax.random.normal(key_list[6], (n_all, D_OUT))
    weight = jax.random.normal(key_list[7], (D_OUT, D_IN)) * (0.25 / math.sqrt(D_IN))
    a_old = spd_factor(key_list[8], key_list[9], D_IN)
    s_old = spd_factor(key_list[10], key_list[11], D_OUT)
    return {'a': act_f32.astype(jnp.bfloat16), 'g': out_grad.astype(jnp.bfloat16), 'w': to_cyclic(weight), 'a_old': to_cyclic(a_old), 's_old': to_cyclic(s_old)}


def damped_solve(rhs_mat, factor):
    damped = factor + DAMP_SHIFT * jnp.eye(factor.shape[0], dtype=factor.dtype)
    lower_fac = jnp.linalg.cholesky(damped)
    first_pass = lax.linalg.triangular_solve(lower_fac, rhs_mat, left_side=False, lower=True, transpose_a=True)
    return lax.linalg.triangular_solve(lower_fac, first_pass, left_side=False, lower=True)


def reference(a, g, w, a_old, s_old):
    n_all = a.shape[0]
    a_stat = jnp.dot(a.T, a, preferred_element_type=jnp.float32) / n_all
    s_stat = jnp.dot(g.T, g, preferred_element_type=jnp.float32) / n_all
    grad_t = jnp.dot(a.T, g, preferred_element_type=jnp.float32) / n_all
    a_new = FACTOR_DECAY * to_natural(a_old) + (1.0 - FACTOR_DECAY) * a_stat
    s_new = FACTOR_DECAY * to_natural(s_old) + (1.0 - FACTOR_DECAY) * s_stat
    half_solved = damped_solve(grad_t, s_new)
    step_delta = damped_solve(half_solved.T, a_new)
    w_new = to_natural(w) - LEARN_RATE * step_delta
    return (to_cyclic(w_new), to_cyclic(a_new), to_cyclic(s_new))
```

```python
import functools
import math
import jax
import jax.numpy as jnp
from jax import lax
from jax.experimental import pallas as pl
from jax.experimental.pallas import tpu as pltpu
from jax.sharding import PartitionSpec as P

FACTOR_DECAY = 0.95
DAMPING = 0.001
DAMP_SHIFT = math.sqrt(DAMPING)
LEARN_RATE = 1.0
BW = 128
PW = 256
F32 = jnp.float32
BF = jnp.bfloat16
NT = (((1,), (1,)), ((), ()))
NN = (((1,), (0,)), ((), ()))


def bc(x, shape=(8, BW)):
    return jnp.broadcast_to(x, shape)

def factor_block(mat, linv, mb=16):
    lane = lax.broadcasted_iota(jnp.int32, (8, BW), 1)
    sub = lax.broadcasted_iota(jnp.int32, (8, BW), 0)
    for t in range(BW // mb):
        k = t * mb
        nr = mb // 8
        rows = [mat[k + 8 * r:k + 8 * r + 8, :] for r in range(nr)]
        cols = [[bc(rows[r][:, k + i:k + i + 1]) for r in range(nr)] for i in range(mb)]
        inside = (lane >= k) & (lane < k + mb)
        ext = [jnp.where(inside, jnp.where(lane == sub + (k + 8 * r), 1.0, 0.0), rows[r]) for r in range(nr)]
        rv = [jnp.zeros((8, BW), F32) for _ in range(nr)]
        below = list(range((k + mb) // 8, BW // 8))
        old = {r: mat[8 * r:8 * r + 8, :] for r in below}
        for j in range(mb):
            jr, js = divmod(j, 8)
            piv = bc(cols[j][jr][js:js + 1, :])
            rinv = 1.0 / piv
            prow = bc(ext[jr][js:js + 1, :])
            linv[k + j:k + j + 1, :] = (prow * lax.rsqrt(piv))[0:1, :]
            here = sub == js
            mask = [jnp.where(here, 0.0, cols[j][r]) if r == jr else cols[j][r] for r in range(nr)]
            fac = [mask[r] * rinv for r in range(nr)]
            for i in range(j + 1, mb):
                b = bc(cols[i][jr][js:js + 1, :])
                if i == j + 1:
                    cols[i] = [cols[i][r] - (mask[r] * b) * rinv for r in range(nr)]
                else:
                    cols[i] = [cols[i][r] - fac[r] * b for r in range(nr)]
            ext = [ext[r] - fac[r] * prow for r in range(nr)]
            rv[jr] = jnp.where(here, rinv, rv[jr])
        w = [ext[r] * rv[r] for r in range(nr)]
        for r in below:
            acc = jnp.where(inside, 0.0, old[r])
            for j in range(mb):
                jr, js = divmod(j, 8)
                acc = acc - bc(old[r][:, k + j:k + j + 1]) * bc(w[jr][js:js + 1, :])
            mat[8 * r:8 * r + 8, :] = acc
    ri = lax.broadcasted_iota(jnp.int32, (BW, BW), 0)
    ci = lax.broadcasted_iota(jnp.int32, (BW, BW), 1)
    linv[...] = jnp.where(ci <= ri, linv[...], 0.0)


def split3(x):
    h = x.astype(BF)
    r = x - h.astype(F32)
    m = r.astype(BF)
    return h, m, (r - m.astype(F32)).astype(BF)

def dot6(a, b, dims):
    d = lambda x, y: lax.dot_general(x, y, dims, preferred_element_type=F32)
    ah, am, al = a
    bh, bm, bl = b
    return (d(am, bm) + d(ah, bl) + d(al, bh)) + (d(ah, bm) + d(am, bh)) + d(ah, bh)

def dotf(a, b, dims):
    return dot6(split3(a), split3(b), dims)

def solve_kernel(n, damp, s_ref, b_ref, x_ref, tmat, mat, linv, inv_all, pan, pant):
    npan = n // PW
    eye = jnp.where(lax.broadcasted_iota(jnp.int32, (PW, PW), 0) == lax.broadcasted_iota(jnp.int32, (PW, PW), 1), damp, 0.0)
    def load(j, _):
        def rows(i, _):
            tmat[j, pl.ds(i * PW, PW), :] = s_ref[j, pl.ds(i * PW, PW), :]
            return 0
        lax.fori_loop(j, npan, rows, 0)
        tmat[j, pl.ds(j * PW, PW), :] = s_ref[j, pl.ds(j * PW, PW), :] + eye
        x_ref[j] = b_ref[j]
        return 0
    lax.fori_loop(0, npan, load, 0)

    def panel(q, _):
        r0 = q * PW
        mat[...] = tmat[q, pl.ds(r0, BW), 0:BW]
        factor_block(mat, linv)
        inv0 = linv[...]
        inv0s = split3(inv0)
        l10 = dot6(split3(tmat[q, pl.ds(r0 + BW, BW), 0:BW]), inv0s, NT)
        l10s = split3(l10)
        mat[...] = tmat[q, pl.ds(r0 + BW, BW), BW:PW] - dot6(l10s, l10s, NT)
        inv_all[q, 0:BW, 0:BW] = inv0
        inv_all[q, 0:BW, BW:PW] = jnp.zeros((BW, BW), F32)
        inv_all[q, BW:PW, 0:BW] = dot6(l10s, inv0s, NN)
        factor_block(mat, linv)
        inv1 = linv[...]
        inv_all[q, BW:PW, BW:PW] = inv1
        inv_all[q, BW:PW, 0:BW] = -dotf(inv1, inv_all[q, BW:PW, 0:BW], NN)
        invs = split3(inv_all[q])
        y = dot6(split3(x_ref[q]), invs, NT)
        x_ref[q] = y
        ys = split3(y)
        def below(i, _):
            r = pl.ds(i * PW, PW)
            lo = dot6(split3(tmat[q, r, :]), invs, NT)
            tmat[q, r, :] = lo
            sp = split3(lo)
            lt = lo.T
            st = split3(lt)
            for z in range(3):
                pan[z, r, :] = sp[z]
                pant[z, i] = st[z]
            return 0
        lax.fori_loop(q + 1, npan, below, 0)
        def trail(j, _):
            w = [pant[z, j] for z in range(3)]
            x_ref[j] = x_ref[j] - dot6(ys, w, NN)
            def rows(i, _):
                r = pl.ds(i * PW, PW)
                tmat[j, r, :] = tmat[j, r, :] - dot6([pan[z, r, :] for z in range(3)], w, NN)
                return 0
            lax.fori_loop(j, npan, rows, 0)
            return 0
        lax.fori_loop(q + 1, npan, trail, 0)
        return 0
    lax.fori_loop(0, npan, panel, 0)

    def back(p, _):
        q = npan - 1 - p
        def sub(i, acc):
            return acc - dotf(x_ref[i], tmat[q, pl.ds(i * PW, PW), :], NN)
        acc = lax.fori_loop(q + 1, npan, sub, x_ref[q])
        x_ref[q] = dotf(acc, inv_all[q], NN)
        return 0
    lax.fori_loop(0, npan, back, 0)

def spd_solve2(s2, b2, damp):
    npan, n, _ = s2.shape
    vm = pl.BlockSpec(memory_space=pltpu.VMEM)
    return pl.pallas_call(functools.partial(solve_kernel, n, damp), out_shape=jax.ShapeDtypeStruct(b2.shape, F32),
        in_specs=[vm, vm], out_specs=vm,
        scratch_shapes=[pltpu.VMEM((npan, n, PW), F32), pltpu.VMEM((BW, BW), F32), pltpu.VMEM((BW, BW), F32), pltpu.VMEM((npan, PW, PW), F32),
            pltpu.VMEM((3, n, PW), BF), pltpu.VMEM((3, npan, PW, PW), BF)],
        compiler_params=pltpu.CompilerParams(vmem_limit_bytes=63 * 2**20), name="spd_solve")(s2, b2)


def own_columns(matrix, my_rank, n_mp):
    n_rows, n_cols = matrix.shape
    split_cols = matrix.reshape(n_rows, n_cols // (n_mp * BW), n_mp, BW)
    return lax.dynamic_index_in_dim(split_cols, my_rank, axis=2, keepdims=False).reshape(n_rows, n_cols // n_mp)


def panels(local_mat):
    n_rows, n_cols = local_mat.shape
    both = lax.all_gather(local_mat, 'mp').reshape(2, n_rows, n_cols // BW, BW)
    return both.transpose(2, 1, 0, 3).reshape(n_cols // BW, n_rows, PW)


def solution(mesh):
    n_mp = mesh.shape['mp']
    n_dp = mesh.shape['dp']

    def local_step(a_loc, g_loc, w_loc, a_old_loc, s_old_loc):
        my_rank = lax.axis_index('mp')
        d_idx = lax.axis_index('dp')
        d_in = a_loc.shape[1]
        d_out = g_loc.shape[1]
        n_all = a_loc.shape[0] * n_dp
        a_mine = own_columns(a_loc, my_rank, n_mp)
        g_mine = own_columns(g_loc, my_rank, n_mp)
        a_part = jnp.einsum('nd,nc->dc', a_loc, a_mine, preferred_element_type=F32)
        s_part = jnp.einsum('no,nc->oc', g_loc, g_mine, preferred_element_type=F32)
        gt_part = jnp.einsum('nd,nc->dc', a_loc, g_mine, preferred_element_type=F32)
        a_sum, s_sum, gt_sum = lax.psum((a_part, s_part, gt_part), 'dp')
        a_new = FACTOR_DECAY * a_old_loc.reshape(d_in, -1) + (1.0 - FACTOR_DECAY) * (a_sum / n_all)
        s_new = FACTOR_DECAY * s_old_loc.reshape(d_out, -1) + (1.0 - FACTOR_DECAY) * (s_sum / n_all)
        n_own = d_in // (n_mp * n_dp)
        m_pad = -(-n_own // 8) * 8
        own = d_idx * n_own + jnp.arange(m_pad)
        spot = (own // BW) * PW + my_rank * BW + own % BW
        pick = jnp.where((jnp.arange(m_pad) < n_own)[:, None] & (spot[:, None] == jnp.arange(d_in)[None, :]), 1.0, 0.0)
        pick = pick.reshape(m_pad, d_in // PW, PW).transpose(1, 0, 2)
        inv_rows = spd_solve2(panels(a_new), pick, DAMP_SHIFT)
        inv_rows = inv_rows.transpose(1, 0, 2).reshape(m_pad, d_in)
        gt_both = lax.all_gather(gt_sum / n_all, 'mp')
        zt = jnp.einsum('md,pdc->pmc', inv_rows, gt_both, precision=lax.Precision.HIGHEST, preferred_element_type=F32)
        zt = zt.reshape(n_mp, m_pad, d_out // PW, BW).transpose(2, 1, 0, 3).reshape(d_out // PW, m_pad, PW)
        xt = spd_solve2(panels(s_new), zt, DAMP_SHIFT)[:, :n_own, :]
        delta = lax.all_gather(xt, 'dp').transpose(1, 3, 0, 2).reshape(w_loc.shape)
        w_new = w_loc - LEARN_RATE * delta
        return (w_new, a_new.reshape(a_old_loc.shape), s_new.reshape(s_old_loc.shape))

    spec_rows = P('dp', None)
    spec_cyc = P(None, 'mp', None)
    return jax.shard_map(local_step, mesh=mesh, in_specs=(spec_rows, spec_rows, spec_cyc, spec_cyc, spec_cyc), out_specs=(spec_cyc, spec_cyc, spec_cyc), check_vma=False)
```

```python
import functools
import math
import numpy as np
import jax
import jax.numpy as jnp
from jax import lax
from jax.experimental import pallas as pl
from jax.experimental.pallas import tpu as pltpu
from jax.sharding import PartitionSpec as P

FACTOR_DECAY = 0.95
DAMPING = 0.001
DAMP_SHIFT = math.sqrt(DAMPING)
LEARN_RATE = 1.0
BW = 128
PW = 256
RING = 4
F32 = jnp.float32
BF = jnp.bfloat16
NT = (((1,), (1,)), ((), ()))
NN = (((1,), (0,)), ((), ()))


def bc(x, shape=(8, BW)):
    return jnp.broadcast_to(x, shape)

def factor_block(mat, linv, mb=16):
    lane = lax.broadcasted_iota(jnp.int32, (8, BW), 1)
    sub = lax.broadcasted_iota(jnp.int32, (8, BW), 0)
    for t in range(BW // mb):
        k = t * mb
        nr = mb // 8
        rows = [mat[k + 8 * r:k + 8 * r + 8, :] for r in range(nr)]
        cols = [[bc(rows[r][:, k + i:k + i + 1]) for r in range(nr)] for i in range(mb)]
        inside = (lane >= k) & (lane < k + mb)
        ext = [jnp.where(inside, jnp.where(lane == sub + (k + 8 * r), 1.0, 0.0), rows[r]) for r in range(nr)]
        rv = [jnp.zeros((8, BW), F32) for _ in range(nr)]
        below = list(range((k + mb) // 8, BW // 8))
        old = {r: mat[8 * r:8 * r + 8, :] for r in below}
        for j in range(mb):
            jr, js = divmod(j, 8)
            piv = bc(cols[j][jr][js:js + 1, :])
            rinv = 1.0 / piv
            prow = bc(ext[jr][js:js + 1, :])
            linv[k + j:k + j + 1, :] = (prow * lax.rsqrt(piv))[0:1, :]
            here = sub == js
            mask = [jnp.where(here, 0.0, cols[j][r]) if r == jr else cols[j][r] for r in range(nr)]
            fac = [mask[r] * rinv for r in range(nr)]
            for i in range(j + 1, mb):
                b = bc(cols[i][jr][js:js + 1, :])
                if i == j + 1:
                    cols[i] = [cols[i][r] - (mask[r] * b) * rinv for r in range(nr)]
                else:
                    cols[i] = [cols[i][r] - fac[r] * b for r in range(nr)]
            ext = [ext[r] - fac[r] * prow for r in range(nr)]
            rv[jr] = jnp.where(here, rinv, rv[jr])
        w = [ext[r] * rv[r] for r in range(nr)]
        for r in below:
            acc = jnp.where(inside, 0.0, old[r])
            for j in range(mb):
                jr, js = divmod(j, 8)
                acc = acc - bc(old[r][:, k + j:k + j + 1]) * bc(w[jr][js:js + 1, :])
            mat[8 * r:8 * r + 8, :] = acc
    ri = lax.broadcasted_iota(jnp.int32, (BW, BW), 0)
    ci = lax.broadcasted_iota(jnp.int32, (BW, BW), 1)
    linv[...] = jnp.where(ci <= ri, linv[...], 0.0)


def split3(x):
    h = x.astype(BF)
    r = x - h.astype(F32)
    m = r.astype(BF)
    return h, m, (r - m.astype(F32)).astype(BF)

def dot6(a, b, dims):
    d = lambda x, y: lax.dot_general(x, y, dims, preferred_element_type=F32)
    ah, am, al = a
    bh, bm, bl = b
    return (d(am, bm) + d(ah, bl) + d(al, bh)) + (d(ah, bm) + d(am, bh)) + d(ah, bh)

def dotf(a, b, dims):
    return dot6(split3(a), split3(b), dims)


def coords():
    d = lax.axis_index('dp')
    x = lax.rem(d, RING)
    y = lax.rem(lax.div(d, RING), RING)
    z = lax.div(d, RING * RING)
    return d, (x, y, z)

def neighbour(d, pos, axis, step):
    stride = (1, RING, RING * RING)[axis]
    return d + (lax.rem(pos[axis] + step, RING) - pos[axis]) * stride

def axis_of(part, phase):
    return (part + phase) % 3

def entry_barrier(d, pos, partner):
    sem = pltpu.get_barrier_semaphore()
    count = 0
    for axis in range(3):
        for step in (1, 3):
            pl.semaphore_signal(sem, inc=1, device_id={'dp': neighbour(d, pos, axis, step)}, device_id_type=pl.DeviceIdType.MESH)
            count += 1
    if partner is not None:
        pl.semaphore_signal(sem, inc=1, device_id={'mp': partner}, device_id_type=pl.DeviceIdType.MESH)
        count += 1
    pl.semaphore_wait(sem, count)

def remote(src, dst, ssem, rsem, dev):
    return pltpu.make_async_remote_copy(src_ref=src, dst_ref=dst, send_sem=ssem, recv_sem=rsem, device_id={'dp': dev}, device_id_type=pl.DeviceIdType.MESH)

def each(lo, hi, fn):
    def body(i, c):
        fn(i)
        return c
    lax.fori_loop(lo, hi, body, 0)

def decode(b, np_in, np_out):
    n_in, n_out = 2 * np_in, 2 * np_out
    starts, at = [], 0
    for q0, base_row, base_col, n in [(0, n_in, np_in, n_out)] + [(q, 0, 0, n_in) for q in range(np_in)] + [(q, n_in, np_in, n_out) for q in range(1, np_out)]:
        starts.append((at, base_row + 2 * q0 - at, base_col + q0))
        at += n - 2 * q0
    row, col, was = b, 0, (0, 0)
    for z, (first, d_row, d_col) in enumerate(starts):
        hit = 1 if z == 0 else (b >= first).astype(jnp.int32)
        row = row + hit * (d_row - was[0])
        col = col + hit * (d_col - was[1])
        was = (d_row, d_col)
    is_g = (b >= at).astype(jnp.int32)
    g_row, g_col = lax.rem(b - at * is_g, n_in), np_in + lax.div(b - at * is_g, n_in)
    row = row + is_g * (g_row - row)
    col = col + is_g * (g_col - col)
    in_s = (col >= np_in).astype(jnp.int32)
    old = in_s * ((col - np_in) * n_out + row - n_in) + (1 - in_s) * (np_out * n_out + col * n_in + row)
    return row, col, (1 - is_g) * old, is_g

def stats_kernel(nm, ns, c_in, c_out, a_hbm, g_hbm, s_hbm, ao_hbm, share, ag, agt, old, acc, ra1, rb1, rc1, rd1, ra2, rb2, rc2, rd2, ra3, rb3, rc3, rd3, lsem, ssem, rsem):
    p = lax.axis_index('mp')
    d, pos = coords()
    n_in, n_out = c_in // BW, c_out // BW
    n_all = ns * RING**3
    nso = s_hbm.shape[0]
    loads = [pltpu.make_async_copy(a_hbm, ag.at[:, 0:c_in], lsem.at[0]), pltpu.make_async_copy(g_hbm, ag.at[:, c_in:c_in + c_out], lsem.at[1]),
        pltpu.make_async_copy(s_hbm, old.at[0:nso], lsem.at[2]), pltpu.make_async_copy(ao_hbm, old.at[nso:nso + ao_hbm.shape[0]], lsem.at[3])]
    for c in loads:
        c.start()
    entry_barrier(d, pos, None)
    ck = min(512, ns)
    for z, (base, cnt) in enumerate(((0, n_in), (n_in, n_out))):
        loads[z].wait()
        def flip(c):
            for r in range(ns // ck):
                agt[base + c, :, r * ck:(r + 1) * ck] = ag[r * ck:(r + 1) * ck, pl.ds(pl.multiple_of((base + c) * BW, BW), BW)].T
        each(0, cnt, flip)
    loads[2].wait()
    loads[3].wait()

    def quarter(rel):
        def body(m):
            for part in range(3):
                c1 = lax.rem(pos[axis_of(part, 0)] + rel, RING)
                b = (m * 3 + part) * RING + c1
                row, col, at, is_g = decode(b, n_in // 2, n_out // 2)
                w_new = jnp.where(is_g == 1, 1.0 / n_all, (1.0 - FACTOR_DECAY) / n_all)
                w_old = jnp.where(is_g == 1, 0.0, FACTOR_DECAY / RING**3)
                rhs = ag[:, pl.ds(pl.multiple_of((2 * col + p) * BW, BW), BW)]
                prod = lax.dot_general(agt[row], rhs, NN, preferred_element_type=F32)
                acc[part, m, c1] = prod * w_new + old[at] * w_old
        each(0, nm, body)

    def hop(part, phase, step):
        return neighbour(d, pos, axis_of(part, phase), step)

    def both(k, part, phase, pairs):
        out = []
        for z, (step, src, dst) in enumerate(pairs):
            s = (k * 3 + part) * 2 + z
            c = remote(src, dst, ssem.at[s], rsem.at[s], hop(part, phase, step))
            c.start()
            out.append(c)
        return out

    cs = [[pos[axis_of(part, ph)] for ph in range(3)] for part in range(3)]
    rel = lambda part, ph, k: lax.rem(cs[part][ph] + k, RING)
    copies = []
    quarter(2)
    s1 = []
    for part in range(3):
        o = rel(part, 0, 2)
        s1.append(both(0, part, 0, [(1, acc.at[part, :, o, 0:64], ra1.at[part]), (3, acc.at[part, :, o, 64:128], rb1.at[part])]))
    quarter(1)
    s2 = []
    for z, k in enumerate((1, 3)):
        if z == 1:
            quarter(3)
        for part in range(3):
            u = rel(part, 0, k)
            s1[part][z].wait_recv()
            src = (ra1, rb1)[z]
            lo = 64 * z
            def body(m):
                acc[part, m, u, lo:lo + 64] = acc[part, m, u, lo:lo + 64] + src[part, m]
            each(0, nm, body)
            n = (3 + part) * 2 + z
            c = remote(acc.at[part, :, u], (rc1, rd1)[z].at[part], ssem.at[n], rsem.at[n], hop(part, 0, k))
            c.start()
            s2.append(c)
    quarter(0)
    for part in range(3):
        c1 = cs[part][0]
        s2[part].wait_recv()
        s2[3 + part].wait_recv()
        def body(m):
            acc[part, m, c1] = acc[part, m, c1] + (rc1[part, m] + rd1[part, m])
        each(0, nm, body)
        o = pl.multiple_of(rel(part, 1, 2) * 32, 32)
        copies.append(both(2, part, 1, [(1, acc.at[part, :, c1, pl.ds(o, 16)], ra2.at[part]), (3, acc.at[part, :, c1, pl.ds(o + 16, 16)], rb2.at[part])]))
    p2 = []
    for part in range(3):
        c1 = cs[part][0]
        lst = []
        for z, k in enumerate((1, 3)):
            u = pl.multiple_of(rel(part, 1, k) * 32, 32)
            copies[part][z].wait_recv()
            src = (ra2, rb2)[z]
            def body(m):
                r = pl.ds(pl.multiple_of(u + 16 * z, 16), 16)
                acc[part, m, c1, r] = acc[part, m, c1, r] + src[part, m]
            each(0, nm, body)
            n = (9 + part) * 2 + z
            c = remote(acc.at[part, :, c1, pl.ds(u, 32)], (rc2, rd2)[z].at[part], ssem.at[n], rsem.at[n], hop(part, 1, k))
            c.start()
            lst.append(c)
        p2.append(lst)
    h = (nm + 1) // 2
    p3 = []
    for part in range(3):
        c1 = cs[part][0]
        e = pl.multiple_of(cs[part][1] * 32, 32)
        for c in p2[part]:
            c.wait_recv()
        def body(m):
            acc[part, m, c1, pl.ds(e, 32)] = acc[part, m, c1, pl.ds(e, 32)] + (rc2[part, m] + rd2[part, m])
        each(0, nm, body)
        o = pl.multiple_of(e + rel(part, 2, 2) * 8, 8)
        p3.append(both(4, part, 2, [(1, acc.at[part, 0:h, c1, pl.ds(o, 8)], ra3.at[part]), (3, acc.at[part, h:nm, c1, pl.ds(o, 8)], rb3.at[part])]))
    p4 = []
    for part in range(3):
        c1 = cs[part][0]
        e = pl.multiple_of(cs[part][1] * 32, 32)
        lst = []
        for z, k in enumerate((1, 3)):
            u = pl.multiple_of(e + rel(part, 2, k) * 8, 8)
            p3[part][z].wait_recv()
            for m in range(h if z == 0 else nm - h):
                mm = m + h * z
                acc[part, mm, c1, pl.ds(u, 8)] = acc[part, mm, c1, pl.ds(u, 8)] + (ra3, rb3)[z][part, m]
            n = (15 + part) * 2 + z
            c = remote(acc.at[part, :, c1, pl.ds(u, 8)], (rc3, rd3)[z].at[part], ssem.at[n], rsem.at[n], hop(part, 2, k))
            c.start()
            lst.append(c)
        p4.append(lst)
    for part in range(3):
        c1 = cs[part][0]
        f = pl.multiple_of(cs[part][1] * 32 + cs[part][2] * 8, 8)
        for c in p4[part]:
            c.wait_recv()
        for m in range(nm):
            share[part, m] = acc[part, m, c1, pl.ds(f, 8)] + (rc3[part, m] + rd3[part, m])
    for group in (s1, copies, p2, p3, p4):
        for lst in group:
            for c in lst:
                c.wait_send()
    for c in s2:
        c.wait_send()

def stats(a_loc, g_loc, a_old3, s_old3):
    ns, c_in = a_loc.shape
    c_out = g_loc.shape[1]
    np_in, np_out = c_in // 256, c_out // 256
    nb = (np_in + np_out) * (np_in + np_out + 1)
    nm = nb // 12
    assert nm * 12 == nb
    h = (nm + 1) // 2
    hb = pl.BlockSpec(memory_space=pl.ANY)
    V = pltpu.VMEM
    s_blk = s_old3.reshape(-1, BW, BW)
    a_blk = a_old3.reshape(-1, BW, BW)
    return pl.pallas_call(functools.partial(stats_kernel, nm, ns, c_in, c_out),
        out_shape=jax.ShapeDtypeStruct((3, nm, 8, BW), F32),
        in_specs=[hb, hb, hb, hb], out_specs=pl.BlockSpec(memory_space=V),
        scratch_shapes=[V((ns, c_in + c_out), BF), V(((c_in + c_out) // BW, BW, ns), BF), V((s_blk.shape[0] + a_blk.shape[0], BW, BW), F32), V((3, nm, 4, BW, BW), F32),
            V((3, nm, 64, BW), F32), V((3, nm, 64, BW), F32), V((3, nm, 128, BW), F32), V((3, nm, 128, BW), F32),
            V((3, nm, 16, BW), F32), V((3, nm, 16, BW), F32), V((3, nm, 32, BW), F32), V((3, nm, 32, BW), F32),
            V((3, h, 8, BW), F32), V((3, nm - h, 8, BW), F32), V((3, nm, 8, BW), F32), V((3, nm, 8, BW), F32),
            pltpu.SemaphoreType.DMA((4,)), pltpu.SemaphoreType.DMA((36,)), pltpu.SemaphoreType.DMA((36,))],
        compiler_params=pltpu.CompilerParams(collective_id=0, has_side_effects=True, vmem_limit_bytes=63 * 2**20), name="stats_rs")(a_loc, g_loc, s_blk, a_blk)


def stack_dot(x, w, dims):
    xh, xm, xl = split3(x)
    wh, wm, wl = split3(w)
    k = x.shape[0]
    d = lambda u, v: lax.dot_general(u, v, dims, preferred_element_type=F32)
    p1 = d(jnp.concatenate([xh, xm, xl], 0), wh)
    p2 = d(jnp.concatenate([xh, xm], 0), wm)
    p3 = d(xh, wl)
    return (p1[2 * k:3 * k] + p2[k:2 * k] + p3) + (p1[k:2 * k] + p2[0:k]) + p1[0:k]

def solve_all_kernel(nm, np_in, np_out, n_dp, damp, share, x_out, a_out, s_out, full, tmat, mat, linv, inv_all, pan, pant, xw, zin, stage, ssem, rsem, psem, osem):
    p = lax.axis_index('mp')
    q_partner = 1 - p
    d, pos = coords()
    n_own = np_in * BW // n_dp
    cs = [[pos[axis_of(part, ph)] for ph in range(3)] for part in range(3)]
    own_rows = [pl.ds(pl.multiple_of(cs[part][1] * 32 + cs[part][2] * 8, 8), 8) for part in range(3)]
    for part in range(3):
        def put(m):
            full[p, m, part, cs[part][0], own_rows[part]] = share[part, m]
        each(0, nm, put)
    entry_barrier(d, pos, q_partner)
    pend = []

    def ag_round(k, m0, m1):
        ms = pl.ds(m0, m1 - m0)
        mh = m0 + (m1 - m0 + 1) // 2
        ma, mb = pl.ds(m0, mh - m0), pl.ds(mh, m1 - mh)
        def go(n, part, phase, step, ref):
            s = k * 36 + n
            c = remote(ref, ref, ssem.at[s], rsem.at[s], neighbour(d, pos, axis_of(part, phase), step))
            c.start()
            pend.append(c)
            return c
        for phase in (2, 1, 0):
            def piece(part, coord, half):
                c1, e = cs[part][0], cs[part][1]
                if phase == 2:
                    r = pl.ds(pl.multiple_of(e * 32 + coord * 8, 8), 8)
                    return full.at[p, (ms, ma, mb)[0 if half is None else half + 1], part, c1, r]
                if phase == 1:
                    r = pl.ds(pl.multiple_of(coord * 32 + (16 if half == 1 else 0), 16), 32 if half is None else 16)
                    return full.at[p, ms, part, c1, r]
                if half is None:
                    return full.at[p, ms, part, coord]
                return full.at[p, ms, part, coord, pl.ds(64 * half, 64)]
            first = []
            for part in range(3):
                c = cs[part][phase]
                n = (phase * 3 + part) * 4
                first.append([go(n, part, phase, 1, piece(part, c, None)), go(n + 1, part, phase, 3, piece(part, c, None))])
            second = []
            for part in range(3):
                c = cs[part][phase]
                n = (phase * 3 + part) * 4
                up, dn = lax.rem(c + 1, RING), lax.rem(c + 3, RING)
                first[part][0].wait_recv()
                second.append(go(n + 2, part, phase, 1, piece(part, dn, 0)))
                first[part][1].wait_recv()
                second.append(go(n + 3, part, phase, 3, piece(part, up, 1)))
            for c in second:
                c.wait_recv()
        ref = full.at[p, ms]
        c = pltpu.make_async_remote_copy(src_ref=ref, dst_ref=ref, send_sem=psem.at[0, k], recv_sem=psem.at[1, k], device_id={'mp': q_partner}, device_id_type=pl.DeviceIdType.MESH)
        c.start()
        pend.append(c)
        return c

    x1 = ag_round(0, 0, nm)
    x1.wait_recv()

    def block(par, b):
        return full[par, lax.div(b, 12), lax.div(lax.rem(b, 12), 4), lax.rem(b, 4)]

    n_in, n_out = 2 * np_in, 2 * np_out
    base_a = n_out
    base_s1 = n_out + np_in * (np_in + 1)
    base_g = base_s1 + np_out * (np_out + 1) - n_out
    def s_base(q):
        return q * n_out - q * (q - 1) + (base_s1 - n_out) * jnp.minimum(q, 1)
    def a_base(q):
        return base_a + q * n_in - q * (q - 1)
    is_a = p
    npan = np_out - (np_out - np_in) * p

    eye = jnp.where(lax.broadcasted_iota(jnp.int32, (BW, BW), 0) == lax.broadcasted_iota(jnp.int32, (BW, BW), 1), damp, 0.0)
    def load(q):
        base = is_a * a_base(q) + (1 - is_a) * s_base(q)
        for par in range(2):
            def rows(i):
                tmat[q, pl.ds(pl.multiple_of(i * BW, BW), BW), par * BW:(par + 1) * BW] = block(par, base + i - 2 * q)
            each(2 * q, 2 * npan, rows)
            r = pl.ds(pl.multiple_of((2 * q + par) * BW, BW), BW)
            tmat[q, r, par * BW:(par + 1) * BW] = tmat[q, r, par * BW:(par + 1) * BW] + eye
    each(0, npan, load)

    def panel(k):
        q = lax.div(k, 2)
        h = lax.rem(k, 2)
        r0 = pl.multiple_of(q * PW, PW)
        @pl.when(h == 0)
        def _():
            mat[...] = tmat[q, pl.ds(r0, BW), 0:BW]
        factor_block(mat, linv)
        @pl.when(h == 0)
        def _():
            inv0 = linv[...]
            inv0s = split3(inv0)
            l10 = dot6(split3(tmat[q, pl.ds(r0 + BW, BW), 0:BW]), inv0s, NT)
            l10s = split3(l10)
            mat[...] = tmat[q, pl.ds(r0 + BW, BW), BW:PW] - dot6(l10s, l10s, NT)
            inv_all[q, 0:BW, 0:BW] = inv0
            inv_all[q, 0:BW, BW:PW] = jnp.zeros((BW, BW), F32)
            inv_all[q, BW:PW, 0:BW] = dot6(l10s, inv0s, NN)
        @pl.when(h == 1)
        def _():
            inv1 = linv[...]
            inv_all[q, BW:PW, BW:PW] = inv1
            inv_all[q, BW:PW, 0:BW] = -dotf(inv1, inv_all[q, BW:PW, 0:BW], NN)
            invs = split3(inv_all[q])
            def below(i):
                r = pl.ds(pl.multiple_of(i * PW, PW), PW)
                lo = dot6(split3(tmat[q, r, :]), invs, NT)
                tmat[q, r, :] = lo
                sp = split3(lo)
                st = split3(lo.T)
                for z in range(3):
                    pan[z, r, :] = sp[z]
                    pant[z, i] = st[z]
            each(q + 1, npan, below)
            def trail(j):
                w = [pant[z, j] for z in range(3)]
                def rows(i):
                    r = pl.ds(pl.multiple_of(i * PW, PW), PW)
                    tmat[j, r, :] = tmat[j, r, :] - dot6([pan[z, r, :] for z in range(3)], w, NN)
                each(j, npan, rows)
            each(q + 1, npan, trail)
    each(0, 2 * npan, panel)

    zcopy = pltpu.make_async_remote_copy(src_ref=zin.at[0], dst_ref=zin.at[1], send_sem=psem.at[0, 2], recv_sem=psem.at[1, 2], device_id={'mp': q_partner}, device_id_type=pl.DeviceIdType.MESH)

    @pl.when(p == 1)
    def _():
        row = lax.broadcasted_iota(jnp.int32, (16, PW), 0)
        lane = lax.broadcasted_iota(jnp.int32, (16, PW), 1)
        par = lax.div(row, 8)
        idx = lax.rem(row, 8)
        col = d * n_own + idx
        for q in range(np_in):
            hit = (idx < n_own) & (lax.div(col, BW) == q) & (lane == par * BW + lax.rem(col, BW))
            xw[q] = jnp.where(hit, 1.0, 0.0)
    @pl.when(p == 0)
    def _():
        zcopy.wait_recv()
        def cp(q):
            xw[q] = zin[1, q]
        each(0, np_out, cp)

    def fwd(q):
        y = stack_dot(xw[q], inv_all[q], NT)
        xw[q] = y
        def sub(j):
            xw[j] = xw[j] - stack_dot(y, tmat[q, pl.ds(pl.multiple_of(j * PW, PW), PW), :], NT)
        each(q + 1, npan, sub)
    each(0, npan, fwd)
    def back(s):
        q = npan - 1 - s
        def sub(i, acc):
            return acc - stack_dot(xw[i], tmat[q, pl.ds(pl.multiple_of(i * PW, PW), PW), :], NN)
        xw[q] = stack_dot(lax.fori_loop(q + 1, npan, sub, xw[q]), inv_all[q], NN)
    each(0, npan, back)

    @pl.when(p == 1)
    def _():
        def zq(q):
            for par in range(2):
                acc = jnp.zeros((16, BW), F32)
                for i in range(n_in):
                    acc = acc + stack_dot(xw[i // 2, :, (i % 2) * BW:(i % 2 + 1) * BW], block(par, base_g + q * n_in + i), NN)
                zin[0, q, :, par * BW:(par + 1) * BW] = acc
        each(0, np_out, zq)
        zcopy.start()

    def column(out, slot, n_blk, par, q, base_fn):
        def lower(i):
            stage[slot, pl.ds(pl.multiple_of(i * BW, BW), BW), :] = block(par, base_fn(q) + i - 2 * q)
        each(2 * q, n_blk, lower)
        def upper(q2):
            for par2 in range(2):
                i = 2 * q2 + par2
                stage[slot, pl.ds(pl.multiple_of(i * BW, BW), BW), :] = block(par2, base_fn(q2) + (2 * q + par) - 2 * q2).T
        each(0, q, upper)

    def remote_out(slot, rows, out, q, s):
        return pltpu.make_async_remote_copy(src_ref=stage.at[slot, pl.ds(0, rows)], dst_ref=out.at[q], send_sem=osem.at[0, s], recv_sem=osem.at[1, s], device_id={'mp': 0}, device_id_type=pl.DeviceIdType.MESH)
    jobs = [(s_out, n_out, q, s_base) for q in range(np_out)] + [(a_out, n_in, q, a_base) for q in range(np_in)]
    @pl.when(p == 1)
    def _():
        live = {}
        for z, (out, n_blk, q, fn) in enumerate(jobs):
            for par in range(2):
                slot = (2 * z + par) % 4
                if slot in live:
                    live[slot]()
                column(out, slot, n_blk, par, q, fn)
                if par == 0:
                    c = remote_out(slot, n_blk * BW, out, q, z)
                    c.start()
                    live[slot] = c.wait_send
                else:
                    c = pltpu.make_async_copy(stage.at[slot, pl.ds(0, n_blk * BW)], out.at[q], osem.at[0, len(jobs) + z])
                    c.start()
                    live[slot] = c.wait
        for fn in live.values():
            fn()
        zcopy.wait_send()

    xcopy = pltpu.make_async_remote_copy(src_ref=zin.at[0, :, pl.ds(8, 8)], dst_ref=x_out, send_sem=psem.at[0, 3], recv_sem=psem.at[1, 3], device_id={'mp': q_partner}, device_id_type=pl.DeviceIdType.MESH)
    @pl.when(p == 0)
    def _():
        def cp(q):
            zin[0, q] = xw[q]
            x_out[q] = xw[q, 0:8]
        each(0, np_out, cp)
        xcopy.start()
        for z, (out, n_blk, q, fn) in enumerate(jobs):
            remote_out(0, n_blk * BW, out, q, z).wait_recv()
        xcopy.wait_send()
    @pl.when(p == 1)
    def _():
        xcopy.wait_recv()
    for c in pend:
        c.wait_send()

def solve_all(share, np_in, np_out, n_dp, damp):
    nm = share.shape[1]
    n_in, n_out = 2 * np_in, 2 * np_out
    hb = pl.BlockSpec(memory_space=pl.ANY)
    V = pltpu.VMEM
    vb = pl.BlockSpec(memory_space=V)
    njob = np_in + np_out
    return pl.pallas_call(functools.partial(solve_all_kernel, nm, np_in, np_out, n_dp, damp),
        out_shape=(jax.ShapeDtypeStruct((np_out, 8, PW), F32), jax.ShapeDtypeStruct((np_in, n_in * BW, BW), F32), jax.ShapeDtypeStruct((np_out, n_out * BW, BW), F32)),
        in_specs=[vb], out_specs=(vb, hb, hb),
        scratch_shapes=[V((2, nm, 3, 4, BW, BW), F32), V((np_out, n_out * BW, PW), F32), V((BW, BW), F32), V((BW, BW), F32), V((np_out, PW, PW), F32),
            V((3, n_out * BW, PW), BF), V((3, np_out, PW, PW), BF), V((np_out, 16, PW), F32), V((2, np_out, 16, PW), F32), V((4, n_out * BW, BW), F32),
            pltpu.SemaphoreType.DMA((36,)), pltpu.SemaphoreType.DMA((36,)), pltpu.SemaphoreType.DMA((2, 4)), pltpu.SemaphoreType.DMA((2, 2 * njob))],
        compiler_params=pltpu.CompilerParams(collective_id=1, has_side_effects=True, vmem_limit_bytes=63 * 2**20), name="factor_solve")(share)


def solution(mesh):
    n_dp = mesh.shape['dp']

    def local_step(a_loc, g_loc, w_loc, a_old_loc, s_old_loc):
        np_in = a_loc.shape[1] // PW
        np_out = g_loc.shape[1] // PW
        share = stats(a_loc, g_loc, a_old_loc.transpose(1, 0, 2), s_old_loc.transpose(1, 0, 2))
        xt, a3, s3 = solve_all(share, np_in, np_out, n_dp, DAMP_SHIFT)
        n_own = np_in * BW // n_dp
        delta = lax.all_gather(xt[:, :n_own, :], 'dp').transpose(1, 3, 0, 2).reshape(w_loc.shape)
        return (w_loc - LEARN_RATE * delta, a3.transpose(1, 0, 2), s3.transpose(1, 0, 2))

    spec_rows = P('dp', None)
    spec_cyc = P(None, 'mp', None)
    return jax.shard_map(local_step, mesh=mesh, in_specs=(spec_rows, spec_rows, spec_cyc, spec_cyc, spec_cyc), out_specs=(spec_cyc, spec_cyc, spec_cyc), check_vma=False)
```

```python
import functools
import math
import numpy as np
import jax
import jax.numpy as jnp
from jax import lax
from jax.experimental import pallas as pl
from jax.experimental.pallas import tpu as pltpu
from jax.sharding import PartitionSpec as P

FACTOR_DECAY = 0.95
DAMPING = 0.001
DAMP_SHIFT = math.sqrt(DAMPING)
LEARN_RATE = 1.0
BW = 128
PW = 256
RING = 4
SUBL = 8
HALVES = (0, 1)
PARTS = (0, 1, 2)
UPDOWN = (1, 3)
HALF = 64
GROUP = 12
F32 = jnp.float32
BF = jnp.bfloat16
NT = (((1,), (1,)), ((), ()))
NN = (((1,), (0,)), ((), ()))


MB = 16

def split3(x):
    h = x.astype(BF)
    r = x - h.astype(F32)
    m = r.astype(BF)
    return h, m, (r - m.astype(F32)).astype(BF)

def lane_bc(x, i, zero):
    return bc(x[:, i:i + 1]) + zero

def bc(x):
    return jnp.broadcast_to(x, (SUBL, BW))

def factor_block(mat, linv, beside=None):
    lane = lax.broadcasted_iota(jnp.int32, (SUBL, BW), 1)
    sub = lax.broadcasted_iota(jnp.int32, (SUBL, BW), 0)
    zero = lane.astype(F32) * 0.0
    nxt = None
    for t in range(BW // MB):
        k = t * MB
        if beside is not None:
            beside(t)
        rows = [mat[k + SUBL * r:k + SUBL * r + SUBL, :] for r in HALVES] if nxt is None else nxt
        cols = [[lane_bc(rows[r], k + i, zero) for r in HALVES] for i in range(MB)]
        inside = (lane >= k) & (lane < k + MB)
        ext = [jnp.where(inside, jnp.where(lane == sub + (k + SUBL * r), 1.0, 0.0), rows[r]) for r in HALVES]
        more = k + MB < BW
        far = k + MB + MB < BW
        if more:
            near = [mat[k + MB + SUBL * r:k + MB + SUBL * r + SUBL, :] for r in HALVES]
            mult = [[lane_bc(near[r], k + i, zero) for r in HALVES] for i in range(MB)]
        if far:
            rh, rm, rl = split3(jnp.concatenate(rows, 0))
            left = jnp.concatenate([rh, rh, rm, rh, rl, rm], 0).T[k + MB + MB:, :]
        rv = [None, None]
        for j in range(0, MB, 2):
            jr, js = divmod(j, SUBL)
            u, v = cols[j], cols[j + 1]
            a, b, c = bc(u[jr][js:js + 1]), bc(u[jr][js + 1:js + 2]), bc(v[jr][js + 1:js + 2])
            det = a * c - b * b
            rdet = 1.0 / det
            ra = 1.0 / a
            e0, e1 = bc(ext[jr][js:js + 1]), bc(ext[jr][js + 1:js + 2])
            linv[k + j:k + j + 1, :] = (e0 * lax.rsqrt(a))[:1]
            linv[k + j + 1:k + j + 2, :] = ((e1 - (b * ra) * e0) * lax.rsqrt(det * ra))[:1]
            pair = (sub == js) | (sub == js + 1)
            um, vm = ([jnp.where(pair, 0.0, x[r]) if r == jr else x[r] for r in HALVES] for x in (u, v))
            n0 = [c * um[r] - b * vm[r] for r in HALVES]
            n1 = [a * vm[r] - b * um[r] for r in HALVES]
            f0 = [n0[r] * rdet for r in HALVES]
            f1 = [n1[r] * rdet for r in HALVES]
            for i in range(j + 2, MB):
                b0, b1 = bc(cols[i][jr][js:js + 1]), bc(cols[i][jr][js + 1:js + 2])
                if i < j + 4:
                    cols[i] = [cols[i][r] - (n0[r] * b0 + n1[r] * b1) * rdet for r in HALVES]
                else:
                    cols[i] = [cols[i][r] - (f0[r] * b0 + f1[r] * b1) for r in HALVES]
            ext = [ext[r] - (f0[r] * e0 + f1[r] * e1) for r in HALVES]
            w0, w1 = (c * e0 - b * e1) * rdet, (a * e1 - b * e0) * rdet
            own = (a * rdet, b * rdet, c * rdet)
            rv[jr] = [(js, own)] if js == 0 else rv[jr] + [(js, own)]
        w = []
        for r in HALVES:
            cur = ext[r]
            swap = jnp.where(lax.rem(sub, 2) == 0, jnp.roll(cur, -1, 0), jnp.roll(cur, 1, 0))
            dg = of = None
            for js, (ad, bd, cd) in rv[r]:
                d_here = jnp.where(sub == js, cd, ad)
                if dg is None:
                    dg, of = d_here, bd
                else:
                    dg = jnp.where(sub >= js, d_here, dg)
                    of = jnp.where(sub >= js, bd, of)
            w.append(cur * dg - swap * of)
        if more:
            nxt = []
            for r in HALVES:
                terms = [mult[j][r] * bc(w[j // SUBL][j % SUBL:j % SUBL + 1]) for j in range(MB)]
                while len(terms) > 1:
                    terms = [x + y for x, y in zip(terms[::2], terms[1::2])]
                nxt.append(jnp.where(inside, 0.0, near[r]) - terms[0])
        if far:
            wh, wm, wl = split3(jnp.concatenate(w, 0))
            right = jnp.concatenate([wh, wm, wh, wl, wh, wm], 0)
            prod = lax.dot_general(left, right, NN, preferred_element_type=F32)
            ins = jnp.broadcast_to(inside[:1], (BW - k - 2 * MB, BW))
            mat[k + MB + MB:, :] = jnp.where(ins, 0.0, mat[k + MB + MB:, :]) - prod
    ri = lax.broadcasted_iota(jnp.int32, (BW, BW), 0)
    ci = lax.broadcasted_iota(jnp.int32, (BW, BW), 1)
    linv[...] = jnp.where(ci <= ri, linv[...], 0.0)


EARLY = 2

def coords():
    d = lax.axis_index('dp')
    x = lax.rem(d, RING)
    y = lax.rem(lax.div(d, RING), RING)
    z = lax.div(d, RING * RING)
    return d, (x, y, z)

def neighbour(d, pos, axis, step):
    stride = (1, RING, RING * RING)[axis]
    return d + (lax.rem(pos[axis] + step, RING) - pos[axis]) * stride

def axis_of(part, phase):
    return (part + phase) % 3

def entry_barrier(d, pos, partner):
    sem = pltpu.get_barrier_semaphore()
    count = 0
    for axis in PARTS:
        for step in ((1, 3, 2) if partner is not None else UPDOWN):
            pl.semaphore_signal(sem, inc=1, device_id={'dp': neighbour(d, pos, axis, step)}, device_id_type=pl.DeviceIdType.MESH)
            count += 1
    if partner is not None:
        pl.semaphore_signal(sem, inc=1, device_id={'mp': partner}, device_id_type=pl.DeviceIdType.MESH)
        count += 1
    pl.semaphore_wait(sem, count)

def remote(src, dst, ssem, rsem, dev):
    return pltpu.make_async_remote_copy(src_ref=src, dst_ref=dst, send_sem=ssem, recv_sem=rsem, device_id={'dp': dev}, device_id_type=pl.DeviceIdType.MESH)

def each(lo, hi, fn):
    def body(i, c):
        fn(i)
        return c
    lax.fori_loop(lo, hi, body, 0)

def decode(b, np_in, np_out):
    n_in, n_out = 2 * np_in, 2 * np_out
    starts, at = [], 0
    for q0, base_row, base_col, n in [(q, n_in, np_in, n_out) for q in range(EARLY)] + [(q, 0, 0, n_in) for q in range(np_in)] + [(q, n_in, np_in, n_out) for q in range(EARLY, np_out)]:
        starts.append((at, base_row + 2 * q0 - at, base_col + q0))
        at += n - 2 * q0
    row, col, was = b, 0, (0, 0)
    for z, (first, d_row, d_col) in enumerate(starts):
        hit = 1 if z == 0 else (b >= first).astype(jnp.int32)
        row = row + hit * (d_row - was[0])
        col = col + hit * (d_col - was[1])
        was = (d_row, d_col)
    is_g = (b >= at).astype(jnp.int32)
    g_row, g_col = lax.rem(b - at * is_g, n_in), np_in + lax.div(b - at * is_g, n_in)
    row = row + is_g * (g_row - row)
    col = col + is_g * (g_col - col)
    in_s = (col >= np_in).astype(jnp.int32)
    old = in_s * ((col - np_in) * n_out + row - n_in) + (1 - in_s) * (np_out * n_out + col * n_in + row)
    return row, col, (1 - is_g) * old, is_g

def stats_kernel(nm, ns, c_in, c_out, a_hbm, g_hbm, s_hbm, ao_hbm, share, ag, agt, old, acc, ra1, rb1, rc1, rd1, ra2, rb2, rc2, rd2, ra3, rb3, rc3, rd3, lsem, ssem, rsem):
    p = lax.axis_index('mp')
    d, pos = coords()
    n_in, n_out = c_in // BW, c_out // BW
    n_all = ns * RING**3
    nso = s_hbm.shape[0]
    loads = [pltpu.make_async_copy(a_hbm, ag.at[:, 0:c_in], lsem.at[0]), pltpu.make_async_copy(g_hbm, ag.at[:, c_in:c_in + c_out], lsem.at[1]),
        pltpu.make_async_copy(s_hbm, old.at[0:nso], lsem.at[2]), pltpu.make_async_copy(ao_hbm, old.at[nso:nso + ao_hbm.shape[0]], lsem.at[3])]
    for c in loads:
        c.start()
    entry_barrier(d, pos, None)
    ck = min(512, ns)
    for z, (base, cnt) in enumerate(((0, n_in), (n_in, n_out))):
        loads[z].wait()
        def flip(c):
            for r in range(ns // ck):
                agt[base + c, :, r * ck:(r + 1) * ck] = ag[r * ck:(r + 1) * ck, pl.ds(pl.multiple_of((base + c) * BW, BW), BW)].T
        each(0, cnt, flip)
    loads[2].wait()
    loads[3].wait()

    def quarter(rel):
        def body(m):
            for part in PARTS:
                c1 = lax.rem(pos[axis_of(part, 0)] + rel, RING)
                b = (m * 3 + part) * RING + c1
                row, col, at, is_g = decode(b, n_in // 2, n_out // 2)
                w_new = jnp.where(is_g == 1, 1.0 / n_all, (1.0 - FACTOR_DECAY) / n_all)
                w_old = jnp.where(is_g == 1, 0.0, FACTOR_DECAY / RING**3)
                rhs = ag[:, pl.ds(pl.multiple_of((2 * col + p) * BW, BW), BW)]
                prod = lax.dot_general(agt[row], rhs, NN, preferred_element_type=F32)
                acc[part, m, c1] = prod * w_new + old[at] * w_old
        each(0, nm, body)

    def hop(part, phase, step):
        return neighbour(d, pos, axis_of(part, phase), step)

    def both(k, part, phase, pairs):
        out = []
        for z, (step, src, dst) in enumerate(pairs):
            s = (k * 3 + part) * 2 + z
            c = remote(src, dst, ssem.at[s], rsem.at[s], hop(part, phase, step))
            c.start()
            out.append(c)
        return out

    cs = [[pos[axis_of(part, ph)] for ph in range(3)] for part in PARTS]
    rel = lambda part, ph, k: lax.rem(cs[part][ph] + k, RING)
    copies = []
    quarter(2)
    s1 = []
    for part in PARTS:
        o = rel(part, 0, 2)
        s1.append(both(0, part, 0, [(1, acc.at[part, :, o, :HALF], ra1.at[part]), (3, acc.at[part, :, o, HALF:], rb1.at[part])]))
    quarter(1)
    s2 = []
    for z, k in enumerate(UPDOWN):
        if z == 1:
            quarter(3)
        for part in PARTS:
            u = rel(part, 0, k)
            s1[part][z].wait_recv()
            src = (ra1, rb1)[z]
            lo = HALF * z
            def body(m):
                acc[part, m, u, lo:lo + HALF] = acc[part, m, u, lo:lo + HALF] + src[part, m]
            each(0, nm, body)
            n = (3 + part) * 2 + z
            c = remote(acc.at[part, :, u], (rc1, rd1)[z].at[part], ssem.at[n], rsem.at[n], hop(part, 0, k))
            c.start()
            s2.append(c)
    quarter(0)
    for part in PARTS:
        c1 = cs[part][0]
        s2[part].wait_recv()
        s2[3 + part].wait_recv()
        def body(m):
            acc[part, m, c1] = acc[part, m, c1] + (rc1[part, m] + rd1[part, m])
        each(0, nm, body)
        o = pl.multiple_of(rel(part, 1, 2) * 32, 32)
        copies.append(both(2, part, 1, [(1, acc.at[part, :, c1, pl.ds(o, 16)], ra2.at[part]), (3, acc.at[part, :, c1, pl.ds(o + 16, 16)], rb2.at[part])]))
    p2 = []
    for part in PARTS:
        c1 = cs[part][0]
        lst = []
        for z, k in enumerate(UPDOWN):
            u = pl.multiple_of(rel(part, 1, k) * 32, 32)
            copies[part][z].wait_recv()
            src = (ra2, rb2)[z]
            def body(m):
                r = pl.ds(pl.multiple_of(u + 16 * z, 16), 16)
                acc[part, m, c1, r] = acc[part, m, c1, r] + src[part, m]
            each(0, nm, body)
            n = (9 + part) * 2 + z
            c = remote(acc.at[part, :, c1, pl.ds(u, 32)], (rc2, rd2)[z].at[part], ssem.at[n], rsem.at[n], hop(part, 1, k))
            c.start()
            lst.append(c)
        p2.append(lst)
    h = (nm + 1) // 2
    p3 = []
    for part in PARTS:
        c1 = cs[part][0]
        e = pl.multiple_of(cs[part][1] * 32, 32)
        for c in p2[part]:
            c.wait_recv()
        def body(m):
            acc[part, m, c1, pl.ds(e, 32)] = acc[part, m, c1, pl.ds(e, 32)] + (rc2[part, m] + rd2[part, m])
        each(0, nm, body)
        o = pl.multiple_of(e + rel(part, 2, 2) * SUBL, SUBL)
        p3.append(both(4, part, 2, [(1, acc.at[part, 0:h, c1, pl.ds(o, SUBL)], ra3.at[part]), (3, acc.at[part, h:nm, c1, pl.ds(o, SUBL)], rb3.at[part])]))
    p4 = []
    for part in PARTS:
        c1 = cs[part][0]
        e = pl.multiple_of(cs[part][1] * 32, 32)
        lst = []
        for z, k in enumerate(UPDOWN):
            u = pl.multiple_of(e + rel(part, 2, k) * SUBL, SUBL)
            p3[part][z].wait_recv()
            for m in range(h if z == 0 else nm - h):
                mm = m + h * z
                acc[part, mm, c1, pl.ds(u, SUBL)] = acc[part, mm, c1, pl.ds(u, SUBL)] + (ra3, rb3)[z][part, m]
            n = (15 + part) * 2 + z
            c = remote(acc.at[part, :, c1, pl.ds(u, SUBL)], (rc3, rd3)[z].at[part], ssem.at[n], rsem.at[n], hop(part, 2, k))
            c.start()
            lst.append(c)
        p4.append(lst)
    for part in PARTS:
        c1 = cs[part][0]
        f = pl.multiple_of(cs[part][1] * 32 + cs[part][2] * SUBL, SUBL)
        for c in p4[part]:
            c.wait_recv()
        for m in range(nm):
            share[part, m] = acc[part, m, c1, pl.ds(f, SUBL)] + (rc3[part, m] + rd3[part, m])
    for group in (s1, copies, p2, p3, p4):
        for lst in group:
            for c in lst:
                c.wait_send()
    for c in s2:
        c.wait_send()

def stats(a_loc, g_loc, a_old3, s_old3):
    ns, c_in = a_loc.shape
    c_out = g_loc.shape[1]
    np_in, np_out = c_in // 256, c_out // 256
    nb = (np_in + np_out) * (np_in + np_out + 1)
    nm = nb // GROUP
    assert nm * GROUP == nb
    h = (nm + 1) // 2
    hb = pl.BlockSpec(memory_space=pl.ANY)
    V = pltpu.VMEM
    slab = lambda n: [V((len(PARTS), nm, n, BW), F32)] * 2
    s_blk = s_old3.reshape(-1, BW, BW)
    a_blk = a_old3.reshape(-1, BW, BW)
    return pl.pallas_call(functools.partial(stats_kernel, nm, ns, c_in, c_out),
        out_shape=jax.ShapeDtypeStruct((3, nm, SUBL, BW), F32),
        in_specs=[hb, hb, hb, hb], out_specs=pl.BlockSpec(memory_space=V),
        scratch_shapes=[V((ns, c_in + c_out), BF), V(((c_in + c_out) // BW, BW, ns), BF), V((s_blk.shape[0] + a_blk.shape[0], BW, BW), F32), V((3, nm, 4, BW, BW), F32),
            *slab(HALF), *slab(BW), *slab(16), *slab(32),
            V((3, h, SUBL, BW), F32), V((3, nm - h, SUBL, BW), F32), *slab(SUBL),
            pltpu.SemaphoreType.DMA((4,)), pltpu.SemaphoreType.DMA((36,)), pltpu.SemaphoreType.DMA((36,))],
        compiler_params=pltpu.CompilerParams(collective_id=0, has_side_effects=True, vmem_limit_bytes=63 * 2**20), name="stats_rs")(a_loc, g_loc, s_blk, a_blk)


def dot6(a, b, dims):
    d = lambda x, y: lax.dot_general(x, y, dims, preferred_element_type=F32)
    ah, am, al = a
    bh, bm, bl = b
    return (d(am, bm) + d(ah, bl) + d(al, bh)) + (d(ah, bm) + d(am, bh)) + d(ah, bh)

def stack_dot(x, w, dims):
    xh, xm, xl = x
    wh, wm, wl = w
    k = xh.shape[0]
    d = lambda u, v: lax.dot_general(u, v, dims, preferred_element_type=F32)
    p1 = d(jnp.concatenate([xh, xm, xl], 0), wh)
    p2 = d(jnp.concatenate([xh, xm], 0), wm)
    p3 = d(xh, wl)
    return (p1[k + k:] + p2[k:] + p3) + (p1[k:k + k] + p2[:k]) + p1[:k]

def pieces(ref, at):
    return [ref[z, at] for z in PARTS]

def rows_at(start, size):
    return pl.ds(pl.multiple_of(start, SUBL), size)

def to_partner(src, dst, sems, s):
    return pltpu.make_async_remote_copy(src_ref=src, dst_ref=dst, send_sem=sems.at[0, s], recv_sem=sems.at[1, s], device_id={'mp': 1 - lax.axis_index('mp')}, device_id_type=pl.DeviceIdType.MESH)

def ring_steps(spot, base, ssem, rsem):
    d, pos = coords()
    def copy(part, phase, z):
        axis = axis_of(part, phase)
        c = pos[axis]
        step, come = ((1, None), (3, None), (2, None), (1, 3), (3, 1))[z]
        ref = spot(part, phase, c, None) if come is None else spot(part, phase, lax.rem(c + come, RING), z - 3)
        s = base + (part * 3 + phase) * 4 + z - (z > 2)
        return remote(ref, ref, ssem.at[s], rsem.at[s], neighbour(d, pos, axis, step))
    def act(phase, zs, name):
        for part in PARTS:
            for z in zs:
                getattr(copy(part, phase, z), name)()
    every, near, on = PARTS, HALVES, (3, 4)
    def relay():
        for z in near:
            act(0, (z,), 'wait_recv')
            act(0, (z + 3,), 'start')
    def settle():
        act(2, every, 'wait_send')
        act(1, every, 'wait_send')
        act(0, near + on, 'wait_send')
    steps = [lambda: act(2, every, 'start'), lambda: (act(2, every, 'wait_recv'), act(1, every, 'start')), lambda: (act(1, every, 'wait_recv'), act(0, near, 'start')),
        relay, lambda: act(0, on, 'wait_recv')]
    return steps, settle

def block_at(q, np_in, np_out, of_s):
    n_in, n_out = 2 * np_in, 2 * np_out
    in_s = q * n_out - q * (q - 1) + np_in * (np_in + 1) * jnp.minimum(lax.div(q, EARLY), 1)
    in_a = EARLY * n_out - EARLY * (EARLY - 1) + q * n_in - q * (q - 1)
    return of_s * in_s + (1 - of_s) * in_a

def solve_all_kernel(nm, np_in, np_out, n_dp, damp, rounds, plan, share, blocks, fin0, fin1, fin2, full, tmat, mat, linv, inv_all, lsp, xw, zin, pack, ssem, rsem, psem, osem):
    p = lax.axis_index('mp')
    d, pos = coords()
    n_own = np_in * BW // n_dp
    n_in, n_out = 2 * np_in, 2 * np_out
    n_rounds = len(rounds) - 1
    per_round = 36
    cs = [[pos[axis_of(part, ph)] for ph in PARTS] for part in PARTS]
    for part in PARTS:
        c1, e, f = cs[part]
        def put(m):
            full[p, m, part, c1, rows_at(e * 32 + f * SUBL, SUBL)] = share[part, m]
        each(0, nm, put)
    entry_barrier(d, pos, 1 - p)

    def gather(k):
        ms = pl.ds(rounds[k], rounds[k + 1] - rounds[k])
        def spot(part, phase, coord, half):
            c1, e, f = cs[part]
            if phase == 2:
                return full.at[p, ms, part, c1, rows_at(e * 32 + coord * SUBL, SUBL)]
            if phase == 1:
                return full.at[p, ms, part, c1, rows_at(coord * 32, 32)]
            size = BW if half is None else BW // 2
            return full.at[p, ms, part, coord, pl.ds((half or 0) * size, size)]
        steps, settle = ring_steps(spot, k * per_round, ssem, rsem)
        swap = lambda: to_partner(full.at[p, ms], full.at[p, ms], psem, k)
        def keep(half):
            return pltpu.make_async_copy(full.at[half, ms], blocks.at[half, ms], osem.at[half, k])
        def close():
            swap().wait_recv()
            for half in HALVES:
                keep(half).start()
        def finish():
            settle()
            swap().wait_send()
            for half in HALVES:
                keep(half).wait()
        last = steps[-1]
        steps[-1] = lambda: (last(), swap().start())
        return steps + [close], finish

    gathers = [gather(k) for k in range(n_rounds)]
    agenda = {}
    for (steps, _), times in zip(gathers, plan):
        for fn, z in zip(steps, times):
            agenda.setdefault(z, []).append(fn)
    for z in sorted(z for z in agenda if z < 0):
        for fn in agenda[z]:
            fn()
    poll = sorted(z for z in agenda if z >= 0)
    closing = [g[0][-1] for g in gathers]
    n_a_round = n_rounds
    @pl.when(p == 1)
    def _():
        for z in poll:
            for fn in agenda[z]:
                if fn not in closing[n_a_round:]:
                    fn()

    def block(par, b):
        return full[par, lax.div(b, GROUP), lax.div(lax.rem(b, GROUP), RING), lax.rem(b, RING)]

    base_g = np_out * (np_out + 1) + np_in * (np_in + 1)
    npan = np_out - (np_out - np_in) * p
    eye = jnp.where(lax.broadcasted_iota(jnp.int32, (BW, BW), 0) == lax.broadcasted_iota(jnp.int32, (BW, BW), 1), damp, 0.0)

    def load(q):
        base = block_at(q, np_in, np_out, 1 - p)
        slot = lax.rem(q, 2)
        for par in HALVES:
            cols = pl.ds(par * BW, BW)
            def rows(i):
                for h in HALVES:
                    tmat[slot, i, h * BW:(h + 1) * BW, cols] = block(par, base + 2 * (i - q) + h)
            each(q, npan, rows)
            tmat[slot, q, cols, cols] = tmat[slot, q, cols, cols] + eye

    def ltile(i, k):
        return lax.div(i * (i - 1), 2) + k

    def update(i, k, q, ok):
        slot = lax.rem(q, 2)
        at = ok * i + (1 - ok) * np_out
        prod = stack_dot(pieces(lsp, ok * ltile(i, k)), pieces(lsp, ok * ltile(q, k)), NT)
        tmat[slot, at] = tmat[slot, at] - prod

    def task(s, q):
        left = jnp.maximum(npan - 1 - q, 1)
        turn = lax.div(s, left)
        ok = (turn <= q).astype(jnp.int32) * jnp.minimum(q, 1) * jnp.minimum(npan - 1 - q, 1)
        k = turn - 1 + q * (1 - jnp.minimum(turn, 1))
        update(q + 1 + lax.rem(s, left), k, q + jnp.minimum(turn, 1), ok)

    load(0)
    n_slot = MB

    def panel(k):
        q = lax.div(k, 2)
        h = lax.rem(k, 2)
        slot = lax.rem(q, 2)
        @pl.when(h == 0)
        def _():
            mat[...] = tmat[slot, q, :BW, :BW]
        factor_block(mat, linv, lambda t: task(h * SUBL + t, q))
        @pl.when(h == 0)
        def _():
            inv0 = linv[...]
            inv0s = split3(inv0)
            l10 = dot6(split3(tmat[slot, q, BW:, :BW]), inv0s, NT)
            l10s = split3(l10)
            mat[...] = tmat[slot, q, BW:, BW:] - dot6(l10s, l10s, NT)
            inv_all[q, :BW, :BW] = inv0
            inv_all[q, :BW, BW:] = jnp.zeros((BW, BW), F32)
            inv_all[q, BW:, :BW] = dot6(l10s, inv0s, NN)
        @pl.when((h == 1) & (q < npan - 1))
        def _():
            each(n_slot, (npan - 1 - q) * (q + 1), lambda s: task(s, q))
        @pl.when(h == 1)
        def _():
            inv1 = linv[...]
            inv_all[q, BW:, BW:] = inv1
            inv_all[q, BW:, :BW] = -dot6(split3(inv1), split3(inv_all[q, BW:, :BW]), NN)
            invs = split3(inv_all[q])
            def below(i):
                for z, v in enumerate(split3(stack_dot(split3(tmat[slot, i]), invs, NT))):
                    lsp[z, ltile(i, q)] = v
            each(q + 1, npan, below)
        for z in poll:
            @pl.when((p == 0) & (k == z))
            def _():
                for fn in agenda[z]:
                    fn()
        @pl.when((h == 1) & (q < npan - 1))
        def _():
            @pl.when(q == 0)
            def _():
                load(1)
            update(q + 1, q, q + 1, 1)
            @pl.when(q < npan - 2)
            def _():
                load(q + 2)
    each(0, 2 * npan, panel)

    zcopy = to_partner(zin.at[0], zin.at[1], psem, n_rounds)
    @pl.when(p == 1)
    def _():
        row = lax.broadcasted_iota(jnp.int32, (MB, PW), 0)
        lane = lax.broadcasted_iota(jnp.int32, (MB, PW), 1)
        par = lax.div(row, SUBL)
        idx = lax.rem(row, SUBL)
        col = d * n_own + idx
        for q in range(np_in):
            hit = (idx < n_own) & (lax.div(col, BW) == q) & (lane == par * BW + lax.rem(col, BW))
            xw[q] = jnp.where(hit, 1.0, 0.0)
    @pl.when(p == 0)
    def _():
        zcopy.wait_recv()
        def cp(q):
            xw[q] = zin[1, q]
        each(0, np_out, cp)

    def fwd(q):
        y = stack_dot(split3(xw[q]), split3(inv_all[q]), NT)
        xw[q] = y
        ys = split3(y)
        def sub(j):
            xw[j] = xw[j] - stack_dot(ys, pieces(lsp, ltile(j, q)), NT)
        each(q + 1, npan, sub)
    each(0, npan, fwd)
    def back(s):
        q = npan - 1 - s
        x = stack_dot(split3(xw[q]), split3(inv_all[q]), NN)
        xw[q] = x
        xs = split3(x)
        def sub(j):
            xw[j] = xw[j] - stack_dot(xs, pieces(lsp, ltile(q, j)), NN)
        each(0, q, sub)
    each(0, npan, back)

    xcopy = to_partner(pack.at[1], pack.at[0], psem, n_rounds + 1)
    @pl.when(p == 1)
    def _():
        for fn in closing[n_a_round:]:
            fn()
        def zq(q):
            for par in HALVES:
                acc = jnp.zeros((MB, BW), F32)
                for i in range(n_in):
                    acc = acc + stack_dot(split3(xw[i // 2, :, (i % 2) * BW:(i % 2 + 1) * BW]), split3(block(par, base_g + q * n_in + i)), NN)
                zin[0, q, :, par * BW:(par + 1) * BW] = acc
        each(0, np_out, zq)
        zcopy.start()
        xcopy.wait_recv()
        zcopy.wait_send()
    @pl.when(p == 0)
    def _():
        for par in reversed(HALVES):
            pack[par, np_out * n_own:] = jnp.zeros((pack.shape[1] - np_out * n_own, PW), F32)
            for q in range(np_out):
                pack[par, q * n_own:(q + 1) * n_own] = xw[q, par * SUBL:par * SUBL + n_own]
            if par == 1:
                xcopy.start()
    fins = (fin0, fin1, fin2)
    t = 0
    for part in PARTS:
        for z in range(fins[part].shape[3]):
            half = t % 2
            fins[part][(*cs[part], z)] = pack[0, t // 2 * SUBL:(t // 2 + 1) * SUBL, half * BW:(half + 1) * BW]
            t += 1
    def spot(part, phase, coord, half):
        at = (*cs[part][:phase], coord)
        return fins[part].at[at if half is None else (*at, pl.ds(2 * half, 2))]
    steps, settle = ring_steps(spot, n_rounds * per_round, ssem, rsem)
    for fn in steps:
        fn()
    settle()
    @pl.when(p == 0)
    def _():
        xcopy.wait_send()
    for _, finish in gathers:
        finish()

def solve_all(share, np_in, np_out, n_dp, damp):
    nm = share.shape[1]
    n_own = np_in * BW // n_dp
    n_row = -(-np_out * n_own // SUBL)
    tiles = [-(-(2 * n_row - part) // 3) for part in PARTS]
    V = pltpu.VMEM
    vb = pl.BlockSpec(memory_space=V)
    hb = pl.BlockSpec(memory_space=pl.ANY)
    gathered = (2, nm, 3, 4, BW, BW)
    rounds = (0, 2, 5, 8, nm)
    plan = [range(k - 9, k - 3) for k in range(len(rounds) - 1)]
    n_rounds = len(rounds) - 1
    n_tile = np_out * (np_out - 1) // 2
    D = pltpu.SemaphoreType.DMA
    sems = 36 * (n_rounds + 1)
    return pl.pallas_call(functools.partial(solve_all_kernel, nm, np_in, np_out, n_dp, damp, rounds, plan),
        out_shape=(jax.ShapeDtypeStruct(gathered, F32), *(jax.ShapeDtypeStruct((4, 4, 4, t, SUBL, BW), F32) for t in tiles)),
        in_specs=[vb], out_specs=(hb, vb, vb, vb),
        scratch_shapes=[V(gathered, F32), V((2, np_out + 1, PW, PW), F32), *[V((BW, BW), F32)] * 2, V((np_out, PW, PW), F32),
            V((3, n_tile, PW, PW), BF), V((np_out, MB, PW), F32), V((2, np_out, MB, PW), F32), V((2, n_row * SUBL, PW), F32),
            D((sems,)), D((sems,)), D((2, n_rounds + 2)), D((2, n_rounds))],
        compiler_params=pltpu.CompilerParams(collective_id=1, has_side_effects=True, vmem_limit_bytes=63 * 2**20), name="factor_solve")(share)

def finish_kernel(np_in, np_out, n_own, w_hbm, blocks, fin0, fin1, fin2, w_out, a_out, s_out, wbuf, gath, cols_s, cols_a, up_s, up_a, isem, lsem, usem, wsem, csem):
    p = lax.axis_index('mp')
    wload = pltpu.make_async_copy(w_hbm, wbuf, isem)
    wload.start()
    sets = [(s_out, cols_s, up_s, np_out, 1), (a_out, cols_a, up_a, np_in, 0)]
    jobs, n = [], 0
    for out, cols, up, n_pan, of_s in sets:
        for q in range(n_pan):
            base = block_at(q, np_in, np_out, of_s) // 2
            low = pltpu.make_async_copy(blocks.at[p, pl.ds(base, n_pan - q)], cols.at[q, pl.ds(q, n_pan - q)], lsem.at[n])
            ups = [pltpu.make_async_copy(blocks.at[par, pl.ds(base + 1, n_pan - 1 - q), p], up.at[par, q, pl.ds(q + 1, n_pan - 1 - q)], usem.at[par, n]) for par in HALVES] if q < n_pan - 1 else []
            send = pltpu.make_async_copy(cols.at[q], out.at[q], csem.at[n])
            jobs.append((low, ups, send, cols, up, q))
            n += 1
    for low, ups, *_ in jobs:
        for c in (*ups, low):
            c.start()
    fins = (fin0, fin1, fin2)
    rows = fins[0].shape[3]
    def tile(t, c):
        part = 0
        while t >= fins[part].shape[3]:
            t -= fins[part].shape[3]
            part += 1
        return fins[part][c[part], c[(part + 1) % 3], c[(part + 2) % 3], t]
    wload.wait()
    for q in range(np_out):
        lo, hi = q * n_own // SUBL, ((q + 1) * n_own - 1) // SUBL
        for half in HALVES:
            def fill(g):
                vals = []
                for x in range(RING):
                    c = (x, lax.rem(g, RING), lax.div(g, RING))
                    v = jnp.concatenate([tile(2 * r + half, c) for r in range(lo, hi + 1)], 0)
                    at = q * n_own - lo * SUBL
                    vals.append(v[at:at + n_own])
                gath[rows_at(g * RING * n_own, RING * n_own)] = jnp.concatenate(vals, 0)
            each(0, RING * RING, fill)
            for b in range(np_in):
                r = slice((2 * q + half) * BW, (2 * q + half + 1) * BW)
                wbuf[b, r] = wbuf[b, r] - LEARN_RATE * gath[b * BW:(b + 1) * BW].T
    wsend = pltpu.make_async_copy(wbuf, w_out, wsem)
    wsend.start()
    for low, ups, send, cols, up, q in jobs:
        low.wait()
        for c in ups:
            c.wait()
    for low, ups, send, cols, up, q in jobs:
        def mirror(q2):
            for par in HALVES:
                cols[q, q2, par] = up[par, q2, q].T
        each(0, q, mirror)
        send.start()
    for low, ups, send, *_ in jobs:
        send.wait()
    wsend.wait()

def finish(w3, blocks, fins, np_in, np_out, n_dp):
    V = pltpu.VMEM
    D = pltpu.SemaphoreType.DMA
    hb = pl.BlockSpec(memory_space=pl.ANY)
    vb = pl.BlockSpec(memory_space=V)
    n_job = np_in + np_out
    square = lambda n: (n, n, 2, BW, BW)
    w_new, a_new, s_new = pl.pallas_call(functools.partial(finish_kernel, np_in, np_out, np_in * BW // n_dp),
        out_shape=(jax.ShapeDtypeStruct(w3.shape, F32), jax.ShapeDtypeStruct(square(np_in), F32), jax.ShapeDtypeStruct(square(np_out), F32)),
        in_specs=[hb, hb, vb, vb, vb], out_specs=(hb, hb, hb),
        scratch_shapes=[V(w3.shape, F32), V((np_in * BW, BW), F32), V(square(np_out), F32), V(square(np_in), F32), V((2, np_out, np_out, BW, BW), F32), V((2, np_in, np_in, BW, BW), F32),
            D, D((n_job,)), D((2, n_job)), D, D((n_job,))],
        compiler_params=pltpu.CompilerParams(vmem_limit_bytes=63 * 2**20), name="outputs")(w3, blocks.reshape(2, -1, 2, BW, BW), *fins)
    return w_new, a_new.reshape(np_in, -1, BW), s_new.reshape(np_out, -1, BW)


def solution(mesh):
    n_dp = mesh.shape['dp']

    def local_step(a_loc, g_loc, w_loc, a_old_loc, s_old_loc):
        np_in = a_loc.shape[1] // PW
        np_out = g_loc.shape[1] // PW
        panels = lambda x: x.transpose(1, 0, 2)
        share = stats(a_loc, g_loc, panels(a_old_loc), panels(s_old_loc))
        blocks, *fins = solve_all(share, np_in, np_out, n_dp, DAMP_SHIFT)
        return tuple(panels(x) for x in finish(panels(w_loc), blocks, fins, np_in, np_out, n_dp))

    spec_rows = P('dp', None)
    spec_cyc = P(None, 'mp', None)
    return jax.shard_map(local_step, mesh=mesh, in_specs=(spec_rows, spec_rows, spec_cyc, spec_cyc, spec_cyc), out_specs=(spec_cyc, spec_cyc, spec_cyc), check_vma=False)
```

```python
import functools
import math
import jax
import jax.numpy as jnp
from jax import lax
from jax.experimental import pallas as pl
from jax.experimental.pallas import tpu as pltpu
from jax.sharding import PartitionSpec as P

BW = 128
PW = 256
RING = 4
SUBL = 8
HALF = 64
ROWS = 32
GROUP = 12
EARLY = 4
PAIR = 2
HALVES = (0, 1)
UPDOWN = (1, 3)
PARTS = (0, 1, 2)
FACTOR_DECAY = 0.95
LEARN_RATE = 1.0
DAMPING = 0.001
DAMP_SHIFT = math.sqrt(DAMPING)
MB = 16
F32 = jnp.float32
BF = jnp.bfloat16
NT = (((1,), (1,)), ((), ()))
NN = (((1,), (0,)), ((), ()))


def split3(x):
    h = x.astype(BF)
    r = x - h.astype(F32)
    m = r.astype(BF)
    return h, m, (r - m.astype(F32)).astype(BF)

def bc(x):
    return jnp.broadcast_to(x, (MB, BW))

def factor_block(mat, linv, beside=None):
    lane = lax.broadcasted_iota(jnp.int32, (MB, BW), 1)
    sub = lax.broadcasted_iota(jnp.int32, (MB, BW), 0)
    odd = lax.rem(sub, PAIR)
    zero = lane.astype(F32) * 0.0
    rows = mat[:MB]
    for t in range(BW // MB):
        k = t * MB
        if beside is not None:
            beside(t)
        cols = jnp.concatenate([bc(rows[:, k + i:k + i + 1]) for i in range(MB)], 0).reshape(MB, MB, BW) + zero
        inside = (lane >= k) & (lane < k + MB)
        ext = jnp.where(inside, jnp.where(lane == sub + k, 1.0, 0.0), rows)
        more = k + MB < BW
        far = k + MB + MB < BW
        if more:
            near = mat[k + MB:k + MB + MB]
            mult = [bc(near[:, k + i:k + i + 1]) for i in range(MB)]
        if far:
            rh, rm, rl = split3(rows)
            left = jnp.concatenate([rh, rh, rm, rh, rl, rm], 0).T[k + MB + MB:]
        dg = of = None
        for j in range(0, MB, PAIR):
            u, v = cols[0], cols[1]
            a, b, c = bc(u[j:j + 1]), bc(u[j + 1:j + 2]), bc(v[j + 1:j + 2])
            det = a * c - b * b
            rdet = 1.0 / det
            ra = 1.0 / a
            e0, e1 = bc(ext[j:j + 1]), bc(ext[j + 1:j + 2])
            linv[k + j:k + j + 1] = (e0 * lax.rsqrt(a))[:1]
            linv[k + j + 1:k + j + 2] = ((e1 - (b * ra) * e0) * lax.rsqrt(det * ra))[:1]
            pair = (sub == j) | (sub == j + 1)
            u, v = jnp.where(pair, 0.0, u), jnp.where(pair, 0.0, v)
            n0, n1 = c * u - b * v, a * v - b * u
            f0, f1 = n0 * rdet, n1 * rdet
            if j + 2 < MB:
                left_cols = cols[2:]
                soon = left_cols[:2]
                soon = soon - (n0 * jnp.broadcast_to(soon[:, j:j + 1], soon.shape) + n1 * jnp.broadcast_to(soon[:, j + 1:j + 2], soon.shape)) * rdet
                if j + 4 < MB:
                    late = left_cols[2:]
                    late = late - (f0 * jnp.broadcast_to(late[:, j:j + 1], late.shape) + f1 * jnp.broadcast_to(late[:, j + 1:j + 2], late.shape))
                    cols = jnp.concatenate([soon, late], 0)
                else:
                    cols = soon
            ext = ext - (f0 * e0 + f1 * e1)
            d_here = jnp.where(odd == 0, c, a) * rdet
            dg = d_here if dg is None else jnp.where(sub >= j, d_here, dg)
            of = b * rdet if of is None else jnp.where(sub >= j, b * rdet, of)
        w = ext * dg - jnp.where(odd == 0, jnp.roll(ext, -1, 0), jnp.roll(ext, 1, 0)) * of
        if far:
            wh, wm, wl = split3(w)
            prod = lax.dot_general(left, jnp.concatenate([wh, wm, wh, wl, wh, wm], 0), NN, preferred_element_type=F32)
            ins = jnp.broadcast_to(inside[:1], prod.shape)
            mat[k + MB + MB:] = jnp.where(ins, 0.0, mat[k + MB + MB:]) - prod
        if more:
            terms = [mult[j] * bc(w[j:j + 1]) for j in range(MB)]
            while len(terms) > 1:
                terms = [x + y for x, y in zip(terms[::2], terms[1::2])]
            rows = jnp.where(inside, 0.0, near) - terms[0]
    ri = lax.broadcasted_iota(jnp.int32, (BW, BW), 0)
    ci = lax.broadcasted_iota(jnp.int32, (BW, BW), 1)
    linv[...] = jnp.where(ci <= ri, linv[...], 0.0)


def dot6(a, b, dims):
    d = lambda x, y: lax.dot_general(x, y, dims, preferred_element_type=F32)
    ah, am, al = a
    bh, bm, bl = b
    return (d(am, bm) + d(ah, bl) + d(al, bh)) + (d(ah, bm) + d(am, bh)) + d(ah, bh)

def stack_dot(x, w, dims):
    xh, xm, xl = x
    wh, wm, wl = w
    k = xh.shape[0]
    d = lambda u, v: lax.dot_general(u, v, dims, preferred_element_type=F32)
    p1 = d(jnp.concatenate([xh, xm, xl], 0), wh)
    p2 = d(jnp.concatenate([xh, xm], 0), wm)
    p3 = d(xh, wl)
    return (p1[k + k:] + p2[k:] + p3) + (p1[k:k + k] + p2[:k]) + p1[:k]

def pieces(ref, at):
    return [ref[z, at] for z in PARTS]

def each(lo, hi, fn):
    def body(i, c):
        fn(i)
        return c
    lax.fori_loop(lo, hi, body, 0)

def upto(n, fn):
    each(0, n, fn)

def rows_at(start, size):
    return pl.ds(pl.multiple_of(start, SUBL), size)

def turn(c, step):
    return lax.rem(c + step, RING)

def place(part, phase):
    stride = RING**((part + phase) % 3)
    return lax.rem(lax.div(lax.axis_index('dp'), stride), RING), stride

def remote(src, dst, ssem, rsem, where):
    return pltpu.make_async_remote_copy(src_ref=src, dst_ref=dst, send_sem=ssem, recv_sem=rsem, device_id=where, device_id_type=pl.DeviceIdType.MESH)

def along(part, phase):
    return place(part, phase)[0]

def chip(part, phase, step):
    c, stride = place(part, phase)
    return {'dp': lax.axis_index('dp') + (turn(c, step) - c) * stride}

def partner():
    return {'mp': 1 - lax.axis_index('mp')}

def entry_barrier():
    sem = pltpu.get_barrier_semaphore()
    where = [chip(part, 0, step + 1) for part in PARTS for step in PARTS] + [partner()]
    for dev in where:
        pl.semaphore_signal(sem, inc=1, device_id=dev, device_id_type=pl.DeviceIdType.MESH)
    pl.semaphore_wait(sem, len(where))

def block_at(q, np_in, np_out, of_s):
    n_in, n_out = PAIR * np_in, PAIR * np_out
    past = min(q // EARLY, 1) if isinstance(q, int) else jnp.minimum(lax.div(q, EARLY), 1)
    in_s = q * n_out - q * (q - 1) + np_in * (np_in + 1) * past
    in_a = EARLY * n_out - EARLY * (EARLY - 1) + q * n_in - q * (q - 1)
    return of_s * in_s + (1 - of_s) * in_a

def decode(b, np_in, np_out):
    n_in, n_out = PAIR * np_in, PAIR * np_out
    at, was = 0, (0, 0)
    row, col = b, 0
    for q, in_s in [(q, 1) for q in range(EARLY)] + [(q, 0) for q in range(np_in)] + [(q, 1) for q in range(EARLY, np_out)]:
        now = (in_s * n_in + PAIR * q - at, in_s * np_in + q)
        hit = (b >= at).astype(jnp.int32)
        row = row + hit * (now[0] - was[0])
        col = col + hit * (now[1] - was[1])
        was = now
        at += in_s * n_out + (1 - in_s) * n_in - PAIR * q
    is_g = (b >= at).astype(jnp.int32)
    off = (b - at) * is_g
    row = row + is_g * (lax.rem(off, n_in) - row)
    col = jnp.minimum(col + is_g * (np_in + lax.div(off, n_in) - col), np_in + np_out - 1)
    in_s = (col >= np_in).astype(jnp.int32)
    old = in_s * ((col - np_in) * n_out + row - n_in) + (1 - in_s) * (col * n_in + row)
    return (1 - is_g) * old, is_g

def front_kernel(np_in, np_out, n_dp, cuts, order, a_hbm, g_hbm, s_hbm, ao_hbm, blocks, quarter, acc, full, agt, own, flip, old, ra, rb, rc, rd, ra2, rb2, rc2, rd2, r3, lsem, ssem, rsem, psem):
    p = lax.axis_index('mp')
    ns = a_hbm.shape[0]
    n_in, n_out = PAIR * np_in, PAIR * np_out
    n_col = np_in + np_out
    n_slot = flip.shape[0]

    def column(i, par):
        src, q = (a_hbm, i) if i < np_in else (g_hbm, i - np_in)
        return src.at[:, pl.ds(pl.multiple_of((PAIR * q + par) * BW, BW), BW)]
    def pair_of(i):
        return (i // PAIR, i % PAIR) if i < np_in else ((np_in + 1) // PAIR + (i - np_in) // PAIR, (i - np_in) % PAIR)
    def mine_at(i):
        z, h = pair_of(i)
        return own.at[z, :, h * BW:(h + 1) * BW]
    mine = [pltpu.make_async_copy(column(i, p), mine_at(i), lsem.at[i]) for i in range(n_col)]
    theirs = [pltpu.make_async_copy(column(i, 1 - p), flip.at[i % n_slot], lsem.at[n_col + i]) for i in range(n_col)]
    of_a = range(block_at(0, np_in, np_out, 0), block_at(np_in, np_in, np_out, 0))
    n_old = block_at(np_out, np_in, np_out, 1)
    mine_rows = [rows_at(along(part, 1) * ROWS + along(part, 2) * SUBL, SUBL) for part in PARTS]
    olds = []
    for j in range(-(-n_old // RING)):
        m, part = divmod(j, 3)
        at, _ = decode(j * RING + along(part, 0), np_in, np_out)
        src = ao_hbm if j * RING in of_a else s_hbm
        olds.append(pltpu.make_async_copy(src.at[at, mine_rows[part]], old.at[m, part], lsem.at[PAIR * n_col + j]))
    for c in theirs[:n_slot] + mine:
        c.start()
    entry_barrier()
    def transpose(src, i, par):
        for kc in range(ns // PW):
            agt[i * (ns // PW) + kc, pl.ds(pl.multiple_of(par * BW, BW), BW), :] = src[kc * PW:(kc + 1) * PW, :].T
    for i in range(n_col):
        theirs[i].wait()
        transpose(flip.at[i % n_slot], i, 1 - p)
        if i + n_slot < n_col:
            theirs[i + n_slot].start()
    for c in olds:
        c.start()
    for i in range(n_col):
        mine[i].wait()
        transpose(mine_at(i), i, p)

    def gram(z, row0, lo, hi, starts, scale):
        n = len(starts)
        rhs = own.at[z, :, :n * BW]
        def some(i):
            lhs = jnp.concatenate([agt[(row0 + i) * (ns // PW) + kc] for kc in range(ns // PW)], 1)
            prod = lax.dot_general(lhs, rhs[...], NN, preferred_element_type=F32) * scale
            for c in reversed(range(n)):
                for h in HALVES:
                    b = starts[c] + PAIR * (i - lo) + h
                    acc[lax.div(b, GROUP), lax.div(lax.rem(b, GROUP), RING), lax.rem(b, RING)] = prod[h * BW:(h + 1) * BW, c * BW:(c + 1) * BW]
        each(lo, hi, some)
    share_of_new = (1.0 - FACTOR_DECAY) / (ns * n_dp)
    n_pair = (np_in + 1) // PAIR
    start_of = lambda q, of_s: block_at(q, np_in, np_out, of_s)
    def grams(of_s, qs):
        n_pan = np_out if of_s else np_in
        for q in qs:
            both = [x for x in (q, q + 1) if x < n_pan]
            gram(n_pair * of_s + q // PAIR, np_in * of_s, q, n_pan, [start_of(x, of_s) - PAIR * (x - q) for x in both], share_of_new)
    def grads(qs):
        base = (np_in + np_out) * (np_in + np_out + 1) - np_out * n_in
        for q in qs:
            both = [x for x in (q, q + 1) if x < np_out]
            gram(n_pair + q // PAIR, 0, 0, np_in, [base + x * n_in for x in both], 1.0 / (ns * n_dp))

    def share(buf, ms, part, phase, coord):
        c1, e = along(part, 0), along(part, 1)
        if phase == 0:
            return buf.at[ms, part, coord]
        return buf.at[ms, part, c1, rows_at(coord * ROWS, ROWS) if phase == 1 else rows_at(e * ROWS + coord * SUBL, SUBL)]
    def cut(buf, ms, part, phase, coord, half):
        if phase == 0:
            return buf.at[ms, part, coord, pl.ds(half * HALF, HALF)]
        return buf.at[ms, part, along(part, 0), rows_at(coord * ROWS + half * MB, MB)]
    firsts = ((ra, rb), (ra2, rb2))
    seconds = ((rc, rd), (rc2, rd2))
    n_copy = 21
    def round_steps(k):
        m0, m1 = cuts[k], cuts[k + 1]
        ms = pl.ds(m0, m1 - m0)
        late = k == len(cuts) - 2
        def copy(part, kind, phase, i):
            c = along(part, phase)
            step = i + 1 if kind == 2 or kind == 3 and phase else UPDOWN[i]
            if kind == 0:
                src, dst = cut(acc, ms, part, phase, turn(c, 2), i), firsts[phase][i].at[ms, part]
            elif kind == 1:
                src, dst = share(acc, ms, part, phase, turn(c, step)), seconds[phase][i].at[ms, part]
            elif kind == 2:
                src, dst = share(acc, ms, part, phase, turn(c, step)), r3.at[i, ms, part]
            else:
                src = share(full, ms, part, phase, c) if kind == 3 else cut(full, ms, part, 0, turn(c, 4 - step), i)
                dst = src
            s = (k * 3 + part) * n_copy + (0, 4, 8, 11, 19)[kind] + (PAIR * phase + i if kind < 2 else 3 * (2 - phase) + i if kind == 3 else i)
            return remote(src, dst, ssem.at[s], rsem.at[s], chip(part, phase, step))
        every, near = PARTS, HALVES
        def go(part, kind, phase, which):
            for i in which:
                copy(part, kind, phase, i).start()
        def come(part, kind, phase, which):
            for i in which:
                copy(part, kind, phase, i).wait_recv()
        def add(part, c1, rows, *srcs):
            def some(m):
                v = acc[m, part, c1, rows]
                for s in srcs:
                    v = v + s(m)
                acc[m, part, c1, rows] = v
            each(m0, m1, some)
        def fold(phase):
            for part in PARTS:
                c = along(part, phase)
                for z in HALVES:
                    come(part, 0, phase, (z,))
                    u = turn(c, UPDOWN[z])
                    buf = firsts[phase][z]
                    if phase == 0:
                        add(part, u, pl.ds(z * HALF, HALF), lambda m: buf[m, part])
                    else:
                        add(part, along(part, 0), rows_at(u * ROWS + z * MB, MB), lambda m: buf[m, part])
                    go(part, 1, phase, (z,))
        def gain(phase):
            for part in PARTS:
                come(part, 1, phase, near)
                b0, b1 = seconds[phase]
                rows = pl.ds(0, BW) if phase == 0 else rows_at(along(part, 1) * ROWS, ROWS)
                add(part, along(part, 0), rows, lambda m: b0[m, part], lambda m: b1[m, part])
                go(part, phase * 2, 1 + phase, every if phase else near)
        def done():
            for part in PARTS:
                come(part, 2, 2, every)
                c1, rows = along(part, 0), mine_rows[part]
                def some(m):
                    v = acc[m, part, c1, rows] + (r3[0, m, part] + r3[1, m, part] + r3[2, m, part])
                    if not late:
                        _, is_g = decode((m * 3 + part) * RING + c1, np_in, np_out)
                        v = v + jnp.where(is_g == 1, 0.0, old[m, part] * FACTOR_DECAY)
                    full[m, part, c1, rows] = v
                each(m0, m1, some)
                go(part, 3, 2, every)
        def widen():
            for part in PARTS:
                come(part, 3, 2, every)
                go(part, 3, 1, every)
        def near_go():
            for part in PARTS:
                come(part, 3, 1, every)
                go(part, 3, 0, near)
        def relay():
            for z in near:
                for part in PARTS:
                    come(part, 3, 0, (z,))
                    go(part, 4, 0, (z,))
        def whole():
            for part in PARTS:
                come(part, 4, 0, near)
                swap(part).start()
                keep(part).start()
        def swap(part):
            return remote(full.at[ms, part], blocks.at[p, ms, part], psem.at[0, k, part], psem.at[1, k, part], partner())
        def keep(part):
            return pltpu.make_async_copy(full.at[ms, part], blocks.at[p, ms, part], psem.at[2, k, part])
        def wide():
            for part in PARTS:
                come(part, 3, 1, every)
                swap_quarter(part).start()
                def some(m):
                    quarter[p, m - m0, part] = full[m, part, along(part, 0)]
                each(m0, m1, some)
        def swap_quarter(part):
            return remote(full.at[ms, part, along(part, 0)], quarter.at[p, :, part], psem.at[0, k, part], psem.at[1, k, part], partner())
        def start():
            for part in PARTS:
                go(part, 0, 0, near)
        kinds = [(0, 0, near), (1, 0, near), (0, 1, near), (1, 1, near), (2, 2, every), (3, 2, every), (3, 1, every), (3, 0, near), (4, 0, near)]
        def settle():
            for part in PARTS:
                for kind, phase, which in kinds[:len(kinds) - PAIR * late]:
                    for i in which:
                        copy(part, kind, phase, i).wait_send()
                c = swap_quarter(part) if late else swap(part)
                c.wait_recv()
                c.wait_send()
                if not late:
                    keep(part).wait()
        return [start, lambda: fold(0), lambda: gain(0), lambda: fold(1), lambda: gain(1), done, widen] + ([wide] if late else [near_go, relay, whole]), settle
    rounds = [round_steps(k) for k in range(len(cuts) - 1)]
    chunks = [lambda: grams(1, (0,)), lambda: (grams(1, (2,)), grams(0, range(0, np_in, PAIR))), lambda: (grams(1, range(EARLY, np_out, PAIR)), grads((0,))), lambda: grads(range(2, np_out, PAIR)),
        lambda: [c.wait() for c in olds]]
    for k, z in order:
        todo = chunks if k < 0 else rounds[k][0]
        if 0 <= z < len(todo):
            todo[z]()
    for _, settle in rounds:
        settle()

def front(a_loc, g_loc, a_old3, s_old3, n_dp, cuts):
    ns, c_in = a_loc.shape
    np_in, np_out = c_in // PW, g_loc.shape[1] // PW
    V = lambda *s: pltpu.VMEM(s, F32)
    B = lambda *s: pltpu.VMEM(s, BF)
    D = lambda *s: pltpu.SemaphoreType.DMA(s)
    hb = pl.BlockSpec(memory_space=pl.ANY)
    vb = pl.BlockSpec(memory_space=pltpu.VMEM)
    nm = cuts[-1]
    order = [(k, x - lag) for x in range(13) for k, lag in ((-1, 0), (0, 0), (1, 3), (2, 3))]
    slab = lambda n: [V(nm, 3, n, BW)] * 2
    n_col = np_in + np_out
    s_blk, a_blk = s_old3.reshape(-1, BW, BW), a_old3.reshape(-1, BW, BW)
    n_old = -(-block_at(np_out, np_in, np_out, 1) // RING)
    f32 = lambda *s: jax.ShapeDtypeStruct(s, F32)
    return pl.pallas_call(functools.partial(front_kernel, np_in, np_out, n_dp, cuts, order),
        out_shape=(f32(2, cuts[-2], 3, RING, BW, BW), f32(2, nm - cuts[-2], 3, BW, BW)),
        in_specs=[hb] * 4, out_specs=(hb, vb),
        scratch_shapes=[*[V(nm, 3, RING, BW, BW)] * 2, B(n_col * ns // PW, PW, PW), B((np_in + 1) // PAIR + (np_out + 1) // PAIR, ns, PW), B(4, ns, BW), V(cuts[-2], 3, SUBL, BW),
            *slab(HALF), *slab(BW), *slab(MB), *slab(ROWS), V(3, nm, 3, SUBL, BW), D(PAIR * n_col + n_old), *[D(63 * (len(cuts) - 1))] * 2, D(3, len(cuts) - 1, 3)],
        compiler_params=pltpu.CompilerParams(collective_id=0, has_side_effects=True, vmem_limit_bytes=67043328), name="front")(a_loc, g_loc, s_blk, a_blk)

def solve_kernel(np_in, np_out, n_dp, damp, cuts, early, quarter, fin, full, tmat, mat, linv, inv_all, lsp, xw, zin, pack, ssem, rsem, psem, osem):
    p = lax.axis_index('mp')
    d = lax.axis_index('dp')
    n_own = np_in * BW // n_dp
    n_in, n_out = PAIR * np_in, PAIR * np_out
    first = [pltpu.make_async_copy(early.at[par], full.at[par, pl.ds(0, cuts[-2])], osem.at[par]) for par in HALVES]
    for c in first:
        c.start()
    entry_barrier()
    ms = pl.ds(cuts[-2], cuts[-1] - cuts[-2])
    def last(par, part, z, on):
        c = along(part, 0)
        ref = full.at[par, ms, part, turn(c, 3 - PAIR * z), pl.ds(z * HALF, HALF)] if on else full.at[par, ms, part, c]
        s = 30 + (par * 3 + part) * 4 + PAIR * on + z
        return remote(ref, ref, ssem.at[s], rsem.at[s], chip(part, 0, UPDOWN[z]))
    every = [(z, part, par) for z in HALVES for part in PARTS for par in HALVES]
    @pl.when(p == 1)
    def _():
        for part in PARTS:
            for par in HALVES:
                def put(m):
                    full[par, m, part, along(part, 0)] = quarter[par, m - cuts[-2], part]
                each(cuts[-2], cuts[-1], put)
        for z, part, par in every:
            last(par, part, z, 0).start()
    for c in first:
        c.wait()

    def block(par, b):
        return full[par, lax.div(b, GROUP), lax.div(lax.rem(b, GROUP), RING), lax.rem(b, RING)]

    base_g = np_out * (np_out + 1) + np_in * (np_in + 1)
    npan = np_out - (np_out - np_in) * p
    eye = jnp.where(lax.broadcasted_iota(jnp.int32, (BW, BW), 0) == lax.broadcasted_iota(jnp.int32, (BW, BW), 1), damp, 0.0)

    def load(q):
        base = block_at(q, np_in, np_out, 1 - p)
        slot = lax.rem(q, PAIR)
        for par in HALVES:
            cols = pl.ds(par * BW, BW)
            def rows(i):
                for h in HALVES:
                    tmat[slot, i, h * BW:(h + 1) * BW, cols] = block(par, base + PAIR * (i - q) + h)
            each(q, npan, rows)
            tmat[slot, q, cols, cols] = tmat[slot, q, cols, cols] + eye

    lsp_spare = lsp.shape[1] - 1
    def ltile(i, k):
        return lax.div(i * (i - 1), PAIR) + k

    def update(i, k, q, ok):
        slot = lax.rem(q, PAIR)
        at = ok * i + (1 - ok) * np_out
        prod = stack_dot(pieces(lsp, ok * ltile(i, k)), pieces(lsp, ok * ltile(q, k)), NT)
        tmat[slot, at] = tmat[slot, at] - prod

    def task(s, q):
        left = jnp.maximum(npan - 1 - q, 1)
        turn = lax.div(s, left)
        ok = (turn <= q).astype(jnp.int32) * jnp.minimum(q, 1) * jnp.minimum(npan - 1 - q, 1)
        k = turn - 1 + q * (1 - jnp.minimum(turn, 1))
        update(q + 1 + lax.rem(s, left), k, q + jnp.minimum(turn, 1), ok)

    load(0)

    def panel(k):
        q = lax.div(k, PAIR)
        h = lax.rem(k, PAIR)
        slot = lax.rem(q, PAIR)
        @pl.when(h == 0)
        def _():
            mat[...] = tmat[slot, q, :BW, :BW]
        factor_block(mat, linv, lambda t: task(h * SUBL + t, q))
        @pl.when(h == 0)
        def _():
            inv0 = linv[...]
            inv0s = split3(inv0)
            l10 = dot6(split3(tmat[slot, q, BW:, :BW]), inv0s, NT)
            l10s = split3(l10)
            mat[...] = tmat[slot, q, BW:, BW:] - dot6(l10s, l10s, NT)
            inv_all[q, :BW, :BW] = inv0
            inv_all[q, :BW, BW:] = jnp.zeros((BW, BW), F32)
            inv_all[q, BW:, :BW] = dot6(l10s, inv0s, NN)
        @pl.when((h == 1) & (q < npan - 1))
        def _():
            each(MB, (npan - 1 - q) * (q + 1), lambda s: task(s, q))
        @pl.when(h == 1)
        def _():
            inv1 = linv[...]
            inv_all[q, BW:, BW:] = inv1
            inv_all[q, BW:, :BW] = -dot6(split3(inv1), split3(inv_all[q, BW:, :BW]), NN)
            invs = split3(inv_all[q])
            def below(s):
                for u in HALVES:
                    i = q + 1 + PAIR * s + u
                    ok = (i < npan).astype(jnp.int32)
                    for z, v in enumerate(split3(stack_dot(split3(tmat[slot, ok * i + (1 - ok) * np_out]), invs, NT))):
                        lsp[z, ok * ltile(i, q) + (1 - ok) * lsp_spare] = v
            upto(lax.div(npan - q, PAIR), below)
        @pl.when((h == 1) & (q < npan - 1))
        def _():
            @pl.when(q == 0)
            def _():
                load(1)
            update(q + 1, q, q + 1, 1)
            @pl.when(q < npan - 2)
            def _():
                load(q + 2)
    upto(PAIR * npan, panel)
    @pl.when(p == 1)
    def _():
        for z, part, par in every:
            last(par, part, z, 0).wait_recv()
            last(par, part, z, 1).start()

    zcopy = remote(zin.at[0], zin.at[1], psem.at[0, 1], psem.at[1, 1], partner())
    @pl.when(p == 1)
    def _():
        row = lax.broadcasted_iota(jnp.int32, (MB, PW), 0)
        lane = lax.broadcasted_iota(jnp.int32, (MB, PW), 1)
        par = lax.div(row, SUBL)
        idx = lax.rem(row, SUBL)
        col = d * n_own + idx
        for q in range(np_in):
            hit = (idx < n_own) & (lax.div(col, BW) == q) & (lane == par * BW + lax.rem(col, BW))
            xw[q] = jnp.where(hit, 1.0, 0.0)
    @pl.when(p == 0)
    def _():
        zcopy.wait_recv()
        def cp(q):
            xw[q] = zin[1, q]
        upto(np_out, cp)

    def spread(x, lo, hi, tile, dims):
        xs = split3(x)
        def some(i):
            for u in range(RING):
                j = lo + RING * i + u
                ok = (j < hi).astype(jnp.int32)
                at = ok * j + (1 - ok) * np_out
                xw[at] = xw[at] - stack_dot(xs, pieces(lsp, ok * tile(j)), dims)
        upto(lax.div(hi - lo + RING - 1, RING), some)
    def fwd(q):
        y = stack_dot(split3(xw[q]), split3(inv_all[q]), NT)
        xw[q] = y
        spread(y, q + 1, npan, lambda j: ltile(j, q), NT)
    upto(npan, fwd)
    def back(s):
        q = npan - 1 - s
        x = stack_dot(split3(xw[q]), split3(inv_all[q]), NN)
        xw[q] = x
        spread(x, 0, q, lambda j: ltile(q, j), NN)
    upto(npan, back)

    xcopy = remote(pack.at[1], pack.at[0], psem.at[0, 2], psem.at[1, 2], partner())
    @pl.when(p == 1)
    def _():
        for z, part, par in every:
            last(par, part, z, 1).wait_recv()
        def zq(q):
            for par in HALVES:
                acc = jnp.zeros((MB, BW), F32)
                for i in range(n_in):
                    acc = acc + stack_dot(split3(xw[i // PAIR, :, (i % PAIR) * BW:(i % PAIR + 1) * BW]), split3(block(par, base_g + q * n_in + i)), NN)
                zin[0, q, :, par * BW:(par + 1) * BW] = acc
        upto(np_out, zq)
        zcopy.start()
        xcopy.wait_recv()
        zcopy.wait_send()
    @pl.when(p == 0)
    def _():
        for par in reversed(HALVES):
            pack[par, np_out * n_own:] = jnp.zeros((pack.shape[1] - np_out * n_own, PW), F32)
            for q in range(np_out):
                pack[par, q * n_own:(q + 1) * n_own] = xw[q, par * SUBL:par * SUBL + n_own]
            if par == 1:
                xcopy.start()
    n_t = fin.shape[4]
    for t in range(PAIR * (pack.shape[1] // SUBL)):
        part, z = divmod(t, n_t)
        half = t % PAIR
        fin[(part, *(along(part, ph) for ph in PARTS), z)] = pack[0, t // PAIR * SUBL:(t // PAIR + 1) * SUBL, half * BW:(half + 1) * BW]
    def fcopy(part, j):
        c1, e, f = (along(part, ph) for ph in PARTS)
        if j < 6:
            phase, step = 2 - j // 3, j % 3 + 1
            ref = fin.at[part, c1, e, f] if phase == 2 else fin.at[part, c1, e]
        else:
            z = j % PAIR
            phase, step = 0, UPDOWN[z]
            ref = fin.at[part, c1] if j < 8 else fin.at[part, turn(c1, 3 - PAIR * z), pl.ds(PAIR * z, 2)]
        s = part * 10 + j
        return remote(ref, ref, ssem.at[s], rsem.at[s], chip(part, phase, step))
    def fstep(came, js):
        def part_fn(part):
            for j in came:
                fcopy(part, j).wait_recv()
            for j in js:
                fcopy(part, j).start()
        for part in PARTS:
            part_fn(part)
    fstep((), (0, 1, 2))
    fstep((0, 1, 2), (3, 4, 5))
    fstep((3, 4, 5), (6, 7))
    def frelay(part):
        for z in HALVES:
            fcopy(part, 6 + z).wait_recv()
            fcopy(part, 8 + z).start()
    for part in PARTS:
        frelay(part)
    fstep((8, 9), ())
    for part in PARTS:
        for j in range(10):
            fcopy(part, j).wait_send()
    @pl.when(p == 1)
    def _():
        for z, part, par in every:
            last(par, part, z, 0).wait_send()
            last(par, part, z, 1).wait_send()
    @pl.when(p == 0)
    def _():
        xcopy.wait_send()

def solve(early, quarter, np_in, np_out, n_dp, damp, cuts):
    n_own = np_in * BW // n_dp
    n_row = -(-np_out * n_own // SUBL)
    n_t = -(-PAIR * n_row // 3)
    n_tile = np_out * (np_out - 1) // PAIR + 1
    V = lambda *s: pltpu.VMEM(s, F32)
    D = lambda *s: pltpu.SemaphoreType.DMA(s)
    hb = pl.BlockSpec(memory_space=pl.ANY)
    vb = pl.BlockSpec(memory_space=pltpu.VMEM)
    f32 = lambda *s: jax.ShapeDtypeStruct(s, F32)
    return pl.pallas_call(functools.partial(solve_kernel, np_in, np_out, n_dp, damp, cuts),
        out_shape=f32(3, RING, RING, RING, n_t, SUBL, BW), in_specs=[hb, vb], out_specs=vb,
        scratch_shapes=[V(2, cuts[-1], 3, RING, BW, BW), V(2, np_out + 1, PW, PW), V(BW, BW), V(BW, BW), V(np_out, PW, PW), pltpu.VMEM((3, n_tile, PW, PW), BF), V(np_out + 1, MB, PW),
            V(2, np_out, MB, PW), V(2, n_row * SUBL, PW), D(54), D(54), D(2, 3), D(2)],
        compiler_params=pltpu.CompilerParams(collective_id=1, has_side_effects=True, vmem_limit_bytes=67043328), name="solve")(early, quarter)

def finish_kernel(np_in, np_out, n_own, w_hbm, blocks, fin, w_out, a_out, s_out, wbuf, gath, cols_s, cols_a, up_s, up_a, isem, lsem, usem, wsem, csem):
    p = lax.axis_index('mp')
    wload = pltpu.make_async_copy(w_hbm, wbuf, isem)
    wload.start()
    sets = [(s_out, cols_s, up_s, np_out, 1), (a_out, cols_a, up_a, np_in, 0)]
    jobs, n = [], 0
    for out, cols, up, n_pan, of_s in sets:
        for q in range(n_pan):
            base = block_at(q, np_in, np_out, of_s) // PAIR
            low = pltpu.make_async_copy(blocks.at[p, pl.ds(base, n_pan - q)], cols.at[q, pl.ds(q, n_pan - q)], lsem.at[n])
            ups = [pltpu.make_async_copy(blocks.at[par, pl.ds(base + 1, n_pan - 1 - q), p], up.at[par, q, pl.ds(q + 1, n_pan - 1 - q)], usem.at[par, n]) for par in HALVES] if q < n_pan - 1 else []
            send = pltpu.make_async_copy(cols.at[q], out.at[q], csem.at[n])
            jobs.append((low, ups, send, cols, up, q))
            n += 1
    for low, ups, *_ in jobs:
        for c in (*ups, low):
            c.start()
    n_t = fin.shape[4]
    def tile(t, c):
        part, z = divmod(t, n_t)
        return fin[(part, *(c + c)[part:part + 3], z)]
    wload.wait()
    def weights(q):
        lo, hi = q * n_own // SUBL, ((q + 1) * n_own - 1) // SUBL
        for half in HALVES:
            def fill(z):
              for y in range(RING):
                vals = []
                for x in range(RING):
                    c = (x, y, z)
                    v = jnp.concatenate([tile(PAIR * r + half, c) for r in range(lo, hi + 1)], 0)
                    at = q * n_own - lo * SUBL
                    vals.append(v[at:at + n_own])
                gath[rows_at((z * RING + y) * RING * n_own, RING * n_own)] = jnp.concatenate(vals, 0)
            upto(RING, fill)
            for b in range(np_in):
                r = slice((PAIR * q + half) * BW, (PAIR * q + half + 1) * BW)
                wbuf[b, r] = wbuf[b, r] - LEARN_RATE * gath[b * BW:(b + 1) * BW].T
    for q in range(np_out // PAIR):
        weights(q)
    for low, ups, send, cols, up, q in jobs:
        low.wait()
        for c in ups:
            c.wait()
    for low, ups, send, cols, up, q in jobs:
        for q2 in range(q):
            for par in HALVES:
                cols[q, q2, par] = up[par, q2, q].T
        send.start()
    for q in range(np_out // PAIR, np_out):
        weights(q)
    wsend = pltpu.make_async_copy(wbuf, w_out, wsem)
    wsend.start()
    for low, ups, send, *_ in jobs:
        send.wait()
    wsend.wait()

def finish(w3, blocks, fin, np_in, np_out, n_dp):
    V = pltpu.VMEM
    D = pltpu.SemaphoreType.DMA
    hb = pl.BlockSpec(memory_space=pl.ANY)
    vb = pl.BlockSpec(memory_space=V)
    n_job = np_in + np_out
    square = lambda n: (n, n, 2, BW, BW)
    w_new, a_new, s_new = pl.pallas_call(functools.partial(finish_kernel, np_in, np_out, np_in * BW // n_dp),
        out_shape=(jax.ShapeDtypeStruct(w3.shape, F32), jax.ShapeDtypeStruct(square(np_in), F32), jax.ShapeDtypeStruct(square(np_out), F32)),
        in_specs=[hb, hb, vb], out_specs=(hb, hb, hb),
        scratch_shapes=[V(w3.shape, F32), V((np_in * BW, BW), F32), V(square(np_out), F32), V(square(np_in), F32), V((2, np_out, np_out, BW, BW), F32), V((2, np_in, np_in, BW, BW), F32),
            D, D((n_job,)), D((2, n_job)), D, D((n_job,))],
        compiler_params=pltpu.CompilerParams(vmem_limit_bytes=63 * 2**20), name="outputs")(w3, blocks.reshape(2, -1, 2, BW, BW), fin)
    return w_new, a_new.reshape(np_in, -1, BW), s_new.reshape(np_out, -1, BW)


def solution(mesh):
    n_dp = mesh.shape['dp']

    def local_step(a_loc, g_loc, w_loc, a_old_loc, s_old_loc):
        np_in = a_loc.shape[1] // PW
        np_out = g_loc.shape[1] // PW
        n_in, n_out = PAIR * np_in, PAIR * np_out
        early = np_in * (np_in + 1) + np_out * (np_out + 1)
        cuts = (0, 2, -(-early // GROUP), (early + n_in * np_out) // GROUP)
        panels = lambda x: x.transpose(1, 0, 2)
        blocks, quarter = front(a_loc, g_loc, panels(a_old_loc), panels(s_old_loc), n_dp, cuts)
        fin = solve(blocks, quarter, np_in, np_out, n_dp, DAMP_SHIFT, cuts)
        return tuple(panels(x) for x in finish(panels(w_loc), blocks, fin, np_in, np_out, n_dp))

    spec_rows = P('dp', None)
    spec_cyc = P(None, 'mp', None)
    return jax.shard_map(local_step, mesh=mesh, in_specs=(spec_rows, spec_rows, spec_cyc, spec_cyc, spec_cyc), out_specs=(spec_cyc, spec_cyc, spec_cyc), check_vma=False)
```

```python
import functools
import math
import jax
import jax.numpy as jnp
from jax import lax
from jax.experimental import pallas as pl
from jax.experimental.pallas import tpu as pltpu
from jax.sharding import PartitionSpec as P

BW = 128
PW = 256
RING = 4
SUBL = 8
HALF = 64
ROWS = 32
GROUP = 12
EARLY = 4
PAIR = 2
HALVES = (0, 1)
UPDOWN = (1, 3)
PARTS = (0, 1, 2)
FACTOR_DECAY = 0.95
LEARN_RATE = 1.0
DAMPING = 0.001
DAMP_SHIFT = math.sqrt(DAMPING)
MB = 16
F32 = jnp.float32
BF = jnp.bfloat16
NT = (((1,), (1,)), ((), ()))
NN = (((1,), (0,)), ((), ()))


def split3(x):
    h = x.astype(BF)
    r = x - h.astype(F32)
    m = r.astype(BF)
    return h, m, (r - m.astype(F32)).astype(BF)

def bc(x):
    return jnp.broadcast_to(x, (MB, BW))

def factor_block(mat, linv, beside=None):
    lane = lax.broadcasted_iota(jnp.int32, (MB, BW), 1)
    sub = lax.broadcasted_iota(jnp.int32, (MB, BW), 0)
    odd = lax.rem(sub, PAIR)
    zero = lane.astype(F32) * 0.0
    rows = mat[:MB]
    for t in range(BW // MB):
        k = t * MB
        if beside is not None:
            beside(t)
        cols = jnp.concatenate([bc(rows[:, k + i:k + i + 1]) for i in range(MB)], 0).reshape(MB, MB, BW) + zero
        inside = (lane >= k) & (lane < k + MB)
        ext = jnp.where(inside, jnp.where(lane == sub + k, 1.0, 0.0), rows)
        more = k + MB < BW
        far = k + MB + MB < BW
        if more:
            near = mat[k + MB:k + MB + MB]
            mult = [bc(near[:, k + i:k + i + 1]) for i in range(MB)]
        if far:
            rh, rm, rl = split3(rows)
            left = jnp.concatenate([rh, rh, rm, rh, rl, rm], 0).T[k + MB + MB:]
        dg = of = None
        for j in range(0, MB, PAIR):
            u, v = cols[0], cols[1]
            a, b, c = bc(u[j:j + 1]), bc(u[j + 1:j + 2]), bc(v[j + 1:j + 2])
            det = a * c - b * b
            rdet = 1.0 / det
            ra = 1.0 / a
            e0, e1 = bc(ext[j:j + 1]), bc(ext[j + 1:j + 2])
            linv[k + j:k + j + 1] = (e0 * lax.rsqrt(a))[:1]
            linv[k + j + 1:k + j + 2] = ((e1 - (b * ra) * e0) * lax.rsqrt(det * ra))[:1]
            pair = (sub == j) | (sub == j + 1)
            u, v = jnp.where(pair, 0.0, u), jnp.where(pair, 0.0, v)
            n0, n1 = c * u - b * v, a * v - b * u
            f0, f1 = n0 * rdet, n1 * rdet
            if j + 2 < MB:
                left_cols = cols[2:]
                soon = left_cols[:2]
                soon = soon - (n0 * jnp.broadcast_to(soon[:, j:j + 1], soon.shape) + n1 * jnp.broadcast_to(soon[:, j + 1:j + 2], soon.shape)) * rdet
                if j + 4 < MB:
                    late = left_cols[2:]
                    late = late - (f0 * jnp.broadcast_to(late[:, j:j + 1], late.shape) + f1 * jnp.broadcast_to(late[:, j + 1:j + 2], late.shape))
                    cols = jnp.concatenate([soon, late], 0)
                else:
                    cols = soon
            ext = ext - (f0 * e0 + f1 * e1)
            d_here = jnp.where(odd == 0, c, a) * rdet
            dg = d_here if dg is None else jnp.where(sub >= j, d_here, dg)
            of = b * rdet if of is None else jnp.where(sub >= j, b * rdet, of)
        w = ext * dg - jnp.where(odd == 0, jnp.roll(ext, -1, 0), jnp.roll(ext, 1, 0)) * of
        if far:
            wh, wm, wl = split3(w)
            prod = lax.dot_general(left, jnp.concatenate([wh, wm, wh, wl, wh, wm], 0), NN, preferred_element_type=F32)
            ins = jnp.broadcast_to(inside[:1], prod.shape)
            mat[k + MB + MB:] = jnp.where(ins, 0.0, mat[k + MB + MB:]) - prod
        if more:
            terms = [mult[j] * bc(w[j:j + 1]) for j in range(MB)]
            while len(terms) > 1:
                terms = [x + y for x, y in zip(terms[::2], terms[1::2])]
            rows = jnp.where(inside, 0.0, near) - terms[0]
    ri = lax.broadcasted_iota(jnp.int32, (BW, BW), 0)
    ci = lax.broadcasted_iota(jnp.int32, (BW, BW), 1)
    linv[...] = jnp.where(ci <= ri, linv[...], 0.0)


def dot6(a, b, dims):
    d = lambda x, y: lax.dot_general(x, y, dims, preferred_element_type=F32)
    ah, am, al = a
    bh, bm, bl = b
    return (d(am, bm) + d(ah, bl) + d(al, bh)) + (d(ah, bm) + d(am, bh)) + d(ah, bh)

def stack_dot(x, w, dims):
    xh, xm, xl = x
    wh, wm, wl = w
    k = xh.shape[0]
    d = lambda u, v: lax.dot_general(u, v, dims, preferred_element_type=F32)
    p1 = d(jnp.concatenate([xh, xm, xl], 0), wh)
    p2 = d(jnp.concatenate([xh, xm], 0), wm)
    p3 = d(xh, wl)
    return (p1[k + k:] + p2[k:] + p3) + (p1[k:k + k] + p2[:k]) + p1[:k]

def pieces(ref, at):
    return [ref[z, at] for z in PARTS]

def each(lo, hi, fn):
    def body(i, c):
        fn(i)
        return c
    lax.fori_loop(lo, hi, body, 0)

def upto(n, fn):
    each(0, n, fn)

def rows_at(start, size):
    return pl.ds(pl.multiple_of(start, SUBL), size)

def turn(c, step):
    return lax.rem(c + step, RING)

def place(part, phase):
    stride = RING**((part + phase) % 3)
    return lax.rem(lax.div(lax.axis_index('dp'), stride), RING), stride

def remote(src, dst, ssem, rsem, where):
    return pltpu.make_async_remote_copy(src_ref=src, dst_ref=dst, send_sem=ssem, recv_sem=rsem, device_id=where, device_id_type=pl.DeviceIdType.MESH)

def along(part, phase):
    return place(part, phase)[0]

def both_ends(sems, *at):
    return sems.at[(0, *at)], sems.at[(1, *at)]

def chip(part, phase, step):
    c, stride = place(part, phase)
    return {'dp': lax.axis_index('dp') + (turn(c, step) - c) * stride}

def partner():
    return {'mp': 1 - lax.axis_index('mp')}

def entry_barrier():
    sem = pltpu.get_barrier_semaphore()
    where = [chip(part, 0, step + 1) for part in PARTS for step in PARTS] + [partner()]
    for dev in where:
        pl.semaphore_signal(sem, inc=1, device_id=dev, device_id_type=pl.DeviceIdType.MESH)
    pl.semaphore_wait(sem, len(where))

def block_at(q, np_in, np_out, of_s):
    n_in, n_out = PAIR * np_in, PAIR * np_out
    past = min(q // EARLY, 1) if isinstance(q, int) else jnp.minimum(lax.div(q, EARLY), 1)
    in_s = q * n_out - q * (q - 1) + np_in * (np_in + 1) * past
    in_a = EARLY * n_out - EARLY * (EARLY - 1) + q * n_in - q * (q - 1)
    return of_s * in_s + (1 - of_s) * in_a

def decode(b, np_in, np_out):
    n_in, n_out = PAIR * np_in, PAIR * np_out
    at, was = 0, (0, 0)
    row, col = b, 0
    for q, in_s in [(q, 1) for q in range(EARLY)] + [(q, 0) for q in range(np_in)] + [(q, 1) for q in range(EARLY, np_out)]:
        now = (in_s * n_in + PAIR * q - at, in_s * np_in + q)
        hit = (b >= at).astype(jnp.int32)
        row = row + hit * (now[0] - was[0])
        col = col + hit * (now[1] - was[1])
        was = now
        at += in_s * n_out + (1 - in_s) * n_in - PAIR * q
    is_g = (b >= at).astype(jnp.int32)
    off = (b - at) * is_g
    row = row + is_g * (lax.rem(off, n_in) - row)
    col = jnp.minimum(col + is_g * (np_in + lax.div(off, n_in) - col), np_in + np_out - 1)
    in_s = (col >= np_in).astype(jnp.int32)
    old = in_s * ((col - np_in) * n_out + row - n_in) + (1 - in_s) * (col * n_in + row)
    return (1 - is_g) * old, is_g

def front_kernel(np_in, np_out, n_dp, cuts, order, a_hbm, g_hbm, s_hbm, ao_hbm, blocks, quarter, acc, full, agt, own, flip, old, ra, rb, rc, rd, ra2, rb2, rc2, rd2, r3, lsem, ssem, rsem, psem):
    p = lax.axis_index('mp')
    ns = a_hbm.shape[0]
    n_in, n_out = PAIR * np_in, PAIR * np_out
    n_col = np_in + np_out
    n_slot = flip.shape[0]

    def column(i, par):
        src, q = (a_hbm, i) if i < np_in else (g_hbm, i - np_in)
        return src.at[:, pl.ds(pl.multiple_of((PAIR * q + par) * BW, BW), BW)]
    def pair_of(i):
        return (i // PAIR, i % PAIR) if i < np_in else ((np_in + 1) // PAIR + (i - np_in) // PAIR, (i - np_in) % PAIR)
    def mine_at(i):
        z, h = pair_of(i)
        return own.at[z, :, h * BW:h * BW + BW]
    mine = [pltpu.make_async_copy(column(i, p), mine_at(i), lsem.at[i]) for i in range(n_col)]
    theirs = [pltpu.make_async_copy(column(i, 1 - p), flip.at[i % n_slot], lsem.at[n_col + i]) for i in range(n_col)]
    of_a = range(block_at(0, np_in, np_out, 0), block_at(np_in, np_in, np_out, 0))
    n_old = block_at(np_out, np_in, np_out, 1)
    mine_rows = [rows_at(along(part, 1) * ROWS + along(part, 2) * SUBL, SUBL) for part in PARTS]
    olds = []
    for j in range(-(-n_old // RING)):
        m, part = divmod(j, 3)
        at, _ = decode(j * RING + along(part, 0), np_in, np_out)
        src = ao_hbm if j * RING in of_a else s_hbm
        olds.append(pltpu.make_async_copy(src.at[at, mine_rows[part]], old.at[m, part], lsem.at[PAIR * n_col + j]))
    for c in theirs[:n_slot] + mine:
        c.start()
    entry_barrier()
    def transpose(src, i, par):
        for kc in range(ns // PW):
            agt[i * (ns // PW) + kc, pl.ds(pl.multiple_of(par * BW, BW), BW), :] = src[kc * PW:kc * PW + PW, :].T
    for i in range(n_col):
        theirs[i].wait()
        transpose(flip.at[i % n_slot], i, 1 - p)
        if i + n_slot < n_col:
            theirs[i + n_slot].start()
    for c in olds:
        c.start()
    for i in range(n_col):
        mine[i].wait()
        transpose(mine_at(i), i, p)

    def gram(z, row0, lo, hi, starts, scale):
        n = len(starts)
        rhs = own.at[z, :, :n * BW]
        def some(i):
            lhs = jnp.concatenate([agt[(row0 + i) * (ns // PW) + kc] for kc in range(ns // PW)], 1)
            prod = lax.dot_general(lhs, rhs[...], NN, preferred_element_type=F32) * scale
            for c in reversed(range(n)):
                for h in HALVES:
                    b = starts[c] + PAIR * (i - lo) + h
                    acc[lax.div(b, GROUP), lax.div(lax.rem(b, GROUP), RING), lax.rem(b, RING)] = prod[h * BW:h * BW + BW, c * BW:c * BW + BW]
        each(lo, hi, some)
    share_of_new = (1.0 - FACTOR_DECAY) / (ns * n_dp)
    n_pair = (np_in + 1) // PAIR
    start_of = lambda q, of_s: block_at(q, np_in, np_out, of_s)
    def grams(of_s, qs):
        n_pan = np_out if of_s else np_in
        for q in qs:
            both = [x for x in (q, q + 1) if x < n_pan]
            gram(n_pair * of_s + q // PAIR, np_in * of_s, q, n_pan, [start_of(x, of_s) - PAIR * (x - q) for x in both], share_of_new)
    def grads(qs):
        base = (np_in + np_out) * (np_in + np_out + 1) - np_out * n_in
        for q in qs:
            both = [x for x in (q, q + 1) if x < np_out]
            gram(n_pair + q // PAIR, 0, 0, np_in, [base + x * n_in for x in both], 1.0 / (ns * n_dp))

    def share(buf, ms, part, phase, coord):
        c1, e = along(part, 0), along(part, 1)
        if phase == 0:
            return buf.at[ms, part, coord]
        return buf.at[ms, part, c1, rows_at(coord * ROWS, ROWS) if phase == 1 else rows_at(e * ROWS + coord * SUBL, SUBL)]
    def cut(buf, ms, part, phase, coord, half):
        if phase == 0:
            return buf.at[ms, part, coord, pl.ds(half * HALF, HALF)]
        return buf.at[ms, part, along(part, 0), rows_at(coord * ROWS + half * MB, MB)]
    firsts = ((ra, rb), (ra2, rb2))
    seconds = ((rc, rd), (rc2, rd2))
    n_copy = 23
    def round_steps(k):
        m0, m1 = cuts[k], cuts[k + 1]
        ms = pl.ds(m0, m1 - m0)
        late = k == len(cuts) - 2
        def copy(part, kind, phase, i):
            c = along(part, phase)
            step = i + 1 if kind == 2 or kind == 3 and phase == 2 else UPDOWN[i]
            if kind == 0:
                src, dst = cut(acc, ms, part, phase, turn(c, 2), i), firsts[phase][i].at[ms, part]
            elif kind == 1:
                src, dst = share(acc, ms, part, phase, turn(c, step)), seconds[phase][i].at[ms, part]
            elif kind == 2:
                src, dst = share(acc, ms, part, phase, turn(c, step)), r3.at[i, ms, part]
            else:
                src = share(full, ms, part, phase, c) if kind == 3 else cut(full, ms, part, phase, turn(c, 4 - step), i)
                dst = src
            s = (k * 3 + part) * n_copy + (0, 4, 8, 11, 19)[kind] + (PAIR * phase + i if kind < 2 or kind == 4 else 3 * (2 - phase) + i if kind == 3 else i)
            return remote(src, dst, ssem.at[s], rsem.at[s], chip(part, phase, step))
        every, near = PARTS, HALVES
        def go(part, kind, phase, which):
            for i in which:
                copy(part, kind, phase, i).start()
        def come(part, kind, phase, which):
            for i in which:
                copy(part, kind, phase, i).wait_recv()
        def add(part, c1, rows, *srcs):
            def some(m):
                v = acc[m, part, c1, rows]
                for s in srcs:
                    v = v + s(m)
                acc[m, part, c1, rows] = v
            each(m0, m1, some)
        def fold(phase):
            for part in PARTS:
                c = along(part, phase)
                for z in HALVES:
                    come(part, 0, phase, (z,))
                    u = turn(c, UPDOWN[z])
                    buf = firsts[phase][z]
                    if phase == 0:
                        add(part, u, pl.ds(z * HALF, HALF), lambda m: buf[m, part])
                    else:
                        add(part, along(part, 0), rows_at(u * ROWS + z * MB, MB), lambda m: buf[m, part])
                    go(part, 1, phase, (z,))
        def gain(phase):
            for part in PARTS:
                come(part, 1, phase, near)
                b0, b1 = seconds[phase]
                rows = pl.ds(0, BW) if phase == 0 else rows_at(along(part, 1) * ROWS, ROWS)
                add(part, along(part, 0), rows, lambda m: b0[m, part], lambda m: b1[m, part])
                go(part, phase * 2, 1 + phase, every if phase else near)
        def done():
            for part in PARTS:
                come(part, 2, 2, every)
                c1, rows = along(part, 0), mine_rows[part]
                def some(m):
                    v = acc[m, part, c1, rows] + (r3[0, m, part] + r3[1, m, part] + r3[2, m, part])
                    if not late:
                        _, is_g = decode((m * 3 + part) * RING + c1, np_in, np_out)
                        v = v + jnp.where(is_g == 1, 0.0, old[m, part] * FACTOR_DECAY)
                    full[m, part, c1, rows] = v
                each(m0, m1, some)
                go(part, 3, 2, every)
        def widen():
            for part in PARTS:
                come(part, 3, 2, every)
                go(part, 3, 1, near)
        def relay_wide():
            for z in near:
                for part in PARTS:
                    come(part, 3, 1, (z,))
                    go(part, 4, 1, (z,))
        def near_go():
            for part in PARTS:
                come(part, 4, 1, near)
                go(part, 3, 0, near)
        def relay():
            for z in near:
                for part in PARTS:
                    come(part, 3, 0, (z,))
                    go(part, 4, 0, (z,))
        def whole():
            for part in PARTS:
                come(part, 4, 0, near)
                swap(part).start()
                keep(part).start()
        def swap(part):
            return remote(full.at[ms, part], blocks.at[p, ms, part], *both_ends(psem, k, part), partner())
        def keep(part):
            return pltpu.make_async_copy(full.at[ms, part], blocks.at[p, ms, part], psem.at[2, k, part])
        def wide():
            for part in PARTS:
                come(part, 4, 1, near)
                swap_quarter(part).start()
                def some(m):
                    quarter[p, m - m0, part] = full[m, part, along(part, 0)]
                each(m0, m1, some)
        def swap_quarter(part):
            return remote(full.at[ms, part, along(part, 0)], quarter.at[p, :, part], *both_ends(psem, k, part), partner())
        def start():
            for part in PARTS:
                go(part, 0, 0, near)
        kinds = [(0, 0, near), (1, 0, near), (0, 1, near), (1, 1, near), (2, 2, every), (3, 2, every), (3, 1, near), (4, 1, near), (3, 0, near), (4, 0, near)]
        def settle():
            for part in PARTS:
                for kind, phase, which in kinds[:len(kinds) - PAIR * late]:
                    for i in which:
                        copy(part, kind, phase, i).wait_send()
                c = swap_quarter(part) if late else swap(part)
                c.wait_recv()
                c.wait_send()
                if not late:
                    keep(part).wait()
        return [start, lambda: fold(0), lambda: gain(0), lambda: fold(1), lambda: gain(1), done, widen, relay_wide] + ([wide] if late else [near_go, relay, whole]), settle
    rounds = [round_steps(k) for k in range(len(cuts) - 1)]
    chunks = [lambda: grams(1, (0,)), lambda: (grams(1, (2,)), grams(0, range(0, np_in, PAIR))), lambda: (grams(1, range(EARLY, np_out, PAIR)), grads((0,))),
        lambda: (grads(range(2, np_out, PAIR)), [c.wait() for c in olds])]
    for k, z in order:
        todo = chunks if k < 0 else rounds[k][0]
        if 0 <= z < len(todo):
            todo[z]()
    for _, settle in rounds:
        settle()

def front(a_loc, g_loc, a_old3, s_old3, n_dp, cuts):
    ns, c_in = a_loc.shape
    np_in, np_out = c_in // PW, g_loc.shape[1] // PW
    V = lambda *s: pltpu.VMEM(s, F32)
    B = lambda *s: pltpu.VMEM(s, BF)
    D = lambda *s: pltpu.SemaphoreType.DMA(s)
    hb = pl.BlockSpec(memory_space=pl.ANY)
    vb = pl.BlockSpec(memory_space=pltpu.VMEM)
    nm = cuts[-1]
    order = [(k, x - lag) for x in range(15) for k, lag in ((-1, 0), (0, 0), (1, 2), (2, 3))]
    slab = lambda n: [V(nm, 3, n, BW)] * 2
    n_col = np_in + np_out
    s_blk, a_blk = s_old3.reshape(-1, BW, BW), a_old3.reshape(-1, BW, BW)
    n_old = -(-block_at(np_out, np_in, np_out, 1) // RING)
    f32 = lambda *s: jax.ShapeDtypeStruct(s, F32)
    return pl.pallas_call(functools.partial(front_kernel, np_in, np_out, n_dp, cuts, order),
        out_shape=(f32(2, cuts[-2], 3, RING, BW, BW), f32(2, nm - cuts[-2], 3, BW, BW)),
        in_specs=[hb] * 4, out_specs=(hb, vb),
        scratch_shapes=[*[V(nm, 3, RING, BW, BW)] * 2, B(n_col * ns // PW, PW, PW), B((np_in + 1) // PAIR + (np_out + 1) // PAIR, ns, PW), B(4, ns, BW), V(cuts[-2], 3, SUBL, BW),
            *slab(HALF), *slab(BW), *slab(MB), *slab(ROWS), V(3, nm, 3, SUBL, BW), D(PAIR * n_col + n_old), *[D(69 * (len(cuts) - 1))] * 2, D(3, len(cuts) - 1, 3)],
        compiler_params=pltpu.CompilerParams(collective_id=0, has_side_effects=True, vmem_limit_bytes=67043328), name="front")(a_loc, g_loc, s_blk, a_blk)

def solve_kernel(np_in, np_out, n_dp, damp, cuts, early, quarter, fin, full, tmat, mat, linv, inv_all, lsp, xw, zin, pack, ssem, rsem, psem, osem):
    p = lax.axis_index('mp')
    d = lax.axis_index('dp')
    n_own = np_in * BW // n_dp
    n_in, n_out = PAIR * np_in, PAIR * np_out
    first, then = [[pltpu.make_async_copy(early.at[par, pl.ds(cuts[z], cuts[z + 1] - cuts[z])], full.at[par, pl.ds(cuts[z], cuts[z + 1] - cuts[z])], osem.at[z, par]) for par in HALVES] for z in HALVES]
    for c in first + then:
        c.start()
    entry_barrier()
    ms = pl.ds(cuts[-2], cuts[-1] - cuts[-2])
    def last(par, part, z, on):
        c = along(part, 0)
        ref = full.at[par, ms, part, turn(c, 3 - PAIR * z), pl.ds(z * HALF, HALF)] if on else full.at[par, ms, part, c]
        s = 30 + (par * 3 + part) * 4 + PAIR * on + z
        return remote(ref, ref, ssem.at[s], rsem.at[s], chip(part, 0, UPDOWN[z]))
    every = [(z, part, par) for z in HALVES for part in PARTS for par in HALVES]
    @pl.when(p == 1)
    def _():
        for part in PARTS:
            for par in HALVES:
                def put(m):
                    full[par, m, part, along(part, 0)] = quarter[par, m - cuts[-2], part]
                each(cuts[-2], cuts[-1], put)
        for z, part, par in every:
            last(par, part, z, 0).start()
    def wait_for(copies):
        for c in copies:
            c.wait()
    wait_for(first)
    @pl.when(p == 1)
    def _():
        wait_for(then)

    def block(par, b):
        return full[par, lax.div(b, GROUP), lax.div(lax.rem(b, GROUP), RING), lax.rem(b, RING)]

    base_g = np_out * (np_out + 1) + np_in * (np_in + 1)
    npan = np_out - (np_out - np_in) * p
    eye = jnp.where(lax.broadcasted_iota(jnp.int32, (BW, BW), 0) == lax.broadcasted_iota(jnp.int32, (BW, BW), 1), damp, 0.0)

    def load(q):
        base = block_at(q, np_in, np_out, 1 - p)
        slot = lax.rem(q, PAIR)
        for par in HALVES:
            cols = pl.ds(par * BW, BW)
            def rows(i):
                for h in HALVES:
                    tmat[slot, i, h * BW:h * BW + BW, cols] = block(par, base + PAIR * (i - q) + h)
            each(q, npan, rows)
            tmat[slot, q, cols, cols] = tmat[slot, q, cols, cols] + eye

    lsp_spare = lsp.shape[1] - 1
    def ltile(i, k):
        return lax.div(i * (i - 1), PAIR) + k

    def update(i, k, q, ok):
        slot = lax.rem(q, PAIR)
        at = ok * i + (1 - ok) * np_out
        prod = stack_dot(pieces(lsp, ok * ltile(i, k)), pieces(lsp, ok * ltile(q, k)), NT)
        tmat[slot, at] = tmat[slot, at] - prod

    def task(s, q):
        left = jnp.maximum(npan - 1 - q, 1)
        turn = lax.div(s, left)
        ok = (turn <= q).astype(jnp.int32) * jnp.minimum(q, 1) * jnp.minimum(npan - 1 - q, 1)
        k = turn - 1 + q * (1 - jnp.minimum(turn, 1))
        update(q + 1 + lax.rem(s, left), k, q + jnp.minimum(turn, 1), ok)

    load(0)

    def panel(k):
        q = lax.div(k, PAIR)
        h = lax.rem(k, PAIR)
        slot = lax.rem(q, PAIR)
        @pl.when(h == 0)
        def _():
            mat[...] = tmat[slot, q, :BW, :BW]
        factor_block(mat, linv, lambda t: task(h * SUBL + t, q))
        @pl.when(h == 0)
        def _():
            inv0 = linv[...]
            inv0s = split3(inv0)
            l10 = dot6(split3(tmat[slot, q, BW:, :BW]), inv0s, NT)
            l10s = split3(l10)
            mat[...] = tmat[slot, q, BW:, BW:] - dot6(l10s, l10s, NT)
            inv_all[q, :BW, :BW] = inv0
            inv_all[q, :BW, BW:] = jnp.zeros((BW, BW), F32)
            inv_all[q, BW:, :BW] = dot6(l10s, inv0s, NN)
        @pl.when((h == 1) & (q < npan - 1))
        def _():
            each(MB, (npan - 1 - q) * (q + 1), lambda s: task(s, q))
        @pl.when(h == 1)
        def _():
            inv1 = linv[...]
            inv_all[q, BW:, BW:] = inv1
            inv_all[q, BW:, :BW] = -dot6(split3(inv1), split3(inv_all[q, BW:, :BW]), NN)
            invs = split3(inv_all[q])
            def below(s):
                i = q + 1 + PAIR * s
                ok = (i + 1 < npan).astype(jnp.int32)
                both = jnp.concatenate([tmat[slot, i], tmat[slot, ok * (i + 1) + (1 - ok) * np_out]], 0)
                for z, v in enumerate(split3(stack_dot(split3(both), invs, NT))):
                    lsp[z, ltile(i, q)] = v[:PW]
                    lsp[z, ok * ltile(i + 1, q) + (1 - ok) * lsp_spare] = v[PW:]
            upto(lax.div(npan - q, PAIR), below)
        @pl.when((h == 1) & (q < npan - 1))
        def _():
            @pl.when(q == 0)
            def _():
                load(1)
            update(q + 1, q, q + 1, 1)
            @pl.when(q < npan - 2)
            def _():
                load(q + 2)
    upto(1, panel)
    @pl.when(p == 0)
    def _():
        wait_for(then)
    each(1, PAIR * npan, panel)
    @pl.when(p == 1)
    def _():
        for z, part, par in every:
            last(par, part, z, 0).wait_recv()
            last(par, part, z, 1).start()

    zcopy = remote(zin.at[0], zin.at[1], *both_ends(psem, 1), partner())
    @pl.when(p == 1)
    def _():
        row = lax.broadcasted_iota(jnp.int32, (MB, PW), 0)
        lane = lax.broadcasted_iota(jnp.int32, (MB, PW), 1)
        par = lax.div(row, SUBL)
        idx = lax.rem(row, SUBL)
        col = d * n_own + idx
        for q in range(np_in):
            hit = (idx < n_own) & (lax.div(col, BW) == q) & (lane == par * BW + lax.rem(col, BW))
            xw[q] = jnp.where(hit, 1.0, 0.0)
    @pl.when(p == 0)
    def _():
        zcopy.wait_recv()
        def cp(q):
            xw[q] = zin[1, q]
        upto(np_out, cp)

    def spread(x, lo, hi, tile, dims):
        xs = split3(x)
        def some(i):
            for u in range(RING):
                j = lo + RING * i + u
                ok = (j < hi).astype(jnp.int32)
                at = ok * j + (1 - ok) * np_out
                xw[at] = xw[at] - stack_dot(xs, pieces(lsp, ok * tile(j)), dims)
        upto(lax.div(hi - lo + RING - 1, RING), some)
    def fwd(q):
        y = stack_dot(split3(xw[q]), split3(inv_all[q]), NT)
        xw[q] = y
        spread(y, q + 1, npan, lambda j: ltile(j, q), NT)
    upto(npan, fwd)
    def back(s):
        q = npan - 1 - s
        x = stack_dot(split3(xw[q]), split3(inv_all[q]), NN)
        xw[q] = x
        spread(x, 0, q, lambda j: ltile(q, j), NN)
    upto(npan, back)

    xcopy = remote(pack.at[1], pack.at[0], *both_ends(psem, 2), partner())
    @pl.when(p == 1)
    def _():
        for z, part, par in every:
            last(par, part, z, 1).wait_recv()
        def zq(q):
            for par in HALVES:
                acc = jnp.zeros((MB, BW), F32)
                for i in range(n_in):
                    acc = acc + stack_dot(split3(xw[i // PAIR, :, (i % PAIR) * BW:(i % PAIR + 1) * BW]), split3(block(par, base_g + q * n_in + i)), NN)
                zin[0, q, :, par * BW:par * BW + BW] = acc
        upto(np_out, zq)
        zcopy.start()
        xcopy.wait_recv()
        zcopy.wait_send()
    @pl.when(p == 0)
    def _():
        for par in reversed(HALVES):
            pack[par, np_out * n_own:] = jnp.zeros((pack.shape[1] - np_out * n_own, PW), F32)
            for q in range(np_out):
                pack[par, q * n_own:(q + 1) * n_own] = xw[q, par * SUBL:par * SUBL + n_own]
            if par == 1:
                xcopy.start()
    n_t = fin.shape[4]
    for t in range(PAIR * (pack.shape[1] // SUBL)):
        part, z = divmod(t, n_t)
        half = t % PAIR
        fin[(part, *(along(part, ph) for ph in PARTS), z)] = pack[0, t // PAIR * SUBL:t // PAIR * SUBL + SUBL, half * BW:half * BW + BW]
    def fcopy(part, j):
        c1, e, f = (along(part, ph) for ph in PARTS)
        if j < 6:
            phase, step = 2 - j // 3, j % 3 + 1
            ref = fin.at[part, c1, e, f] if phase == 2 else fin.at[part, c1, e]
        else:
            z = j % PAIR
            phase, step = 0, UPDOWN[z]
            ref = fin.at[part, c1] if j < 8 else fin.at[part, turn(c1, 3 - PAIR * z), pl.ds(PAIR * z, 2)]
        s = part * 10 + j
        return remote(ref, ref, ssem.at[s], rsem.at[s], chip(part, phase, step))
    def fstep(came, js):
        def part_fn(part):
            for j in came:
                fcopy(part, j).wait_recv()
            for j in js:
                fcopy(part, j).start()
        for part in PARTS:
            part_fn(part)
    fstep((), (0, 1, 2))
    fstep((0, 1, 2), (3, 4, 5))
    fstep((3, 4, 5), (6, 7))
    def frelay(part):
        for z in HALVES:
            fcopy(part, 6 + z).wait_recv()
            fcopy(part, 8 + z).start()
    for part in PARTS:
        frelay(part)
    fstep((8, 9), ())
    for part in PARTS:
        for j in range(10):
            fcopy(part, j).wait_send()
    @pl.when(p == 1)
    def _():
        for z, part, par in every:
            last(par, part, z, 0).wait_send()
            last(par, part, z, 1).wait_send()
    @pl.when(p == 0)
    def _():
        xcopy.wait_send()

def solve(early, quarter, np_in, np_out, n_dp, damp, cuts):
    n_own = np_in * BW // n_dp
    n_row = -(-np_out * n_own // SUBL)
    n_t = -(-PAIR * n_row // 3)
    n_tile = np_out * (np_out - 1) // PAIR + 1
    V = lambda *s: pltpu.VMEM(s, F32)
    D = lambda *s: pltpu.SemaphoreType.DMA(s)
    hb = pl.BlockSpec(memory_space=pl.ANY)
    vb = pl.BlockSpec(memory_space=pltpu.VMEM)
    f32 = lambda *s: jax.ShapeDtypeStruct(s, F32)
    return pl.pallas_call(functools.partial(solve_kernel, np_in, np_out, n_dp, damp, cuts),
        out_shape=f32(3, RING, RING, RING, n_t, SUBL, BW), in_specs=[hb, vb], out_specs=vb,
        scratch_shapes=[V(2, cuts[-1], 3, RING, BW, BW), V(2, np_out + 1, PW, PW), V(BW, BW), V(BW, BW), V(np_out, PW, PW), pltpu.VMEM((3, n_tile, PW, PW), BF), V(np_out + 1, MB, PW),
            V(2, np_out, MB, PW), V(2, n_row * SUBL, PW), D(54), D(54), D(2, 3), D(2, 2)],
        compiler_params=pltpu.CompilerParams(collective_id=1, has_side_effects=True, vmem_limit_bytes=67043328), name="solve")(early, quarter)

def finish_kernel(np_in, np_out, n_own, w_hbm, blocks, fin, w_out, a_out, s_out, wbuf, gath, cols_s, cols_a, up_s, up_a, isem, lsem, usem, wsem, csem):
    p = lax.axis_index('mp')
    wload = pltpu.make_async_copy(w_hbm, wbuf, isem)
    wload.start()
    sets = [(s_out, cols_s, up_s, np_out, 1), (a_out, cols_a, up_a, np_in, 0)]
    jobs, n = [], 0
    for out, cols, up, n_pan, of_s in sets:
        for q in range(n_pan):
            base = block_at(q, np_in, np_out, of_s) // PAIR
            low = pltpu.make_async_copy(blocks.at[p, pl.ds(base, n_pan - q)], cols.at[q, pl.ds(q, n_pan - q)], lsem.at[n])
            ups = [pltpu.make_async_copy(blocks.at[par, pl.ds(base + 1, n_pan - 1 - q), p], up.at[par, q, pl.ds(q + 1, n_pan - 1 - q)], usem.at[par, n]) for par in HALVES] if q < n_pan - 1 else []
            send = pltpu.make_async_copy(cols.at[q], out.at[q], csem.at[n])
            jobs.append((low, ups, send, cols, up, q))
            n += 1
    for low, ups, *_ in jobs:
        for c in (*ups, low):
            c.start()
    n_t = fin.shape[4]
    def tile(t, c):
        part, z = divmod(t, n_t)
        return fin[(part, *(c + c)[part:part + 3], z)]
    wload.wait()
    def weights(q):
        lo, hi = q * n_own // SUBL, ((q + 1) * n_own - 1) // SUBL
        for half in HALVES:
            def fill(z):
              for y in range(RING):
                vals = []
                for x in range(RING):
                    c = (x, y, z)
                    v = jnp.concatenate([tile(PAIR * r + half, c) for r in range(lo, hi + 1)], 0)
                    at = q * n_own - lo * SUBL
                    vals.append(v[at:at + n_own])
                gath[rows_at((z * RING + y) * RING * n_own, RING * n_own)] = jnp.concatenate(vals, 0)
            upto(RING, fill)
            for b in range(np_in):
                r = slice((PAIR * q + half) * BW, (PAIR * q + half + 1) * BW)
                wbuf[b, r] = wbuf[b, r] - LEARN_RATE * gath[b * BW:b * BW + BW].T
    for q in range(np_out // PAIR):
        weights(q)
    for low, ups, send, cols, up, q in jobs:
        low.wait()
        for c in ups:
            c.wait()
    for low, ups, send, cols, up, q in jobs:
        for q2 in range(q):
            for par in HALVES:
                cols[q, q2, par] = up[par, q2, q].T
        send.start()
    for q in range(np_out // PAIR, np_out):
        weights(q)
    wsend = pltpu.make_async_copy(wbuf, w_out, wsem)
    wsend.start()
    for low, ups, send, *_ in jobs:
        send.wait()
    wsend.wait()

def finish(w3, blocks, fin, np_in, np_out, n_dp):
    V = pltpu.VMEM
    D = pltpu.SemaphoreType.DMA
    hb = pl.BlockSpec(memory_space=pl.ANY)
    vb = pl.BlockSpec(memory_space=V)
    n_job = np_in + np_out
    square = lambda n: (n, n, 2, BW, BW)
    w_new, a_new, s_new = pl.pallas_call(functools.partial(finish_kernel, np_in, np_out, np_in * BW // n_dp),
        out_shape=(jax.ShapeDtypeStruct(w3.shape, F32), jax.ShapeDtypeStruct(square(np_in), F32), jax.ShapeDtypeStruct(square(np_out), F32)),
        in_specs=[hb, hb, vb], out_specs=(hb, hb, hb),
        scratch_shapes=[V(w3.shape, F32), V((np_in * BW, BW), F32), V(square(np_out), F32), V(square(np_in), F32), V((2, np_out, np_out, BW, BW), F32), V((2, np_in, np_in, BW, BW), F32),
            D, D((n_job,)), D((2, n_job)), D, D((n_job,))],
        compiler_params=pltpu.CompilerParams(vmem_limit_bytes=63 * 2**20), name="outputs")(w3, blocks.reshape(2, -1, 2, BW, BW), fin)
    return w_new, a_new.reshape(np_in, -1, BW), s_new.reshape(np_out, -1, BW)


def solution(mesh):
    n_dp = mesh.shape['dp']

    def local_step(a_loc, g_loc, w_loc, a_old_loc, s_old_loc):
        np_in = a_loc.shape[1] // PW
        np_out = g_loc.shape[1] // PW
        n_in, n_out = PAIR * np_in, PAIR * np_out
        early = np_in * (np_in + 1) + np_out * (np_out + 1)
        cuts = (0, 2, -(-early // GROUP), (early + n_in * np_out) // GROUP)
        panels = lambda x: x.transpose(1, 0, 2)
        blocks, quarter = front(a_loc, g_loc, panels(a_old_loc), panels(s_old_loc), n_dp, cuts)
        fin = solve(blocks, quarter, np_in, np_out, n_dp, DAMP_SHIFT, cuts)
        return tuple(panels(x) for x in finish(panels(w_loc), blocks, fin, np_in, np_out, n_dp))

    spec_rows = P('dp', None)
    spec_cyc = P(None, 'mp', None)
    return jax.shard_map(local_step, mesh=mesh, in_specs=(spec_rows, spec_rows, spec_cyc, spec_cyc, spec_cyc), out_specs=(spec_cyc, spec_cyc, spec_cyc), check_vma=False)
```

```python
import functools
import math
import jax
import jax.numpy as jnp
from jax import lax
from jax.experimental import pallas as pl
from jax.experimental.pallas import tpu as pltpu
from jax.sharding import PartitionSpec as P

BW = 128
PW = 256
RING = 4
SUBL = 8
HALF = 64
ROWS = 32
GROUP = 12
EARLY = 4
PAIR = 2
HALVES = (0, 1)
UPDOWN = (1, 3)
PARTS = (0, 1, 2)
FACTOR_DECAY = 0.95
LEARN_RATE = 1.0
DAMPING = 0.001
DAMP_SHIFT = math.sqrt(DAMPING)
MB = 16
F32 = jnp.float32
BF = jnp.bfloat16
NT = (((1,), (1,)), ((), ()))
NN = (((1,), (0,)), ((), ()))


def split3(x):
    h = x.astype(BF)
    r = x - h.astype(F32)
    m = r.astype(BF)
    return h, m, (r - m.astype(F32)).astype(BF)

def bc(x):
    return jnp.broadcast_to(x, (MB, BW))

def factor_block(mat, linv, beside=None):
    lane = lax.broadcasted_iota(jnp.int32, (MB, BW), 1)
    sub = lax.broadcasted_iota(jnp.int32, (MB, BW), 0)
    odd = lax.rem(sub, PAIR)
    zero = lane.astype(F32) * 0.0
    rows = mat[:MB]
    for t in range(BW // MB):
        k = t * MB
        if beside is not None:
            beside(t)
        cols = jnp.concatenate([bc(rows[:, k + i:k + i + 1]) for i in range(MB)], 0).reshape(MB, MB, BW) + zero
        inside = (lane >= k) & (lane < k + MB)
        ext = jnp.where(inside, jnp.where(lane == sub + k, 1.0, 0.0), rows)
        more = k + MB < BW
        far = k + MB + MB < BW
        if more:
            near = mat[k + MB:k + MB + MB]
            mult = [bc(near[:, k + i:k + i + 1]) for i in range(MB)]
        if far:
            rh, rm, rl = split3(rows)
            left = jnp.concatenate([rh, rh, rm, rh, rl, rm], 0).T[k + MB + MB:]
        dg = of = None
        for j in range(0, MB, PAIR):
            u, v = cols[0], cols[1]
            a, b, c = bc(u[j:j + 1]), bc(u[j + 1:j + 2]), bc(v[j + 1:j + 2])
            det = a * c - b * b
            rdet = 1.0 / det
            ra = 1.0 / a
            e0, e1 = bc(ext[j:j + 1]), bc(ext[j + 1:j + 2])
            linv[k + j:k + j + 1] = (e0 * lax.rsqrt(a))[:1]
            linv[k + j + 1:k + j + 2] = ((e1 - (b * ra) * e0) * lax.rsqrt(det * ra))[:1]
            pair = (sub == j) | (sub == j + 1)
            u, v = jnp.where(pair, 0.0, u), jnp.where(pair, 0.0, v)
            n0, n1 = c * u - b * v, a * v - b * u
            f0, f1 = n0 * rdet, n1 * rdet
            if j + 2 < MB:
                left_cols = cols[2:]
                soon = left_cols[:2]
                soon = soon - (n0 * jnp.broadcast_to(soon[:, j:j + 1], soon.shape) + n1 * jnp.broadcast_to(soon[:, j + 1:j + 2], soon.shape)) * rdet
                if j + 4 < MB:
                    late = left_cols[2:]
                    late = late - (f0 * jnp.broadcast_to(late[:, j:j + 1], late.shape) + f1 * jnp.broadcast_to(late[:, j + 1:j + 2], late.shape))
                    cols = jnp.concatenate([soon, late], 0)
                else:
                    cols = soon
            ext = ext - (f0 * e0 + f1 * e1)
            d_here = jnp.where(odd == 0, c, a) * rdet
            dg = d_here if dg is None else jnp.where(sub >= j, d_here, dg)
            of = b * rdet if of is None else jnp.where(sub >= j, b * rdet, of)
        w = ext * dg - jnp.where(odd == 0, jnp.roll(ext, -1, 0), jnp.roll(ext, 1, 0)) * of
        if far:
            wh, wm, wl = split3(w)
            prod = lax.dot_general(left, jnp.concatenate([wh, wm, wh, wl, wh, wm], 0), NN, preferred_element_type=F32)
            ins = jnp.broadcast_to(inside[:1], prod.shape)
            mat[k + MB + MB:] = jnp.where(ins, 0.0, mat[k + MB + MB:]) - prod
        if more:
            terms = [mult[j] * bc(w[j:j + 1]) for j in range(MB)]
            while len(terms) > 1:
                terms = [x + y for x, y in zip(terms[::2], terms[1::2])]
            rows = jnp.where(inside, 0.0, near) - terms[0]
    ri = lax.broadcasted_iota(jnp.int32, (BW, BW), 0)
    ci = lax.broadcasted_iota(jnp.int32, (BW, BW), 1)
    linv[...] = jnp.where(ci <= ri, linv[...], 0.0)


def dot6(a, b, dims):
    d = lambda x, y: lax.dot_general(x, y, dims, preferred_element_type=F32)
    ah, am, al = a
    bh, bm, bl = b
    return (d(am, bm) + d(ah, bl) + d(al, bh)) + (d(ah, bm) + d(am, bh)) + d(ah, bh)

def stack_dot(x, w, dims):
    xh, xm, xl = x
    wh, wm, wl = w
    k = xh.shape[0]
    d = lambda u, v: lax.dot_general(u, v, dims, preferred_element_type=F32)
    p1 = d(jnp.concatenate([xh, xm, xl], 0), wh)
    p2 = d(jnp.concatenate([xh, xm], 0), wm)
    p3 = d(xh, wl)
    return (p1[k + k:] + p2[k:] + p3) + (p1[k:k + k] + p2[:k]) + p1[:k]

def pieces(ref, at):
    return [ref[z, at] for z in PARTS]

def each(lo, hi, fn):
    def body(i, c):
        fn(i)
        return c
    lax.fori_loop(lo, hi, body, 0)

def upto(n, fn):
    each(0, n, fn)

def rows_at(start, size):
    return pl.ds(pl.multiple_of(start, SUBL), size)

def turn(c, step):
    return lax.rem(c + step, RING)

def place(part, phase):
    stride = RING**((part + phase) % 3)
    return lax.rem(lax.div(lax.axis_index('dp'), stride), RING), stride

def remote(src, dst, ssem, rsem, where):
    return pltpu.make_async_remote_copy(src_ref=src, dst_ref=dst, send_sem=ssem, recv_sem=rsem, device_id=where, device_id_type=pl.DeviceIdType.MESH)

def along(part, phase):
    return place(part, phase)[0]

def both_ends(sems, *at):
    return sems.at[(0, *at)], sems.at[(1, *at)]

def chip(part, phase, step):
    c, stride = place(part, phase)
    return {'dp': lax.axis_index('dp') + (turn(c, step) - c) * stride}

def partner():
    return {'mp': 1 - lax.axis_index('mp')}

def entry_barrier():
    sem = pltpu.get_barrier_semaphore()
    where = [chip(part, 0, step + 1) for part in PARTS for step in PARTS] + [partner()]
    for dev in where:
        pl.semaphore_signal(sem, inc=1, device_id=dev, device_id_type=pl.DeviceIdType.MESH)
    pl.semaphore_wait(sem, len(where))

def block_at(q, np_in, np_out, of_s):
    n_in, n_out = PAIR * np_in, PAIR * np_out
    past = min(q // EARLY, 1) if isinstance(q, int) else jnp.minimum(lax.div(q, EARLY), 1)
    in_s = q * n_out - q * (q - 1) + np_in * (np_in + 1) * past
    in_a = EARLY * n_out - EARLY * (EARLY - 1) + q * n_in - q * (q - 1)
    return of_s * in_s + (1 - of_s) * in_a

def decode(b, np_in, np_out):
    n_in, n_out = PAIR * np_in, PAIR * np_out
    at, was = 0, (0, 0)
    row, col = b, 0
    for q, in_s in [(q, 1) for q in range(EARLY)] + [(q, 0) for q in range(np_in)] + [(q, 1) for q in range(EARLY, np_out)]:
        now = (in_s * n_in + PAIR * q - at, in_s * np_in + q)
        hit = (b >= at).astype(jnp.int32)
        row = row + hit * (now[0] - was[0])
        col = col + hit * (now[1] - was[1])
        was = now
        at += in_s * n_out + (1 - in_s) * n_in - PAIR * q
    is_g = (b >= at).astype(jnp.int32)
    off = (b - at) * is_g
    row = row + is_g * (lax.rem(off, n_in) - row)
    col = jnp.minimum(col + is_g * (np_in + lax.div(off, n_in) - col), np_in + np_out - 1)
    in_s = (col >= np_in).astype(jnp.int32)
    old = in_s * ((col - np_in) * n_out + row - n_in) + (1 - in_s) * (col * n_in + row)
    return (1 - is_g) * old, is_g

def front_kernel(np_in, np_out, n_dp, cuts, order, a_hbm, g_hbm, s_hbm, ao_hbm, blocks, quarter, acc, full, agt, own, flip, old, ra, rb, rc, rd, ra2, rb2, rc2, rd2, r3, lsem, ssem, rsem, psem):
    p = lax.axis_index('mp')
    ns = a_hbm.shape[0]
    n_in, n_out = PAIR * np_in, PAIR * np_out
    n_col = np_in + np_out
    n_slot = flip.shape[0]

    def column(i, par):
        src, q = (a_hbm, i) if i < np_in else (g_hbm, i - np_in)
        return src.at[:, pl.ds(pl.multiple_of((PAIR * q + par) * BW, BW), BW)]
    def pair_of(i):
        return (i // PAIR, i % PAIR) if i < np_in else ((np_in + 1) // PAIR + (i - np_in) // PAIR, (i - np_in) % PAIR)
    def mine_at(i):
        z, h = pair_of(i)
        return own.at[z, :, h * BW:h * BW + BW]
    mine = [pltpu.make_async_copy(column(i, p), mine_at(i), lsem.at[i]) for i in range(n_col)]
    turns = [*range(np_in, n_col), *range(np_in)]
    theirs = [pltpu.make_async_copy(column(i, 1 - p), flip.at[z % n_slot], lsem.at[n_col + i]) for z, i in enumerate(turns)]
    of_a = range(block_at(0, np_in, np_out, 0), block_at(np_in, np_in, np_out, 0))
    n_old = block_at(np_out, np_in, np_out, 1)
    mine_rows = [rows_at(along(part, 1) * ROWS + along(part, 2) * SUBL, SUBL) for part in PARTS]
    olds = []
    for j in range(-(-n_old // RING)):
        m, part = divmod(j, 3)
        at, _ = decode(j * RING + along(part, 0), np_in, np_out)
        src = ao_hbm if j * RING in of_a else s_hbm
        olds.append(pltpu.make_async_copy(src.at[at, mine_rows[part]], old.at[m, part], lsem.at[PAIR * n_col + j]))
    for c in theirs[:n_slot] + mine[np_in:] + mine[:np_in]:
        c.start()
    entry_barrier()
    def transpose(src, i, par):
        for kc in range(ns // PW):
            agt[i * (ns // PW) + kc, pl.ds(pl.multiple_of(par * BW, BW), BW), :] = src[kc * PW:kc * PW + PW, :].T
    def ready(zs):
        for z in zs:
            i = turns[z]
            theirs[z].wait()
            transpose(flip.at[z % n_slot], i, 1 - p)
            if z + n_slot < n_col:
                theirs[z + n_slot].start()
        for z in zs:
            mine[turns[z]].wait()
            transpose(mine_at(turns[z]), turns[z], p)
    ready(range(np_out))
    for c in olds:
        c.start()

    def gram(z, row0, lo, hi, starts, scale):
        n = len(starts)
        rhs = own.at[z, :, :n * BW]
        def some(i):
            lhs = jnp.concatenate([agt[(row0 + i) * (ns // PW) + kc] for kc in range(ns // PW)], 1)
            prod = lax.dot_general(lhs, rhs[...], NN, preferred_element_type=F32) * scale
            for c in reversed(range(n)):
                for h in HALVES:
                    b = starts[c] + PAIR * (i - lo) + h
                    acc[lax.div(b, GROUP), lax.div(lax.rem(b, GROUP), RING), lax.rem(b, RING)] = prod[h * BW:h * BW + BW, c * BW:c * BW + BW]
        each(lo, hi, some)
    share_of_new = (1.0 - FACTOR_DECAY) / (ns * n_dp)
    n_pair = (np_in + 1) // PAIR
    start_of = lambda q, of_s: block_at(q, np_in, np_out, of_s)
    def grams(of_s, qs):
        n_pan = np_out if of_s else np_in
        for q in qs:
            both = [x for x in (q, q + 1) if x < n_pan]
            gram(n_pair * of_s + q // PAIR, np_in * of_s, q, n_pan, [start_of(x, of_s) - PAIR * (x - q) for x in both], share_of_new)
    def grads(qs):
        base = (np_in + np_out) * (np_in + np_out + 1) - np_out * n_in
        for q in qs:
            both = [x for x in (q, q + 1) if x < np_out]
            gram(n_pair + q // PAIR, 0, 0, np_in, [base + x * n_in for x in both], 1.0 / (ns * n_dp))

    def share(buf, ms, part, phase, coord):
        c1, e = along(part, 0), along(part, 1)
        if phase == 0:
            return buf.at[ms, part, coord]
        return buf.at[ms, part, c1, rows_at(coord * ROWS, ROWS) if phase == 1 else rows_at(e * ROWS + coord * SUBL, SUBL)]
    def cut(buf, ms, part, phase, coord, half):
        if phase == 0:
            return buf.at[ms, part, coord, pl.ds(half * HALF, HALF)]
        return buf.at[ms, part, along(part, 0), rows_at(coord * ROWS + half * MB, MB)]
    firsts = ((ra, rb), (ra2, rb2))
    seconds = ((rc, rd), (rc2, rd2))
    n_copy = 23
    def round_steps(k):
        m0, m1 = cuts[k], cuts[k + 1]
        ms = pl.ds(m0, m1 - m0)
        late = k == len(cuts) - 2
        def copy(part, kind, phase, i):
            c = along(part, phase)
            step = i + 1 if kind == 2 or kind == 3 and phase == 2 else UPDOWN[i]
            if kind == 0:
                src, dst = cut(acc, ms, part, phase, turn(c, 2), i), firsts[phase][i].at[ms, part]
            elif kind == 1:
                src, dst = share(acc, ms, part, phase, turn(c, step)), seconds[phase][i].at[ms, part]
            elif kind == 2:
                src, dst = share(acc, ms, part, phase, turn(c, step)), r3.at[i, ms, part]
            else:
                src = share(full, ms, part, phase, c) if kind == 3 else cut(full, ms, part, phase, turn(c, 4 - step), i)
                dst = src
            s = (k * 3 + part) * n_copy + (0, 4, 8, 11, 19)[kind] + (PAIR * phase + i if kind < 2 or kind == 4 else 3 * (2 - phase) + i if kind == 3 else i)
            return remote(src, dst, ssem.at[s], rsem.at[s], chip(part, phase, step))
        every, near = PARTS, HALVES
        def go(part, kind, phase, which):
            for i in which:
                copy(part, kind, phase, i).start()
        def come(part, kind, phase, which):
            for i in which:
                copy(part, kind, phase, i).wait_recv()
        def add(part, c1, rows, *srcs):
            def some(m):
                v = acc[m, part, c1, rows]
                for s in srcs:
                    v = v + s(m)
                acc[m, part, c1, rows] = v
            each(m0, m1, some)
        def fold(phase):
            for part in PARTS:
                c = along(part, phase)
                for z in HALVES:
                    come(part, 0, phase, (z,))
                    u = turn(c, UPDOWN[z])
                    buf = firsts[phase][z]
                    if phase == 0:
                        add(part, u, pl.ds(z * HALF, HALF), lambda m: buf[m, part])
                    else:
                        add(part, along(part, 0), rows_at(u * ROWS + z * MB, MB), lambda m: buf[m, part])
                    go(part, 1, phase, (z,))
        def gain(phase):
            for part in PARTS:
                come(part, 1, phase, near)
                b0, b1 = seconds[phase]
                rows = pl.ds(0, BW) if phase == 0 else rows_at(along(part, 1) * ROWS, ROWS)
                add(part, along(part, 0), rows, lambda m: b0[m, part], lambda m: b1[m, part])
                go(part, phase * 2, 1 + phase, every if phase else near)
        def done():
            for part in PARTS:
                come(part, 2, 2, every)
                c1, rows = along(part, 0), mine_rows[part]
                def some(m):
                    v = acc[m, part, c1, rows] + (r3[0, m, part] + r3[1, m, part] + r3[2, m, part])
                    if not late:
                        _, is_g = decode((m * 3 + part) * RING + c1, np_in, np_out)
                        v = v + jnp.where(is_g == 1, 0.0, old[m, part] * FACTOR_DECAY)
                    full[m, part, c1, rows] = v
                each(m0, m1, some)
                go(part, 3, 2, every)
        def widen():
            for part in PARTS:
                come(part, 3, 2, every)
                go(part, 3, 1, near)
        def relay_wide():
            for z in near:
                for part in PARTS:
                    come(part, 3, 1, (z,))
                    go(part, 4, 1, (z,))
        def near_go():
            for part in PARTS:
                come(part, 4, 1, near)
                go(part, 3, 0, near)
        def relay():
            for z in near:
                for part in PARTS:
                    come(part, 3, 0, (z,))
                    go(part, 4, 0, (z,))
        def whole():
            for part in PARTS:
                come(part, 4, 0, near)
                swap(part).start()
                keep(part).start()
        def swap(part):
            return remote(full.at[ms, part], blocks.at[p, ms, part], *both_ends(psem, k, part), partner())
        def keep(part):
            return pltpu.make_async_copy(full.at[ms, part], blocks.at[p, ms, part], psem.at[2, k, part])
        def wide():
            for part in PARTS:
                come(part, 4, 1, near)
                swap_quarter(part).start()
                def some(m):
                    quarter[p, m - m0, part] = full[m, part, along(part, 0)]
                each(m0, m1, some)
        def swap_quarter(part):
            return remote(full.at[ms, part, along(part, 0)], quarter.at[p, :, part], *both_ends(psem, k, part), partner())
        def start():
            for part in PARTS:
                go(part, 0, 0, near)
        kinds = [(0, 0, near), (1, 0, near), (0, 1, near), (1, 1, near), (2, 2, every), (3, 2, every), (3, 1, near), (4, 1, near), (3, 0, near), (4, 0, near)]
        def settle():
            for part in PARTS:
                for kind, phase, which in kinds[:len(kinds) - PAIR * late]:
                    for i in which:
                        copy(part, kind, phase, i).wait_send()
                c = swap_quarter(part) if late else swap(part)
                c.wait_recv()
                c.wait_send()
                if not late:
                    keep(part).wait()
        return [start, lambda: fold(0), lambda: gain(0), lambda: fold(1), lambda: gain(1), done, widen, relay_wide] + ([wide] if late else [near_go, relay, whole]), settle
    rounds = [round_steps(k) for k in range(len(cuts) - 1)]
    chunks = [lambda: grams(1, (0,)), lambda: (grams(1, (2,)), ready(range(np_out, n_col)), grams(0, range(0, np_in, PAIR))), lambda: (grams(1, range(EARLY, np_out, PAIR)), grads((0,))),
        lambda: (grads(range(2, np_out, PAIR)), [c.wait() for c in olds])]
    for k, z in order:
        todo = chunks if k < 0 else rounds[k][0]
        if 0 <= z < len(todo):
            todo[z]()
    for _, settle in rounds:
        settle()

def front(a_loc, g_loc, a_old3, s_old3, n_dp, cuts):
    ns, c_in = a_loc.shape
    np_in, np_out = c_in // PW, g_loc.shape[1] // PW
    V = lambda *s: pltpu.VMEM(s, F32)
    B = lambda *s: pltpu.VMEM(s, BF)
    D = lambda *s: pltpu.SemaphoreType.DMA(s)
    hb = pl.BlockSpec(memory_space=pl.ANY)
    vb = pl.BlockSpec(memory_space=pltpu.VMEM)
    nm = cuts[-1]
    order = [(k, x - lag) for x in range(15) for k, lag in ((-1, 0), (0, 0), (1, 2), (2, 3))]
    slab = lambda n: [V(nm, 3, n, BW)] * 2
    n_col = np_in + np_out
    s_blk, a_blk = s_old3.reshape(-1, BW, BW), a_old3.reshape(-1, BW, BW)
    n_old = -(-block_at(np_out, np_in, np_out, 1) // RING)
    f32 = lambda *s: jax.ShapeDtypeStruct(s, F32)
    return pl.pallas_call(functools.partial(front_kernel, np_in, np_out, n_dp, cuts, order),
        out_shape=(f32(2, cuts[-2], 3, RING, BW, BW), f32(2, nm - cuts[-2], 3, BW, BW)),
        in_specs=[hb] * 4, out_specs=(hb, vb),
        scratch_shapes=[*[V(nm, 3, RING, BW, BW)] * 2, B(n_col * ns // PW, PW, PW), B((np_in + 1) // PAIR + (np_out + 1) // PAIR, ns, PW), B(4, ns, BW), V(cuts[-2], 3, SUBL, BW),
            *slab(HALF), *slab(BW), *slab(MB), *slab(ROWS), V(3, nm, 3, SUBL, BW), D(PAIR * n_col + n_old), *[D(69 * (len(cuts) - 1))] * 2, D(3, len(cuts) - 1, 3)],
        compiler_params=pltpu.CompilerParams(collective_id=0, has_side_effects=True, vmem_limit_bytes=67043328), name="front")(a_loc, g_loc, s_blk, a_blk)

def solve_kernel(np_in, np_out, n_dp, damp, cuts, early, quarter, fin, full, tmat, mat, linv, inv_all, lsp, lspt, xw, zin, pack, ssem, rsem, psem, osem):
    p = lax.axis_index('mp')
    d = lax.axis_index('dp')
    n_own = np_in * BW // n_dp
    n_in, n_out = PAIR * np_in, PAIR * np_out
    first, then = [[pltpu.make_async_copy(early.at[par, pl.ds(cuts[z], cuts[z + 1] - cuts[z])], full.at[par, pl.ds(cuts[z], cuts[z + 1] - cuts[z])], osem.at[z, par]) for par in HALVES] for z in HALVES]
    for c in first + then:
        c.start()
    entry_barrier()
    ms = pl.ds(cuts[-2], cuts[-1] - cuts[-2])
    def last(par, part, z, on):
        c = along(part, 0)
        ref = full.at[par, ms, part, turn(c, 3 - PAIR * z), pl.ds(z * HALF, HALF)] if on else full.at[par, ms, part, c]
        s = 30 + (par * 3 + part) * 4 + PAIR * on + z
        return remote(ref, ref, ssem.at[s], rsem.at[s], chip(part, 0, UPDOWN[z]))
    every = [(z, part, par) for z in HALVES for part in PARTS for par in HALVES]
    @pl.when(p == 1)
    def _():
        for part in PARTS:
            for par in HALVES:
                def put(m):
                    full[par, m, part, along(part, 0)] = quarter[par, m - cuts[-2], part]
                each(cuts[-2], cuts[-1], put)
        for z, part, par in every:
            last(par, part, z, 0).start()
    def wait_for(copies):
        for c in copies:
            c.wait()
    wait_for(first)
    @pl.when(p == 1)
    def _():
        wait_for(then)

    def block(par, b):
        return full[par, lax.div(b, GROUP), lax.div(lax.rem(b, GROUP), RING), lax.rem(b, RING)]

    base_g = np_out * (np_out + 1) + np_in * (np_in + 1)
    npan = np_out - (np_out - np_in) * p
    eye = jnp.where(lax.broadcasted_iota(jnp.int32, (BW, BW), 0) == lax.broadcasted_iota(jnp.int32, (BW, BW), 1), damp, 0.0)

    def load(q):
        base = block_at(q, np_in, np_out, 1 - p)
        slot = lax.rem(q, PAIR)
        for par in HALVES:
            cols = pl.ds(par * BW, BW)
            def rows(i):
                for h in HALVES:
                    tmat[slot, i, h * BW:h * BW + BW, cols] = block(par, base + PAIR * (i - q) + h)
            each(q, npan, rows)
            tmat[slot, q, cols, cols] = tmat[slot, q, cols, cols] + eye

    lsp_spare = lsp.shape[1] - 1
    def ltile(i, k):
        return lax.div(i * (i - 1), PAIR) + k

    def update(i, k, q, ok):
        slot = lax.rem(q, PAIR)
        at = ok * i + (1 - ok) * np_out
        prod = stack_dot(pieces(lsp, ok * ltile(i, k)), pieces(lspt, ok * ltile(q, k)), NN)
        tmat[slot, at] = tmat[slot, at] - prod

    def task(s, q):
        left = jnp.maximum(npan - 1 - q, 1)
        turn = lax.div(s, left)
        ok = (turn <= q).astype(jnp.int32) * jnp.minimum(q, 1) * jnp.minimum(npan - 1 - q, 1)
        k = turn - 1 + q * (1 - jnp.minimum(turn, 1))
        update(q + 1 + lax.rem(s, left), k, q + jnp.minimum(turn, 1), ok)

    load(0)

    def panel(k):
        q = lax.div(k, PAIR)
        h = lax.rem(k, PAIR)
        slot = lax.rem(q, PAIR)
        @pl.when(h == 0)
        def _():
            mat[...] = tmat[slot, q, :BW, :BW]
        factor_block(mat, linv, lambda t: task(h * SUBL + t, q))
        @pl.when(h == 0)
        def _():
            inv0 = linv[...]
            inv0s = split3(inv0)
            l10 = dot6(split3(tmat[slot, q, BW:, :BW]), inv0s, NT)
            l10s = split3(l10)
            mat[...] = tmat[slot, q, BW:, BW:] - dot6(l10s, l10s, NT)
            inv_all[q, :BW, :BW] = inv0
            inv_all[q, :BW, BW:] = jnp.zeros((BW, BW), F32)
            inv_all[q, BW:, :BW] = dot6(l10s, inv0s, NN)
        @pl.when((h == 1) & (q < npan - 1))
        def _():
            each(MB, (npan - 1 - q) * (q + 1), lambda s: task(s, q))
        @pl.when(h == 1)
        def _():
            inv1 = linv[...]
            inv_all[q, BW:, BW:] = inv1
            inv_all[q, BW:, :BW] = -dot6(split3(inv1), split3(inv_all[q, BW:, :BW]), NN)
            invs = split3(inv_all[q].T)
            def below(s):
                i = q + 1 + PAIR * s
                ok = (i + 1 < npan).astype(jnp.int32)
                both = jnp.concatenate([tmat[slot, i], tmat[slot, ok * (i + 1) + (1 - ok) * np_out]], 0)
                low = stack_dot(split3(both), invs, NN)
                at = ltile(i, q), ok * ltile(i + 1, q) + (1 - ok) * lsp_spare
                for u in HALVES:
                    one = low[u * PW:(u + 1) * PW]
                    for ref, v in ((lsp, one), (lspt, one.T)):
                        for z, piece in enumerate(split3(v)):
                            ref[z, at[u]] = piece
            upto(lax.div(npan - q, PAIR), below)
        @pl.when((h == 1) & (q < npan - 1))
        def _():
            @pl.when(q == 0)
            def _():
                load(1)
            update(q + 1, q, q + 1, 1)
            @pl.when(q < npan - 2)
            def _():
                load(q + 2)
    upto(1, panel)
    @pl.when(p == 0)
    def _():
        wait_for(then)
    each(1, PAIR * npan, panel)
    @pl.when(p == 1)
    def _():
        for z, part, par in every:
            last(par, part, z, 0).wait_recv()
            last(par, part, z, 1).start()

    zcopy = remote(zin.at[0], zin.at[1], *both_ends(psem, 1), partner())
    @pl.when(p == 1)
    def _():
        row = lax.broadcasted_iota(jnp.int32, (MB, PW), 0)
        lane = lax.broadcasted_iota(jnp.int32, (MB, PW), 1)
        par = lax.div(row, SUBL)
        idx = lax.rem(row, SUBL)
        col = d * n_own + idx
        for q in range(np_in):
            hit = (idx < n_own) & (lax.div(col, BW) == q) & (lane == par * BW + lax.rem(col, BW))
            xw[q] = jnp.where(hit, 1.0, 0.0)
    @pl.when(p == 0)
    def _():
        zcopy.wait_recv()
        def cp(q):
            xw[q] = zin[1, q]
        upto(np_out, cp)

    def spread(x, lo, hi, tile, ref):
        xs = split3(x)
        def some(i):
            for u in range(RING):
                j = lo + RING * i + u
                ok = (j < hi).astype(jnp.int32)
                at = ok * j + (1 - ok) * np_out
                xw[at] = xw[at] - stack_dot(xs, pieces(ref, ok * tile(j)), NN)
        upto(lax.div(hi - lo + RING - 1, RING), some)
    def fwd(q):
        y = stack_dot(split3(xw[q]), split3(inv_all[q]), NT)
        xw[q] = y
        spread(y, q + 1, npan, lambda j: ltile(j, q), lspt)
    upto(npan, fwd)
    def back(s):
        q = npan - 1 - s
        x = stack_dot(split3(xw[q]), split3(inv_all[q]), NN)
        xw[q] = x
        spread(x, 0, q, lambda j: ltile(q, j), lsp)
    upto(npan, back)

    xcopy = remote(pack.at[1], pack.at[0], *both_ends(psem, 2), partner())
    @pl.when(p == 1)
    def _():
        for z, part, par in every:
            last(par, part, z, 1).wait_recv()
        def zq(q):
            for par in HALVES:
                acc = jnp.zeros((MB, BW), F32)
                for i in range(n_in):
                    acc = acc + stack_dot(split3(xw[i // PAIR, :, (i % PAIR) * BW:(i % PAIR + 1) * BW]), split3(block(par, base_g + q * n_in + i)), NN)
                zin[0, q, :, par * BW:par * BW + BW] = acc
        upto(np_out, zq)
        zcopy.start()
        xcopy.wait_recv()
        zcopy.wait_send()
    @pl.when(p == 0)
    def _():
        for par in reversed(HALVES):
            pack[par, np_out * n_own:] = jnp.zeros((pack.shape[1] - np_out * n_own, PW), F32)
            for q in range(np_out):
                pack[par, q * n_own:(q + 1) * n_own] = xw[q, par * SUBL:par * SUBL + n_own]
            if par == 1:
                xcopy.start()
    n_t = fin.shape[4]
    for t in range(PAIR * (pack.shape[1] // SUBL)):
        part, z = divmod(t, n_t)
        half = t % PAIR
        fin[(part, *(along(part, ph) for ph in PARTS), z)] = pack[0, t // PAIR * SUBL:t // PAIR * SUBL + SUBL, half * BW:half * BW + BW]
    def fcopy(part, j):
        c1, e, f = (along(part, ph) for ph in PARTS)
        if j < 6:
            phase, step = 2 - j // 3, j % 3 + 1
            ref = fin.at[part, c1, e, f] if phase == 2 else fin.at[part, c1, e]
        else:
            z = j % PAIR
            phase, step = 0, UPDOWN[z]
            ref = fin.at[part, c1] if j < 8 else fin.at[part, turn(c1, 3 - PAIR * z), pl.ds(PAIR * z, 2)]
        s = part * 10 + j
        return remote(ref, ref, ssem.at[s], rsem.at[s], chip(part, phase, step))
    def fstep(came, js):
        def part_fn(part):
            for j in came:
                fcopy(part, j).wait_recv()
            for j in js:
                fcopy(part, j).start()
        for part in PARTS:
            part_fn(part)
    fstep((), (0, 1, 2))
    fstep((0, 1, 2), (3, 4, 5))
    fstep((3, 4, 5), (6, 7))
    def frelay(part):
        for z in HALVES:
            fcopy(part, 6 + z).wait_recv()
            fcopy(part, 8 + z).start()
    for part in PARTS:
        frelay(part)
    fstep((8, 9), ())
    for part in PARTS:
        for j in range(10):
            fcopy(part, j).wait_send()
    @pl.when(p == 1)
    def _():
        for z, part, par in every:
            last(par, part, z, 0).wait_send()
            last(par, part, z, 1).wait_send()
    @pl.when(p == 0)
    def _():
        xcopy.wait_send()

def solve(early, quarter, np_in, np_out, n_dp, damp, cuts):
    n_own = np_in * BW // n_dp
    n_row = -(-np_out * n_own // SUBL)
    n_t = -(-PAIR * n_row // 3)
    n_tile = np_out * (np_out - 1) // PAIR + 1
    V = lambda *s: pltpu.VMEM(s, F32)
    D = lambda *s: pltpu.SemaphoreType.DMA(s)
    hb = pl.BlockSpec(memory_space=pl.ANY)
    vb = pl.BlockSpec(memory_space=pltpu.VMEM)
    f32 = lambda *s: jax.ShapeDtypeStruct(s, F32)
    return pl.pallas_call(functools.partial(solve_kernel, np_in, np_out, n_dp, damp, cuts),
        out_shape=f32(3, RING, RING, RING, n_t, SUBL, BW), in_specs=[hb, vb], out_specs=vb,
        scratch_shapes=[V(2, cuts[-1], 3, RING, BW, BW), V(2, np_out + 1, PW, PW), V(BW, BW), V(BW, BW), V(np_out, PW, PW), *[pltpu.VMEM((3, n_tile, PW, PW), BF)] * 2, V(np_out + 1, MB, PW),
            V(2, np_out, MB, PW), V(2, n_row * SUBL, PW), D(54), D(54), D(2, 3), D(2, 2)],
        compiler_params=pltpu.CompilerParams(collective_id=1, has_side_effects=True, vmem_limit_bytes=67043328), name="solve")(early, quarter)

def finish_kernel(np_in, np_out, n_own, w_hbm, blocks, fin, w_out, a_out, s_out, wbuf, gath, cols_s, cols_a, up_s, up_a, isem, lsem, usem, wsem, csem):
    p = lax.axis_index('mp')
    wload = pltpu.make_async_copy(w_hbm, wbuf, isem)
    wload.start()
    sets = [(s_out, cols_s, up_s, np_out, 1), (a_out, cols_a, up_a, np_in, 0)]
    jobs, n = [], 0
    for out, cols, up, n_pan, of_s in sets:
        for q in range(n_pan):
            base = block_at(q, np_in, np_out, of_s) // PAIR
            low = pltpu.make_async_copy(blocks.at[p, pl.ds(base, n_pan - q)], cols.at[q, pl.ds(q, n_pan - q)], lsem.at[n])
            ups = [pltpu.make_async_copy(blocks.at[par, pl.ds(base + 1, n_pan - 1 - q), p], up.at[par, q, pl.ds(q + 1, n_pan - 1 - q)], usem.at[par, n]) for par in HALVES] if q < n_pan - 1 else []
            send = pltpu.make_async_copy(cols.at[q], out.at[q], csem.at[n])
            jobs.append((low, ups, send, cols, up, q))
            n += 1
    for low, ups, *_ in jobs:
        for c in (*ups, low):
            c.start()
    n_t = fin.shape[4]
    def tile(t, c):
        part, z = divmod(t, n_t)
        return fin[(part, *(c + c)[part:part + 3], z)]
    wload.wait()
    def weights(q):
        lo, hi = q * n_own // SUBL, ((q + 1) * n_own - 1) // SUBL
        for half in HALVES:
            def fill(z):
              for y in range(RING):
                vals = []
                for x in range(RING):
                    c = (x, y, z)
                    v = jnp.concatenate([tile(PAIR * r + half, c) for r in range(lo, hi + 1)], 0)
                    at = q * n_own - lo * SUBL
                    vals.append(v[at:at + n_own])
                gath[rows_at((z * RING + y) * RING * n_own, RING * n_own)] = jnp.concatenate(vals, 0)
            upto(RING, fill)
            for b in range(np_in):
                r = slice((PAIR * q + half) * BW, (PAIR * q + half + 1) * BW)
                wbuf[b, r] = wbuf[b, r] - LEARN_RATE * gath[b * BW:b * BW + BW].T
    for q in range(np_out // PAIR):
        weights(q)
    for low, ups, send, cols, up, q in jobs:
        low.wait()
        for c in ups:
            c.wait()
    for low, ups, send, cols, up, q in jobs:
        for q2 in range(q):
            for par in HALVES:
                cols[q, q2, par] = up[par, q2, q].T
        send.start()
    for q in range(np_out // PAIR, np_out):
        weights(q)
    wsend = pltpu.make_async_copy(wbuf, w_out, wsem)
    wsend.start()
    for low, ups, send, *_ in jobs:
        send.wait()
    wsend.wait()

def finish(w3, blocks, fin, np_in, np_out, n_dp):
    V = pltpu.VMEM
    D = pltpu.SemaphoreType.DMA
    hb = pl.BlockSpec(memory_space=pl.ANY)
    vb = pl.BlockSpec(memory_space=V)
    n_job = np_in + np_out
    square = lambda n: (n, n, 2, BW, BW)
    w_new, a_new, s_new = pl.pallas_call(functools.partial(finish_kernel, np_in, np_out, np_in * BW // n_dp),
        out_shape=(jax.ShapeDtypeStruct(w3.shape, F32), jax.ShapeDtypeStruct(square(np_in), F32), jax.ShapeDtypeStruct(square(np_out), F32)),
        in_specs=[hb, hb, vb], out_specs=(hb, hb, hb),
        scratch_shapes=[V(w3.shape, F32), V((np_in * BW, BW), F32), V(square(np_out), F32), V(square(np_in), F32), V((2, np_out, np_out, BW, BW), F32), V((2, np_in, np_in, BW, BW), F32),
            D, D((n_job,)), D((2, n_job)), D, D((n_job,))],
        compiler_params=pltpu.CompilerParams(vmem_limit_bytes=63 * 2**20), name="outputs")(w3, blocks.reshape(2, -1, 2, BW, BW), fin)
    return w_new, a_new.reshape(np_in, -1, BW), s_new.reshape(np_out, -1, BW)


def solution(mesh):
    n_dp = mesh.shape['dp']

    def local_step(a_loc, g_loc, w_loc, a_old_loc, s_old_loc):
        np_in = a_loc.shape[1] // PW
        np_out = g_loc.shape[1] // PW
        n_in, n_out = PAIR * np_in, PAIR * np_out
        early = np_in * (np_in + 1) + np_out * (np_out + 1)
        cuts = (0, 2, -(-early // GROUP), (early + n_in * np_out) // GROUP)
        panels = lambda x: x.transpose(1, 0, 2)
        blocks, quarter = front(a_loc, g_loc, panels(a_old_loc), panels(s_old_loc), n_dp, cuts)
        fin = solve(blocks, quarter, np_in, np_out, n_dp, DAMP_SHIFT, cuts)
        return tuple(panels(x) for x in finish(panels(w_loc), blocks, fin, np_in, np_out, n_dp))

    spec_rows = P('dp', None)
    spec_cyc = P(None, 'mp', None)
    return jax.shard_map(local_step, mesh=mesh, in_specs=(spec_rows, spec_rows, spec_cyc, spec_cyc, spec_cyc), out_specs=(spec_cyc, spec_cyc, spec_cyc), check_vma=False)
```

```python
import functools
import math
import jax
import jax.numpy as jnp
from jax import lax
from jax.experimental import pallas as pl
from jax.experimental.pallas import tpu as pltpu
from jax.sharding import PartitionSpec as P

BW = 128
PW = 256
RING = 4
SUBL = 8
HALF = 64
ROWS = 32
GROUP = 12
EARLY = 4
PAIR = 2
HALVES = (0, 1)
UPDOWN = (1, 3)
PARTS = (0, 1, 2)
FACTOR_DECAY = 0.95
LEARN_RATE = 1.0
DAMPING = 0.001
DAMP_SHIFT = math.sqrt(DAMPING)
MB = 16
F32 = jnp.float32
BF = jnp.bfloat16
NT = (((1,), (1,)), ((), ()))
NN = (((1,), (0,)), ((), ()))


def split3(x):
    h = x.astype(BF)
    r = x - h.astype(F32)
    m = r.astype(BF)
    return h, m, (r - m.astype(F32)).astype(BF)

def bc(x):
    return jnp.broadcast_to(x, (MB, BW))

def factor_block(mat, linv, beside=None):
    lane = lax.broadcasted_iota(jnp.int32, (MB, BW), 1)
    sub = lax.broadcasted_iota(jnp.int32, (MB, BW), 0)
    odd = lax.rem(sub, PAIR)
    zero = lane.astype(F32) * 0.0
    ri = lax.broadcasted_iota(jnp.int32, (BW, BW), 0)
    ci = lax.broadcasted_iota(jnp.int32, (BW, BW), 1)
    whole = mat[...]
    diag = jnp.where(ci == ri, whole, 0.0)
    down, along_row = lax.rsqrt(jnp.sum(diag, axis=1, keepdims=True)), lax.rsqrt(jnp.sum(diag, axis=0, keepdims=True))
    mat[...] = whole * down * along_row
    rows = mat[:MB]
    for t in range(BW // MB):
        k = t * MB
        if beside is not None:
            beside(t)
        cols = jnp.concatenate([bc(rows[:, k + i:k + i + 1]) for i in range(MB)], 0).reshape(MB, MB, BW) + zero
        inside = (lane >= k) & (lane < k + MB)
        ext = jnp.where(inside, jnp.where(lane == sub + k, 1.0, 0.0), rows)
        more = k + MB < BW
        far = k + MB + MB < BW
        if more:
            near = mat[k + MB:k + MB + MB]
            mult = [bc(near[:, k + i:k + i + 1]) for i in range(MB)]
        if far:
            rh, rm, rl = split3(rows)
            left = jnp.concatenate([rh, rh, rm, rh, rl, rm], 0).T[k + MB + MB:]
        dg = of = None
        for j in range(0, MB, PAIR):
            u, v = cols[0], cols[1]
            a, b, c = bc(u[j:j + 1]), bc(u[j + 1:j + 2]), bc(v[j + 1:j + 2])
            det = a * c - b * b
            rdet = 1.0 / det
            ra = 1.0 / a
            e0, e1 = bc(ext[j:j + 1]), bc(ext[j + 1:j + 2])
            linv[k + j:k + j + 1] = (e0 * lax.rsqrt(a))[:1]
            linv[k + j + 1:k + j + 2] = ((e1 - (b * ra) * e0) * lax.rsqrt(det * ra))[:1]
            pair = (sub == j) | (sub == j + 1)
            u, v = jnp.where(pair, 0.0, u), jnp.where(pair, 0.0, v)
            n0, n1 = c * u - b * v, a * v - b * u
            f0, f1 = n0 * rdet, n1 * rdet
            if j + 2 < MB:
                left_cols = cols[2:]
                soon = left_cols[:2]
                soon = soon - (n0 * jnp.broadcast_to(soon[:, j:j + 1], soon.shape) + n1 * jnp.broadcast_to(soon[:, j + 1:j + 2], soon.shape)) * rdet
                if j + 4 < MB:
                    late = left_cols[2:]
                    late = late - (f0 * jnp.broadcast_to(late[:, j:j + 1], late.shape) + f1 * jnp.broadcast_to(late[:, j + 1:j + 2], late.shape))
                    cols = jnp.concatenate([soon, late], 0)
                else:
                    cols = soon
            ext = ext - (f0 * e0 + f1 * e1)
            d_here = jnp.where(odd == 0, c, a) * rdet
            dg = d_here if dg is None else jnp.where(sub >= j, d_here, dg)
            of = b * rdet if of is None else jnp.where(sub >= j, b * rdet, of)
        w = ext * dg - jnp.where(odd == 0, jnp.roll(ext, -1, 0), jnp.roll(ext, 1, 0)) * of
        if far:
            wh, wm, wl = split3(w)
            prod = lax.dot_general(left, jnp.concatenate([wh, wm, wh, wl, wh, wm], 0), NN, preferred_element_type=F32)
            ins = jnp.broadcast_to(inside[:1], prod.shape)
            mat[k + MB + MB:] = jnp.where(ins, 0.0, mat[k + MB + MB:]) - prod
        if more:
            terms = [mult[j] * bc(w[j:j + 1]) for j in range(MB)]
            while len(terms) > 1:
                terms = [x + y for x, y in zip(terms[::PAIR], terms[1::PAIR])]
            rows = jnp.where(inside, 0.0, near) - terms[0]
    linv[...] = jnp.where(ci <= ri, linv[...], 0.0) * along_row


def dot6(a, b, dims):
    d = lambda x, y: lax.dot_general(x, y, dims, preferred_element_type=F32)
    ah, am, al = a
    bh, bm, bl = b
    return (d(am, bm) + d(ah, bl) + d(al, bh)) + (d(ah, bm) + d(am, bh)) + d(ah, bh)

def stack_dot(x, w, dims):
    xh, xm, xl = x
    wh, wm, wl = w
    k = xh.shape[0]
    d = lambda u, v: lax.dot_general(u, v, dims, preferred_element_type=F32)
    p1 = d(jnp.concatenate([xh, xm, xl], 0), wh)
    p2 = d(jnp.concatenate([xh, xm], 0), wm)
    p3 = d(xh, wl)
    return (p1[k + k:] + p2[k:] + p3) + (p1[k:k + k] + p2[:k]) + p1[:k]

def pieces(ref, at):
    return [ref[z, at] for z in PARTS]

def each(lo, hi, fn):
    def body(i, c):
        fn(i)
        return c
    lax.fori_loop(lo, hi, body, 0)

def upto(n, fn):
    each(0, n, fn)

def rows_at(start, size):
    return pl.ds(pl.multiple_of(start, SUBL), size)

def turn(c, step):
    return lax.rem(c + step, RING)

def place(part, phase):
    stride = RING**((part + phase) % 3)
    return lax.rem(lax.div(lax.axis_index('dp'), stride), RING), stride

def remote(src, dst, ssem, rsem, where):
    return pltpu.make_async_remote_copy(src_ref=src, dst_ref=dst, send_sem=ssem, recv_sem=rsem, device_id=where, device_id_type=pl.DeviceIdType.MESH)

def along(part, phase):
    return place(part, phase)[0]

def both_ends(sems, *at):
    return sems.at[(0, *at)], sems.at[(1, *at)]

def chip(part, phase, step):
    c, stride = place(part, phase)
    return {'dp': lax.axis_index('dp') + (turn(c, step) - c) * stride}

def partner():
    return {'mp': 1 - lax.axis_index('mp')}

def entry_barrier():
    sem = pltpu.get_barrier_semaphore()
    where = [chip(part, 0, step + 1) for part in PARTS for step in PARTS] + [partner()]
    for dev in where:
        pl.semaphore_signal(sem, inc=1, device_id=dev, device_id_type=pl.DeviceIdType.MESH)
    pl.semaphore_wait(sem, len(where))

def block_at(q, np_in, np_out, of_s):
    n_in, n_out = PAIR * np_in, PAIR * np_out
    past = min(q // EARLY, 1) if isinstance(q, int) else jnp.minimum(lax.div(q, EARLY), 1)
    in_s = q * n_out - q * (q - 1) + np_in * (np_in + 1) * past
    in_a = EARLY * n_out - EARLY * (EARLY - 1) + q * n_in - q * (q - 1)
    return of_s * in_s + (1 - of_s) * in_a

def decode(b, np_in, np_out):
    n_in, n_out = PAIR * np_in, PAIR * np_out
    at, was = 0, (0, 0)
    row, col = b, 0
    for q, in_s in [(q, 1) for q in range(EARLY)] + [(q, 0) for q in range(np_in)] + [(q, 1) for q in range(EARLY, np_out)]:
        now = (in_s * n_in + PAIR * q - at, in_s * np_in + q)
        hit = (b >= at).astype(jnp.int32)
        row = row + hit * (now[0] - was[0])
        col = col + hit * (now[1] - was[1])
        was = now
        at += in_s * n_out + (1 - in_s) * n_in - PAIR * q
    is_g = (b >= at).astype(jnp.int32)
    off = (b - at) * is_g
    row = row + is_g * (lax.rem(off, n_in) - row)
    col = jnp.minimum(col + is_g * (np_in + lax.div(off, n_in) - col), np_in + np_out - 1)
    in_s = (col >= np_in).astype(jnp.int32)
    old = in_s * ((col - np_in) * n_out + row - n_in) + (1 - in_s) * (col * n_in + row)
    return (1 - is_g) * old, is_g

def front_kernel(np_in, np_out, n_dp, cuts, order, a_hbm, g_hbm, s_hbm, ao_hbm, blocks, quarter, acc, full, agt, own, flip, old, ra, rb, rc, rd, ra2, rb2, rc2, rd2, r3, lsem, ssem, rsem, psem):
    p = lax.axis_index('mp')
    ns = a_hbm.shape[0]
    n_in, n_out = PAIR * np_in, PAIR * np_out
    n_col = np_in + np_out
    n_slot = flip.shape[0]

    def column(i, par):
        src, q = (a_hbm, i) if i < np_in else (g_hbm, i - np_in)
        return src.at[:, pl.ds(pl.multiple_of((PAIR * q + par) * BW, BW), BW)]
    def pair_of(i):
        return (i // PAIR, i % PAIR) if i < np_in else ((np_in + 1) // PAIR + (i - np_in) // PAIR, (i - np_in) % PAIR)
    def mine_at(i):
        z, h = pair_of(i)
        return own.at[z, :, h * BW:h * BW + BW]
    mine = [pltpu.make_async_copy(column(i, p), mine_at(i), lsem.at[i]) for i in range(n_col)]
    turns = [*range(np_in, n_col), *range(np_in)]
    theirs = [pltpu.make_async_copy(column(i, 1 - p), flip.at[z % n_slot], lsem.at[n_col + i]) for z, i in enumerate(turns)]
    of_a = range(block_at(0, np_in, np_out, 0), block_at(np_in, np_in, np_out, 0))
    n_old = block_at(np_out, np_in, np_out, 1)
    mine_rows = [rows_at(along(part, 1) * ROWS + along(part, 2) * SUBL, SUBL) for part in PARTS]
    olds = []
    for j in range(-(-n_old // RING)):
        m, part = divmod(j, 3)
        at, _ = decode(j * RING + along(part, 0), np_in, np_out)
        src = ao_hbm if j * RING in of_a else s_hbm
        olds.append(pltpu.make_async_copy(src.at[at, mine_rows[part]], old.at[m, part], lsem.at[PAIR * n_col + j]))
    for c in theirs[:n_slot] + mine[np_in:] + mine[:np_in]:
        c.start()
    entry_barrier()
    def transpose(src, i, par):
        for kc in range(ns // PW):
            agt[i * (ns // PW) + kc, pl.ds(pl.multiple_of(par * BW, BW), BW), :] = src[kc * PW:kc * PW + PW, :].T
    def ready(zs):
        for z in zs:
            i = turns[z]
            theirs[z].wait()
            transpose(flip.at[z % n_slot], i, 1 - p)
            if z + n_slot < n_col:
                theirs[z + n_slot].start()
        for z in zs:
            mine[turns[z]].wait()
            transpose(mine_at(turns[z]), turns[z], p)
    ready(range(np_out))
    for c in olds:
        c.start()

    def gram(z, row0, lo, hi, starts, scale):
        n = len(starts)
        rhs = own.at[z, :, :n * BW]
        def some(i):
            lhs = jnp.concatenate([agt[(row0 + i) * (ns // PW) + kc] for kc in range(ns // PW)], 1)
            prod = lax.dot_general(lhs, rhs[...], NN, preferred_element_type=F32) * scale
            for c in reversed(range(n)):
                for h in HALVES:
                    b = starts[c] + PAIR * (i - lo) + h
                    acc[lax.div(b, GROUP), lax.div(lax.rem(b, GROUP), RING), lax.rem(b, RING)] = prod[h * BW:h * BW + BW, c * BW:c * BW + BW]
        each(lo, hi, some)
    share_of_new = (1.0 - FACTOR_DECAY) / (ns * n_dp)
    n_pair = (np_in + 1) // PAIR
    start_of = lambda q, of_s: block_at(q, np_in, np_out, of_s)
    def grams(of_s, qs):
        n_pan = np_out if of_s else np_in
        for q in qs:
            both = [x for x in (q, q + 1) if x < n_pan]
            gram(n_pair * of_s + q // PAIR, np_in * of_s, q, n_pan, [start_of(x, of_s) - PAIR * (x - q) for x in both], share_of_new)
    def grads(qs):
        base = (np_in + np_out) * (np_in + np_out + 1) - np_out * n_in
        for q in qs:
            both = [x for x in (q, q + 1) if x < np_out]
            gram(n_pair + q // PAIR, 0, 0, np_in, [base + x * n_in for x in both], 1.0 / (ns * n_dp))

    def share(buf, ms, part, phase, coord):
        c1, e = along(part, 0), along(part, 1)
        if phase == 0:
            return buf.at[ms, part, coord]
        return buf.at[ms, part, c1, rows_at(coord * ROWS, ROWS) if phase == 1 else rows_at(e * ROWS + coord * SUBL, SUBL)]
    def cut(buf, ms, part, phase, coord, half):
        if phase == 0:
            return buf.at[ms, part, coord, pl.ds(half * HALF, HALF)]
        return buf.at[ms, part, along(part, 0), rows_at(coord * ROWS + half * MB, MB)]
    firsts = ((ra, rb), (ra2, rb2))
    seconds = ((rc, rd), (rc2, rd2))
    n_copy = 23
    def round_steps(k):
        m0, m1 = cuts[k], cuts[k + 1]
        ms = pl.ds(m0, m1 - m0)
        late = k == len(cuts) - 2
        def copy(part, kind, phase, i):
            c = along(part, phase)
            step = i + 1 if kind == 2 or kind == 3 and phase == 2 else UPDOWN[i]
            if kind == 0:
                src, dst = cut(acc, ms, part, phase, turn(c, 2), i), firsts[phase][i].at[ms, part]
            elif kind == 1:
                src, dst = share(acc, ms, part, phase, turn(c, step)), seconds[phase][i].at[ms, part]
            elif kind == 2:
                src, dst = share(acc, ms, part, phase, turn(c, step)), r3.at[i, ms, part]
            else:
                src = share(full, ms, part, phase, c) if kind == 3 else cut(full, ms, part, phase, turn(c, 4 - step), i)
                dst = src
            s = (k * 3 + part) * n_copy + (0, 4, 8, 11, 19)[kind] + (PAIR * phase + i if kind < 2 or kind == 4 else 3 * (2 - phase) + i if kind == 3 else i)
            return remote(src, dst, ssem.at[s], rsem.at[s], chip(part, phase, step))
        every, near = PARTS, HALVES
        def go(part, kind, phase, which):
            for i in which:
                copy(part, kind, phase, i).start()
        def come(part, kind, phase, which):
            for i in which:
                copy(part, kind, phase, i).wait_recv()
        def add(part, c1, rows, *srcs):
            def some(m):
                v = acc[m, part, c1, rows]
                for s in srcs:
                    v = v + s(m)
                acc[m, part, c1, rows] = v
            each(m0, m1, some)
        def fold(phase):
            for part in PARTS:
                c = along(part, phase)
                for z in HALVES:
                    come(part, 0, phase, (z,))
                    u = turn(c, UPDOWN[z])
                    buf = firsts[phase][z]
                    if phase == 0:
                        add(part, u, pl.ds(z * HALF, HALF), lambda m: buf[m, part])
                    else:
                        add(part, along(part, 0), rows_at(u * ROWS + z * MB, MB), lambda m: buf[m, part])
                    go(part, 1, phase, (z,))
        def gain(phase):
            for part in PARTS:
                come(part, 1, phase, near)
                b0, b1 = seconds[phase]
                rows = pl.ds(0, BW) if phase == 0 else rows_at(along(part, 1) * ROWS, ROWS)
                add(part, along(part, 0), rows, lambda m: b0[m, part], lambda m: b1[m, part])
                go(part, phase * 2, 1 + phase, every if phase else near)
        def done():
            for part in PARTS:
                come(part, 2, 2, every)
                c1, rows = along(part, 0), mine_rows[part]
                def some(m):
                    v = acc[m, part, c1, rows] + (r3[0, m, part] + r3[1, m, part] + r3[2, m, part])
                    if not late:
                        _, is_g = decode((m * 3 + part) * RING + c1, np_in, np_out)
                        v = v + jnp.where(is_g == 1, 0.0, old[m, part] * FACTOR_DECAY)
                    full[m, part, c1, rows] = v
                each(m0, m1, some)
                go(part, 3, 2, every)
        def widen():
            for part in PARTS:
                come(part, 3, 2, every)
                go(part, 3, 1, near)
        def relay_wide():
            for z in near:
                for part in PARTS:
                    come(part, 3, 1, (z,))
                    go(part, 4, 1, (z,))
        def near_go():
            for part in PARTS:
                come(part, 4, 1, near)
                go(part, 3, 0, near)
        def relay():
            for z in near:
                for part in PARTS:
                    come(part, 3, 0, (z,))
                    go(part, 4, 0, (z,))
        def whole():
            for part in PARTS:
                come(part, 4, 0, near)
                swap(part).start()
                keep(part).start()
        def swap(part):
            return remote(full.at[ms, part], blocks.at[p, ms, part], *both_ends(psem, k, part), partner())
        def keep(part):
            return pltpu.make_async_copy(full.at[ms, part], blocks.at[p, ms, part], psem.at[2, k, part])
        def wide():
            for part in PARTS:
                come(part, 4, 1, near)
                swap_quarter(part).start()
                def some(m):
                    quarter[p, m - m0, part] = full[m, part, along(part, 0)]
                each(m0, m1, some)
        def swap_quarter(part):
            return remote(full.at[ms, part, along(part, 0)], quarter.at[p, :, part], *both_ends(psem, k, part), partner())
        def start():
            for part in PARTS:
                go(part, 0, 0, near)
        kinds = [(0, 0, near), (1, 0, near), (0, 1, near), (1, 1, near), (2, 2, every), (3, 2, every), (3, 1, near), (4, 1, near), (3, 0, near), (4, 0, near)]
        def settle():
            for part in PARTS:
                for kind, phase, which in kinds[:len(kinds) - PAIR * late]:
                    for i in which:
                        copy(part, kind, phase, i).wait_send()
                c = swap_quarter(part) if late else swap(part)
                c.wait_recv()
                c.wait_send()
                if not late:
                    keep(part).wait()
        return [start, lambda: fold(0), lambda: gain(0), lambda: fold(1), lambda: gain(1), done, widen, relay_wide] + ([wide] if late else [near_go, relay, whole]), settle
    rounds = [round_steps(k) for k in range(len(cuts) - 1)]
    chunks = [lambda: grams(1, (0,)), lambda: (grams(1, (2,)), ready(range(np_out, n_col)), grams(0, range(0, np_in, PAIR))), lambda: (grams(1, range(EARLY, np_out, PAIR)), grads((0,))),
        lambda: (grads(range(2, np_out, PAIR)), [c.wait() for c in olds])]
    for k, z in order:
        todo = chunks if k < 0 else rounds[k][0]
        if 0 <= z < len(todo):
            todo[z]()
    for _, settle in rounds:
        settle()

def front(a_loc, g_loc, a_old3, s_old3, n_dp, cuts):
    ns, c_in = a_loc.shape
    np_in, np_out = c_in // PW, g_loc.shape[1] // PW
    V = lambda *s: pltpu.VMEM(s, F32)
    B = lambda *s: pltpu.VMEM(s, BF)
    D = lambda *s: pltpu.SemaphoreType.DMA(s)
    hb = pl.BlockSpec(memory_space=pl.ANY)
    vb = pl.BlockSpec(memory_space=pltpu.VMEM)
    nm = cuts[-1]
    order = [(k, x - lag) for x in range(15) for k, lag in ((-1, 0), (0, 0), (1, 2), (2, 3))]
    slab = lambda n: [V(nm, 3, n, BW)] * 2
    n_col = np_in + np_out
    s_blk, a_blk = s_old3.reshape(-1, BW, BW), a_old3.reshape(-1, BW, BW)
    n_old = -(-block_at(np_out, np_in, np_out, 1) // RING)
    f32 = lambda *s: jax.ShapeDtypeStruct(s, F32)
    return pl.pallas_call(functools.partial(front_kernel, np_in, np_out, n_dp, cuts, order),
        out_shape=(f32(2, cuts[-2], 3, RING, BW, BW), f32(2, nm - cuts[-2], 3, BW, BW)),
        in_specs=[hb] * 4, out_specs=(hb, vb),
        scratch_shapes=[*[V(nm, 3, RING, BW, BW)] * 2, B(n_col * ns // PW, PW, PW), B((np_in + 1) // PAIR + (np_out + 1) // PAIR, ns, PW), B(4, ns, BW), V(cuts[-2], 3, SUBL, BW),
            *slab(HALF), *slab(BW), *slab(MB), *slab(ROWS), V(3, nm, 3, SUBL, BW), D(PAIR * n_col + n_old), *[D(69 * (len(cuts) - 1))] * 2, D(3, len(cuts) - 1, 3)],
        compiler_params=pltpu.CompilerParams(collective_id=0, has_side_effects=True, vmem_limit_bytes=67043328), name="front")(a_loc, g_loc, s_blk, a_blk)

def solve_kernel(np_in, np_out, n_dp, damp, cuts, early, quarter, fin, full, tmat, mat, linv, inv_all, lsp, lspt, xw, zin, pack, ssem, rsem, psem, osem):
    p = lax.axis_index('mp')
    d = lax.axis_index('dp')
    n_own = np_in * BW // n_dp
    n_in, n_out = PAIR * np_in, PAIR * np_out
    first, then = [[pltpu.make_async_copy(early.at[par, pl.ds(cuts[z], cuts[z + 1] - cuts[z])], full.at[par, pl.ds(cuts[z], cuts[z + 1] - cuts[z])], osem.at[z, par]) for par in HALVES] for z in HALVES]
    for c in first + then:
        c.start()
    entry_barrier()
    ms = pl.ds(cuts[-2], cuts[-1] - cuts[-2])
    def last(par, part, z, on):
        c = along(part, 0)
        ref = full.at[par, ms, part, turn(c, 3 - PAIR * z), pl.ds(z * HALF, HALF)] if on else full.at[par, ms, part, c]
        s = 30 + (par * 3 + part) * 4 + PAIR * on + z
        return remote(ref, ref, ssem.at[s], rsem.at[s], chip(part, 0, UPDOWN[z]))
    every = [(z, part, par) for z in HALVES for part in PARTS for par in HALVES]
    @pl.when(p == 1)
    def _():
        for part in PARTS:
            for par in HALVES:
                def put(m):
                    full[par, m, part, along(part, 0)] = quarter[par, m - cuts[-2], part]
                each(cuts[-2], cuts[-1], put)
        for z, part, par in every:
            last(par, part, z, 0).start()
    def wait_for(copies):
        for c in copies:
            c.wait()
    wait_for(first)
    @pl.when(p == 1)
    def _():
        wait_for(then)

    def block(par, b):
        return full[par, lax.div(b, GROUP), lax.div(lax.rem(b, GROUP), RING), lax.rem(b, RING)]

    base_g = np_out * (np_out + 1) + np_in * (np_in + 1)
    npan = np_out - (np_out - np_in) * p
    eye = jnp.where(lax.broadcasted_iota(jnp.int32, (BW, BW), 0) == lax.broadcasted_iota(jnp.int32, (BW, BW), 1), damp, 0.0)

    def load(q):
        base = block_at(q, np_in, np_out, 1 - p)
        slot = lax.rem(q, PAIR)
        for par in HALVES:
            cols = pl.ds(par * BW, BW)
            def rows(i):
                for h in HALVES:
                    tmat[slot, i, h * BW:h * BW + BW, cols] = block(par, base + PAIR * (i - q) + h)
            each(q, npan, rows)
            tmat[slot, q, cols, cols] = tmat[slot, q, cols, cols] + eye

    lsp_spare = lsp.shape[1] - 1
    def ltile(i, k):
        return lax.div(i * (i - 1), PAIR) + k

    def update(i, k, q, ok):
        slot = lax.rem(q, PAIR)
        at = ok * i + (1 - ok) * np_out
        prod = stack_dot(pieces(lsp, ok * ltile(i, k)), pieces(lspt, ok * ltile(q, k)), NN)
        tmat[slot, at] = tmat[slot, at] - prod

    def task(s, q):
        left = jnp.maximum(npan - 1 - q, 1)
        turn = lax.div(s, left)
        ok = (turn <= q).astype(jnp.int32) * jnp.minimum(q, 1) * jnp.minimum(npan - 1 - q, 1)
        k = turn - 1 + q * (1 - jnp.minimum(turn, 1))
        update(q + 1 + lax.rem(s, left), k, q + jnp.minimum(turn, 1), ok)

    load(0)

    def panel(k):
        q = lax.div(k, PAIR)
        h = lax.rem(k, PAIR)
        slot = lax.rem(q, PAIR)
        @pl.when(h == 0)
        def _():
            mat[...] = tmat[slot, q, :BW, :BW]
        factor_block(mat, linv, lambda t: task(h * SUBL + t, q))
        @pl.when(h == 0)
        def _():
            inv0 = linv[...]
            inv0s = split3(inv0)
            l10 = dot6(split3(tmat[slot, q, BW:, :BW]), inv0s, NT)
            l10s = split3(l10)
            mat[...] = tmat[slot, q, BW:, BW:] - dot6(l10s, l10s, NT)
            inv_all[q, :BW, :BW] = inv0
            inv_all[q, :BW, BW:] = jnp.zeros((BW, BW), F32)
            inv_all[q, BW:, :BW] = dot6(l10s, inv0s, NN)
        @pl.when((h == 1) & (q < npan - 1))
        def _():
            each(MB, (npan - 1 - q) * (q + 1), lambda s: task(s, q))
        @pl.when(h == 1)
        def _():
            inv1 = linv[...]
            inv_all[q, BW:, BW:] = inv1
            inv_all[q, BW:, :BW] = -dot6(split3(inv1), split3(inv_all[q, BW:, :BW]), NN)
            invs = split3(inv_all[q].T)
            def below(s):
                i = q + 1 + PAIR * s
                ok = (i + 1 < npan).astype(jnp.int32)
                both = jnp.concatenate([tmat[slot, i], tmat[slot, ok * (i + 1) + (1 - ok) * np_out]], 0)
                low = stack_dot(split3(both), invs, NN)
                at = ltile(i, q), ok * ltile(i + 1, q) + (1 - ok) * lsp_spare
                for u in HALVES:
                    one = low[u * PW:(u + 1) * PW]
                    for ref, v in ((lsp, one), (lspt, one.T)):
                        for z, piece in enumerate(split3(v)):
                            ref[z, at[u]] = piece
            upto(lax.div(npan - q, PAIR), below)
        @pl.when((h == 1) & (q < npan - 1))
        def _():
            @pl.when(q == 0)
            def _():
                load(1)
            update(q + 1, q, q + 1, 1)
            @pl.when(q < npan - 2)
            def _():
                load(q + 2)
    upto(1, panel)
    @pl.when(p == 0)
    def _():
        wait_for(then)
    each(1, PAIR * npan, panel)
    @pl.when(p == 1)
    def _():
        for z, part, par in every:
            last(par, part, z, 0).wait_recv()
            last(par, part, z, 1).start()

    zcopy = remote(zin.at[0], zin.at[1], *both_ends(psem, 1), partner())
    @pl.when(p == 1)
    def _():
        row = lax.broadcasted_iota(jnp.int32, (MB, PW), 0)
        lane = lax.broadcasted_iota(jnp.int32, (MB, PW), 1)
        par = lax.div(row, SUBL)
        idx = lax.rem(row, SUBL)
        col = d * n_own + idx
        for q in range(np_in):
            hit = (idx < n_own) & (lax.div(col, BW) == q) & (lane == par * BW + lax.rem(col, BW))
            xw[q] = jnp.where(hit, 1.0, 0.0)
    @pl.when(p == 0)
    def _():
        zcopy.wait_recv()
        def cp(q):
            xw[q] = zin[1, q]
        upto(np_out, cp)

    def spread(x, lo, hi, tile, ref):
        xs = split3(x)
        def some(i):
            for u in range(RING):
                j = lo + RING * i + u
                ok = (j < hi).astype(jnp.int32)
                at = ok * j + (1 - ok) * np_out
                xw[at] = xw[at] - stack_dot(xs, pieces(ref, ok * tile(j)), NN)
        upto(lax.div(hi - lo + RING - 1, RING), some)
    def fwd(q):
        y = stack_dot(split3(xw[q]), split3(inv_all[q]), NT)
        xw[q] = y
        spread(y, q + 1, npan, lambda j: ltile(j, q), lspt)
    upto(npan, fwd)
    def back(s):
        q = npan - 1 - s
        x = stack_dot(split3(xw[q]), split3(inv_all[q]), NN)
        xw[q] = x
        spread(x, 0, q, lambda j: ltile(q, j), lsp)
    upto(npan, back)

    xcopy = remote(pack.at[1], pack.at[0], *both_ends(psem, 2), partner())
    @pl.when(p == 1)
    def _():
        for z, part, par in every:
            last(par, part, z, 1).wait_recv()
        def zq(q):
            for par in HALVES:
                acc = jnp.zeros((MB, BW), F32)
                for i in range(n_in):
                    acc = acc + stack_dot(split3(xw[i // PAIR, :, (i % PAIR) * BW:(i % PAIR + 1) * BW]), split3(block(par, base_g + q * n_in + i)), NN)
                zin[0, q, :, par * BW:par * BW + BW] = acc
        upto(np_out, zq)
        zcopy.start()
        xcopy.wait_recv()
        zcopy.wait_send()
    @pl.when(p == 0)
    def _():
        for par in reversed(HALVES):
            pack[par, np_out * n_own:] = jnp.zeros((pack.shape[1] - np_out * n_own, PW), F32)
            for q in range(np_out):
                pack[par, q * n_own:(q + 1) * n_own] = xw[q, par * SUBL:par * SUBL + n_own]
            if par == 1:
                xcopy.start()
    n_t = fin.shape[4]
    for t in range(PAIR * (pack.shape[1] // SUBL)):
        part, z = divmod(t, n_t)
        half = t % PAIR
        fin[(part, *(along(part, ph) for ph in PARTS), z)] = pack[0, t // PAIR * SUBL:t // PAIR * SUBL + SUBL, half * BW:half * BW + BW]
    def fcopy(part, j):
        c1, e, f = (along(part, ph) for ph in PARTS)
        if j < 6:
            phase, step = 2 - j // 3, j % 3 + 1
            ref = fin.at[part, c1, e, f] if phase == 2 else fin.at[part, c1, e]
        else:
            z = j % PAIR
            phase, step = 0, UPDOWN[z]
            ref = fin.at[part, c1] if j < 8 else fin.at[part, turn(c1, 3 - PAIR * z), pl.ds(PAIR * z, 2)]
        s = part * 10 + j
        return remote(ref, ref, ssem.at[s], rsem.at[s], chip(part, phase, step))
    def fstep(came, js):
        def part_fn(part):
            for j in came:
                fcopy(part, j).wait_recv()
            for j in js:
                fcopy(part, j).start()
        for part in PARTS:
            part_fn(part)
    fstep((), (0, 1, 2))
    fstep((0, 1, 2), (3, 4, 5))
    fstep((3, 4, 5), (6, 7))
    def frelay(part):
        for z in HALVES:
            fcopy(part, 6 + z).wait_recv()
            fcopy(part, 8 + z).start()
    for part in PARTS:
        frelay(part)
    fstep((8, 9), ())
    for part in PARTS:
        for j in range(10):
            fcopy(part, j).wait_send()
    @pl.when(p == 1)
    def _():
        for z, part, par in every:
            last(par, part, z, 0).wait_send()
            last(par, part, z, 1).wait_send()
    @pl.when(p == 0)
    def _():
        xcopy.wait_send()

def solve(early, quarter, np_in, np_out, n_dp, damp, cuts):
    n_own = np_in * BW // n_dp
    n_row = -(-np_out * n_own // SUBL)
    n_t = -(-PAIR * n_row // 3)
    n_tile = np_out * (np_out - 1) // PAIR + 1
    V = lambda *s: pltpu.VMEM(s, F32)
    D = lambda *s: pltpu.SemaphoreType.DMA(s)
    hb = pl.BlockSpec(memory_space=pl.ANY)
    vb = pl.BlockSpec(memory_space=pltpu.VMEM)
    f32 = lambda *s: jax.ShapeDtypeStruct(s, F32)
    return pl.pallas_call(functools.partial(solve_kernel, np_in, np_out, n_dp, damp, cuts),
        out_shape=f32(3, RING, RING, RING, n_t, SUBL, BW), in_specs=[hb, vb], out_specs=vb,
        scratch_shapes=[V(2, cuts[-1], 3, RING, BW, BW), V(2, np_out + 1, PW, PW), V(BW, BW), V(BW, BW), V(np_out, PW, PW), *[pltpu.VMEM((3, n_tile, PW, PW), BF)] * 2, V(np_out + 1, MB, PW),
            V(2, np_out, MB, PW), V(2, n_row * SUBL, PW), D(54), D(54), D(2, 3), D(2, 2)],
        compiler_params=pltpu.CompilerParams(collective_id=1, has_side_effects=True, vmem_limit_bytes=67043328), name="solve")(early, quarter)

def finish_kernel(np_in, np_out, n_own, w_hbm, blocks, fin, w_out, a_out, s_out, wbuf, gath, cols_s, cols_a, up_s, up_a, isem, lsem, usem, wsem, csem):
    p = lax.axis_index('mp')
    wload = pltpu.make_async_copy(w_hbm, wbuf, isem)
    wload.start()
    sets = [(s_out, cols_s, up_s, np_out, 1), (a_out, cols_a, up_a, np_in, 0)]
    jobs, n = [], 0
    for out, cols, up, n_pan, of_s in sets:
        for q in range(n_pan):
            base = block_at(q, np_in, np_out, of_s) // PAIR
            low = pltpu.make_async_copy(blocks.at[p, pl.ds(base, n_pan - q)], cols.at[q, pl.ds(q, n_pan - q)], lsem.at[n])
            ups = [pltpu.make_async_copy(blocks.at[par, pl.ds(base + 1, n_pan - 1 - q), p], up.at[par, q, pl.ds(q + 1, n_pan - 1 - q)], usem.at[par, n]) for par in HALVES] if q < n_pan - 1 else []
            send = pltpu.make_async_copy(cols.at[q], out.at[q], csem.at[n])
            jobs.append((low, ups, send, cols, up, q))
            n += 1
    for low, ups, *_ in jobs:
        for c in (*ups, low):
            c.start()
    n_t = fin.shape[4]
    def tile(t, c):
        part, z = divmod(t, n_t)
        return fin[(part, *(c + c)[part:part + 3], z)]
    wload.wait()
    def weights(q):
        lo, hi = q * n_own // SUBL, ((q + 1) * n_own - 1) // SUBL
        for half in HALVES:
            def fill(z):
              for y in range(RING):
                vals = []
                for x in range(RING):
                    c = (x, y, z)
                    v = jnp.concatenate([tile(PAIR * r + half, c) for r in range(lo, hi + 1)], 0)
                    at = q * n_own - lo * SUBL
                    vals.append(v[at:at + n_own])
                gath[rows_at((z * RING + y) * RING * n_own, RING * n_own)] = jnp.concatenate(vals, 0)
            upto(RING, fill)
            for b in range(np_in):
                r = slice((PAIR * q + half) * BW, (PAIR * q + half + 1) * BW)
                wbuf[b, r] = wbuf[b, r] - LEARN_RATE * gath[b * BW:b * BW + BW].T
    for q in range(np_out // PAIR):
        weights(q)
    for low, ups, send, cols, up, q in jobs:
        low.wait()
        for c in ups:
            c.wait()
    for low, ups, send, cols, up, q in jobs:
        for q2 in range(q):
            for par in HALVES:
                cols[q, q2, par] = up[par, q2, q].T
        send.start()
    for q in range(np_out // PAIR, np_out):
        weights(q)
    wsend = pltpu.make_async_copy(wbuf, w_out, wsem)
    wsend.start()
    for low, ups, send, *_ in jobs:
        send.wait()
    wsend.wait()

def finish(w3, blocks, fin, np_in, np_out, n_dp):
    V = pltpu.VMEM
    D = pltpu.SemaphoreType.DMA
    hb = pl.BlockSpec(memory_space=pl.ANY)
    vb = pl.BlockSpec(memory_space=V)
    n_job = np_in + np_out
    square = lambda n: (n, n, 2, BW, BW)
    w_new, a_new, s_new = pl.pallas_call(functools.partial(finish_kernel, np_in, np_out, np_in * BW // n_dp),
        out_shape=(jax.ShapeDtypeStruct(w3.shape, F32), jax.ShapeDtypeStruct(square(np_in), F32), jax.ShapeDtypeStruct(square(np_out), F32)),
        in_specs=[hb, hb, vb], out_specs=(hb, hb, hb),
        scratch_shapes=[V(w3.shape, F32), V((np_in * BW, BW), F32), V(square(np_out), F32), V(square(np_in), F32), V((2, np_out, np_out, BW, BW), F32), V((2, np_in, np_in, BW, BW), F32),
            D, D((n_job,)), D((2, n_job)), D, D((n_job,))],
        compiler_params=pltpu.CompilerParams(vmem_limit_bytes=63 * 2**20), name="outputs")(w3, blocks.reshape(2, -1, 2, BW, BW), fin)
    return w_new, a_new.reshape(np_in, -1, BW), s_new.reshape(np_out, -1, BW)


def solution(mesh):
    n_dp = mesh.shape['dp']

    def local_step(a_loc, g_loc, w_loc, a_old_loc, s_old_loc):
        np_in = a_loc.shape[1] // PW
        np_out = g_loc.shape[1] // PW
        n_in, n_out = PAIR * np_in, PAIR * np_out
        early = np_in * (np_in + 1) + np_out * (np_out + 1)
        cuts = (0, 2, -(-early // GROUP), (early + n_in * np_out) // GROUP)
        panels = lambda x: x.transpose(1, 0, 2)
        blocks, quarter = front(a_loc, g_loc, panels(a_old_loc), panels(s_old_loc), n_dp, cuts)
        fin = solve(blocks, quarter, np_in, np_out, n_dp, DAMP_SHIFT, cuts)
        return tuple(panels(x) for x in finish(panels(w_loc), blocks, fin, np_in, np_out, n_dp))

    spec_rows = P('dp', None)
    spec_cyc = P(None, 'mp', None)
    return jax.shard_map(local_step, mesh=mesh, in_specs=(spec_rows, spec_rows, spec_cyc, spec_cyc, spec_cyc), out_specs=(spec_cyc, spec_cyc, spec_cyc), check_vma=False)
```

```python
import functools
import math
import jax
import jax.numpy as jnp
from jax import lax
from jax.experimental import pallas as pl
from jax.experimental.pallas import tpu as pltpu
from jax.sharding import PartitionSpec as P

BW = 128
PW = 256
RING = 4
SUBL = 8
HALF = 64
ROWS = 32
GROUP = 12
EARLY = 4
PAIR = 2
HALVES = (0, 1)
UPDOWN = (1, 3)
PARTS = (0, 1, 2)
FACTOR_DECAY = 0.95
LEARN_RATE = 1.0
DAMPING = 0.001
DAMP_SHIFT = math.sqrt(DAMPING)
MB = 16
F32 = jnp.float32
BF = jnp.bfloat16
NT = (((1,), (1,)), ((), ()))
NN = (((1,), (0,)), ((), ()))


def split3(x):
    h = x.astype(BF)
    r = x - h.astype(F32)
    m = r.astype(BF)
    return h, m, (r - m.astype(F32)).astype(BF)

def bc(x):
    return jnp.broadcast_to(x, (MB, BW))

def factor_block(mat, linv, beside=None):
    lane = lax.broadcasted_iota(jnp.int32, (MB, BW), 1)
    sub = lax.broadcasted_iota(jnp.int32, (MB, BW), 0)
    odd = lax.rem(sub, PAIR)
    zero = lane.astype(F32) * 0.0
    ri = lax.broadcasted_iota(jnp.int32, (BW, BW), 0)
    ci = lax.broadcasted_iota(jnp.int32, (BW, BW), 1)
    whole = mat[...]
    diag = jnp.where(ci == ri, whole, 0.0)
    down, along_row = lax.rsqrt(jnp.sum(diag, axis=1, keepdims=True)), lax.rsqrt(jnp.sum(diag, axis=0, keepdims=True))
    mat[...] = whole * down * along_row
    rows = mat[:MB]
    for t in range(BW // MB):
        k = t * MB
        if beside is not None:
            beside(t)
        cols = jnp.concatenate([bc(rows[:, k + i:k + i + 1]) for i in range(MB)], 0).reshape(MB, MB, BW) + zero
        inside = (lane >= k) & (lane < k + MB)
        ext = jnp.where(inside, jnp.where(lane == sub + k, 1.0, 0.0), rows)
        more = k + MB < BW
        far = k + MB + MB < BW
        if more:
            near = mat[k + MB:k + MB + MB]
            mult = [bc(near[:, k + i:k + i + 1]) for i in range(MB)]
        if far:
            rh, rm, rl = split3(rows)
            left = jnp.concatenate([rh, rh, rm, rh, rl, rm], 0).T[k + MB + MB:]
        dg = of = None
        for j in range(0, MB, PAIR):
            u, v = cols[0], cols[1]
            a, b, c = bc(u[j:j + 1]), bc(u[j + 1:j + 2]), bc(v[j + 1:j + 2])
            det = a * c - b * b
            rdet = 1.0 / det
            ra = 1.0 / a
            e0, e1 = bc(ext[j:j + 1]), bc(ext[j + 1:j + 2])
            linv[k + j:k + j + 1] = (e0 * lax.rsqrt(a))[:1]
            linv[k + j + 1:k + j + 2] = ((e1 - (b * ra) * e0) * lax.rsqrt(det * ra))[:1]
            pair = (sub == j) | (sub == j + 1)
            u, v = jnp.where(pair, 0.0, u), jnp.where(pair, 0.0, v)
            n0, n1 = c * u - b * v, a * v - b * u
            f0, f1 = n0 * rdet, n1 * rdet
            if j + 2 < MB:
                left_cols = cols[2:]
                soon = left_cols[:2]
                soon = soon - (n0 * jnp.broadcast_to(soon[:, j:j + 1], soon.shape) + n1 * jnp.broadcast_to(soon[:, j + 1:j + 2], soon.shape)) * rdet
                if j + 4 < MB:
                    late = left_cols[2:]
                    late = late - (f0 * jnp.broadcast_to(late[:, j:j + 1], late.shape) + f1 * jnp.broadcast_to(late[:, j + 1:j + 2], late.shape))
                    cols = jnp.concatenate([soon, late], 0)
                else:
                    cols = soon
            ext = ext - (f0 * e0 + f1 * e1)
            d_here = jnp.where(odd == 0, c, a) * rdet
            dg = d_here if dg is None else jnp.where(sub >= j, d_here, dg)
            of = b * rdet if of is None else jnp.where(sub >= j, b * rdet, of)
        w = ext * dg - jnp.where(odd == 0, jnp.roll(ext, -1, 0), jnp.roll(ext, 1, 0)) * of
        if far:
            wh, wm, wl = split3(w)
            prod = lax.dot_general(left, jnp.concatenate([wh, wm, wh, wl, wh, wm], 0), NN, preferred_element_type=F32)
            ins = jnp.broadcast_to(inside[:1], prod.shape)
            mat[k + MB + MB:] = jnp.where(ins, 0.0, mat[k + MB + MB:]) - prod
        if more:
            terms = [mult[j] * bc(w[j:j + 1]) for j in range(MB)]
            while len(terms) > 1:
                terms = [x + y for x, y in zip(terms[::PAIR], terms[1::PAIR])]
            rows = jnp.where(inside, 0.0, near) - terms[0]
    linv[...] = jnp.where(ci <= ri, linv[...], 0.0) * along_row


def dot6(a, b, dims):
    d = lambda x, y: lax.dot_general(x, y, dims, preferred_element_type=F32)
    ah, am, al = a
    bh, bm, bl = b
    return (d(am, bm) + d(ah, bl) + d(al, bh)) + (d(ah, bm) + d(am, bh)) + d(ah, bh)

def stack_dot(x, w, dims):
    xh, xm, xl = x
    wh, wm, wl = w
    k = xh.shape[0]
    d = lambda u, v: lax.dot_general(u, v, dims, preferred_element_type=F32)
    p1 = d(jnp.concatenate([xh, xm, xl], 0), wh)
    p2 = d(jnp.concatenate([xh, xm], 0), wm)
    p3 = d(xh, wl)
    return (p1[k + k:] + p2[k:] + p3) + (p1[k:k + k] + p2[:k]) + p1[:k]

def pieces(ref, at):
    return [ref[z, at] for z in PARTS]

def each(lo, hi, fn):
    def body(i, c):
        fn(i)
        return c
    lax.fori_loop(lo, hi, body, 0)

def upto(n, fn):
    each(0, n, fn)

def rows_at(start, size):
    return pl.ds(pl.multiple_of(start, SUBL), size)

def turn(c, step):
    return lax.rem(c + step, RING)

def place(part, phase):
    stride = RING**((part + phase) % 3)
    return lax.rem(lax.div(lax.axis_index('dp'), stride), RING), stride

def remote(src, dst, ssem, rsem, where):
    return pltpu.make_async_remote_copy(src_ref=src, dst_ref=dst, send_sem=ssem, recv_sem=rsem, device_id=where, device_id_type=pl.DeviceIdType.MESH)

def along(part, phase):
    return place(part, phase)[0]

def both_ends(sems, *at):
    return sems.at[(0, *at)], sems.at[(1, *at)]

def chip(part, phase, step):
    c, stride = place(part, phase)
    return {'dp': lax.axis_index('dp') + (turn(c, step) - c) * stride}

def partner():
    return {'mp': 1 - lax.axis_index('mp')}

def entry_barrier():
    sem = pltpu.get_barrier_semaphore()
    where = [chip(part, 0, step + 1) for part in PARTS for step in PARTS] + [partner()]
    for dev in where:
        pl.semaphore_signal(sem, inc=1, device_id=dev, device_id_type=pl.DeviceIdType.MESH)
    pl.semaphore_wait(sem, len(where))

def block_at(q, np_in, np_out, of_s):
    n_in, n_out = PAIR * np_in, PAIR * np_out
    past = min(q // EARLY, 1) if isinstance(q, int) else jnp.minimum(lax.div(q, EARLY), 1)
    in_s = q * n_out - q * (q - 1) + np_in * (np_in + 1) * past
    in_a = EARLY * n_out - EARLY * (EARLY - 1) + q * n_in - q * (q - 1)
    return of_s * in_s + (1 - of_s) * in_a

def decode(b, np_in, np_out):
    n_in, n_out = PAIR * np_in, PAIR * np_out
    at, was = 0, (0, 0)
    row, col = b, 0
    for q, in_s in [(q, 1) for q in range(EARLY)] + [(q, 0) for q in range(np_in)] + [(q, 1) for q in range(EARLY, np_out)]:
        now = (in_s * n_in + PAIR * q - at, in_s * np_in + q)
        hit = (b >= at).astype(jnp.int32)
        row = row + hit * (now[0] - was[0])
        col = col + hit * (now[1] - was[1])
        was = now
        at += in_s * n_out + (1 - in_s) * n_in - PAIR * q
    is_g = (b >= at).astype(jnp.int32)
    off = (b - at) * is_g
    row = row + is_g * (lax.rem(off, n_in) - row)
    col = jnp.minimum(col + is_g * (np_in + lax.div(off, n_in) - col), np_in + np_out - 1)
    in_s = (col >= np_in).astype(jnp.int32)
    old = in_s * ((col - np_in) * n_out + row - n_in) + (1 - in_s) * (col * n_in + row)
    return (1 - is_g) * old, is_g

def front_kernel(np_in, np_out, n_dp, cuts, order, a_hbm, g_hbm, s_hbm, ao_hbm, blocks, quarter, acc, full, agt, own, flip, old, ra, rb, rc, rd, ra2, rb2, rc2, rd2, r3, lsem, ssem, rsem, psem):
    p = lax.axis_index('mp')
    ns = a_hbm.shape[0]
    n_in, n_out = PAIR * np_in, PAIR * np_out
    n_col = np_in + np_out
    n_slot = flip.shape[0]

    def column(i, par):
        src, q = (a_hbm, i) if i < np_in else (g_hbm, i - np_in)
        return src.at[:, pl.ds(pl.multiple_of((PAIR * q + par) * BW, BW), BW)]
    def pair_of(i):
        return (i // PAIR, i % PAIR) if i < np_in else ((np_in + 1) // PAIR + (i - np_in) // PAIR, (i - np_in) % PAIR)
    def mine_at(i):
        z, h = pair_of(i)
        return own.at[z, :, h * BW:h * BW + BW]
    mine = [pltpu.make_async_copy(column(i, p), mine_at(i), lsem.at[i]) for i in range(n_col)]
    turns = [*range(np_in, n_col), *range(np_in)]
    theirs = [pltpu.make_async_copy(column(i, 1 - p), flip.at[z % n_slot], lsem.at[n_col + i]) for z, i in enumerate(turns)]
    of_a = range(block_at(0, np_in, np_out, 0), block_at(np_in, np_in, np_out, 0))
    n_old = block_at(np_out, np_in, np_out, 1)
    mine_rows = [rows_at(along(part, 1) * ROWS + along(part, 2) * SUBL, SUBL) for part in PARTS]
    olds = []
    for j in range(-(-n_old // RING)):
        m, part = divmod(j, 3)
        at, _ = decode(j * RING + along(part, 0), np_in, np_out)
        src = ao_hbm if j * RING in of_a else s_hbm
        olds.append(pltpu.make_async_copy(src.at[at, mine_rows[part]], old.at[m, part], lsem.at[PAIR * n_col + j]))
    for c in theirs[:n_slot] + mine[np_in:] + mine[:np_in]:
        c.start()
    entry_barrier()
    def transpose(src, i, par):
        for kc in range(ns // PW):
            agt[i * (ns // PW) + kc, pl.ds(pl.multiple_of(par * BW, BW), BW), :] = src[kc * PW:kc * PW + PW, :].T
    def ready(zs):
        for z in zs:
            i = turns[z]
            theirs[z].wait()
            transpose(flip.at[z % n_slot], i, 1 - p)
            if z + n_slot < n_col:
                theirs[z + n_slot].start()
        for z in zs:
            mine[turns[z]].wait()
            transpose(mine_at(turns[z]), turns[z], p)
    ready(range(np_out))
    for c in olds:
        c.start()

    def gram(z, row0, lo, hi, starts, scale):
        n = len(starts)
        rhs = own.at[z, :, :n * BW]
        def some(i):
            lhs = jnp.concatenate([agt[(row0 + i) * (ns // PW) + kc] for kc in range(ns // PW)], 1)
            prod = lax.dot_general(lhs, rhs[...], NN, preferred_element_type=F32) * scale
            for c in reversed(range(n)):
                for h in HALVES:
                    b = starts[c] + PAIR * (i - lo) + h
                    acc[lax.div(b, GROUP), lax.div(lax.rem(b, GROUP), RING), lax.rem(b, RING)] = prod[h * BW:h * BW + BW, c * BW:c * BW + BW]
        each(lo, hi, some)
    share_of_new = (1.0 - FACTOR_DECAY) / (ns * n_dp)
    n_pair = (np_in + 1) // PAIR
    start_of = lambda q, of_s: block_at(q, np_in, np_out, of_s)
    def grams(of_s, qs):
        n_pan = np_out if of_s else np_in
        for q in qs:
            both = [x for x in (q, q + 1) if x < n_pan]
            gram(n_pair * of_s + q // PAIR, np_in * of_s, q, n_pan, [start_of(x, of_s) - PAIR * (x - q) for x in both], share_of_new)
    def grads(qs):
        base = (np_in + np_out) * (np_in + np_out + 1) - np_out * n_in
        for q in qs:
            both = [x for x in (q, q + 1) if x < np_out]
            gram(n_pair + q // PAIR, 0, 0, np_in, [base + x * n_in for x in both], 1.0 / (ns * n_dp))

    def share(buf, ms, part, phase, coord):
        c1, e = along(part, 0), along(part, 1)
        if phase == 0:
            return buf.at[ms, part, coord]
        return buf.at[ms, part, c1, rows_at(coord * ROWS, ROWS) if phase == 1 else rows_at(e * ROWS + coord * SUBL, SUBL)]
    def cut(buf, ms, part, phase, coord, half):
        if phase == 0:
            return buf.at[ms, part, coord, pl.ds(half * HALF, HALF)]
        return buf.at[ms, part, along(part, 0), rows_at(coord * ROWS + half * MB, MB)]
    firsts = ((ra, rb), (ra2, rb2))
    seconds = ((rc, rd), (rc2, rd2))
    n_copy = 23
    def round_steps(k):
        m0, m1 = cuts[k], cuts[k + 1]
        ms = pl.ds(m0, m1 - m0)
        late = k == len(cuts) - 2
        def copy(part, kind, phase, i):
            c = along(part, phase)
            step = i + 1 if kind == 2 or kind == 3 and phase == 2 else UPDOWN[i]
            if kind == 0:
                src, dst = cut(acc, ms, part, phase, turn(c, 2), i), firsts[phase][i].at[ms, part]
            elif kind == 1:
                src, dst = share(acc, ms, part, phase, turn(c, step)), seconds[phase][i].at[ms, part]
            elif kind == 2:
                src, dst = share(acc, ms, part, phase, turn(c, step)), r3.at[i, ms, part]
            else:
                src = share(full, ms, part, phase, c) if kind == 3 else cut(full, ms, part, phase, turn(c, 4 - step), i)
                dst = src
            s = (k * 3 + part) * n_copy + (0, 4, 8, 11, 19)[kind] + (PAIR * phase + i if kind < 2 or kind == 4 else 3 * (2 - phase) + i if kind == 3 else i)
            return remote(src, dst, ssem.at[s], rsem.at[s], chip(part, phase, step))
        every, near = PARTS, HALVES
        def go(part, kind, phase, which):
            for i in which:
                copy(part, kind, phase, i).start()
        def come(part, kind, phase, which):
            for i in which:
                copy(part, kind, phase, i).wait_recv()
        def add(part, c1, rows, *srcs):
            def some(m):
                v = acc[m, part, c1, rows]
                for s in srcs:
                    v = v + s(m)
                acc[m, part, c1, rows] = v
            each(m0, m1, some)
        def fold(phase):
            for part in PARTS:
                c = along(part, phase)
                for z in HALVES:
                    come(part, 0, phase, (z,))
                    u = turn(c, UPDOWN[z])
                    buf = firsts[phase][z]
                    if phase == 0:
                        add(part, u, pl.ds(z * HALF, HALF), lambda m: buf[m, part])
                    else:
                        add(part, along(part, 0), rows_at(u * ROWS + z * MB, MB), lambda m: buf[m, part])
                    go(part, 1, phase, (z,))
        def gain(phase):
            for part in PARTS:
                come(part, 1, phase, near)
                b0, b1 = seconds[phase]
                rows = pl.ds(0, BW) if phase == 0 else rows_at(along(part, 1) * ROWS, ROWS)
                add(part, along(part, 0), rows, lambda m: b0[m, part], lambda m: b1[m, part])
                go(part, phase * 2, 1 + phase, every if phase else near)
        def done():
            for part in PARTS:
                come(part, 2, 2, every)
                c1, rows = along(part, 0), mine_rows[part]
                def some(m):
                    v = acc[m, part, c1, rows] + (r3[0, m, part] + r3[1, m, part] + r3[2, m, part])
                    if not late:
                        _, is_g = decode((m * 3 + part) * RING + c1, np_in, np_out)
                        v = v + jnp.where(is_g == 1, 0.0, old[m, part] * FACTOR_DECAY)
                    full[m, part, c1, rows] = v
                each(m0, m1, some)
                go(part, 3, 2, every)
        def widen():
            for part in PARTS:
                come(part, 3, 2, every)
                go(part, 3, 1, near)
        def relay_wide():
            for z in near:
                for part in PARTS:
                    come(part, 3, 1, (z,))
                    go(part, 4, 1, (z,))
        def near_go():
            for part in PARTS:
                come(part, 4, 1, near)
                go(part, 3, 0, near)
        def relay():
            for z in near:
                for part in PARTS:
                    come(part, 3, 0, (z,))
                    go(part, 4, 0, (z,))
        def whole():
            for part in PARTS:
                come(part, 4, 0, near)
                swap(part).start()
                keep(part).start()
        def swap(part):
            return remote(full.at[ms, part], blocks.at[p, ms, part], *both_ends(psem, k, part), partner())
        def keep(part):
            return pltpu.make_async_copy(full.at[ms, part], blocks.at[p, ms, part], psem.at[2, k, part])
        def wide():
            for part in PARTS:
                come(part, 4, 1, near)
                swap_quarter(part).start()
                def some(m):
                    quarter[p, m - m0, part] = full[m, part, along(part, 0)]
                each(m0, m1, some)
        def swap_quarter(part):
            return remote(full.at[ms, part, along(part, 0)], quarter.at[p, :, part], *both_ends(psem, k, part), partner())
        def start():
            for part in PARTS:
                go(part, 0, 0, near)
        kinds = [(0, 0, near), (1, 0, near), (0, 1, near), (1, 1, near), (2, 2, every), (3, 2, every), (3, 1, near), (4, 1, near), (3, 0, near), (4, 0, near)]
        def settle():
            for part in PARTS:
                for kind, phase, which in kinds[:len(kinds) - PAIR * late]:
                    for i in which:
                        copy(part, kind, phase, i).wait_send()
                c = swap_quarter(part) if late else swap(part)
                c.wait_recv()
                c.wait_send()
                if not late:
                    keep(part).wait()
        return [start, lambda: fold(0), lambda: gain(0), lambda: fold(1), lambda: gain(1), done, widen, relay_wide] + ([wide] if late else [near_go, relay, whole]), settle
    rounds = [round_steps(k) for k in range(len(cuts) - 1)]
    chunks = [lambda: grams(1, (0,)), lambda: (grams(1, (2,)), ready(range(np_out, n_col)), grams(0, range(0, np_in, PAIR))), lambda: (grams(1, range(EARLY, np_out, PAIR)), grads((0,))),
        lambda: (grads(range(2, np_out, PAIR)), [c.wait() for c in olds])]
    for k, z in order:
        todo = chunks if k < 0 else rounds[k][0]
        if 0 <= z < len(todo):
            todo[z]()
    for _, settle in rounds:
        settle()

def front(a_loc, g_loc, a_old3, s_old3, n_dp, cuts):
    ns, c_in = a_loc.shape
    np_in, np_out = c_in // PW, g_loc.shape[1] // PW
    V = lambda *s: pltpu.VMEM(s, F32)
    B = lambda *s: pltpu.VMEM(s, BF)
    D = lambda *s: pltpu.SemaphoreType.DMA(s)
    hb = pl.BlockSpec(memory_space=pl.ANY)
    vb = pl.BlockSpec(memory_space=pltpu.VMEM)
    nm = cuts[-1]
    order = [(k, x - lag) for x in range(15) for k, lag in ((-1, 0), (0, 0), (1, 2), (2, 3))]
    slab = lambda n: [V(nm, 3, n, BW)] * 2
    n_col = np_in + np_out
    s_blk, a_blk = s_old3.reshape(-1, BW, BW), a_old3.reshape(-1, BW, BW)
    n_old = -(-block_at(np_out, np_in, np_out, 1) // RING)
    f32 = lambda *s: jax.ShapeDtypeStruct(s, F32)
    return pl.pallas_call(functools.partial(front_kernel, np_in, np_out, n_dp, cuts, order),
        out_shape=(f32(2, cuts[-2], 3, RING, BW, BW), f32(2, nm - cuts[-2], 3, BW, BW)),
        in_specs=[hb] * 4, out_specs=(hb, vb),
        scratch_shapes=[*[V(nm, 3, RING, BW, BW)] * 2, B(n_col * ns // PW, PW, PW), B((np_in + 1) // PAIR + (np_out + 1) // PAIR, ns, PW), B(4, ns, BW), V(cuts[-2], 3, SUBL, BW),
            *slab(HALF), *slab(BW), *slab(MB), *slab(ROWS), V(3, nm, 3, SUBL, BW), D(PAIR * n_col + n_old), *[D(69 * (len(cuts) - 1))] * 2, D(3, len(cuts) - 1, 3)],
        compiler_params=pltpu.CompilerParams(collective_id=0, has_side_effects=True, vmem_limit_bytes=67043328), name="front")(a_loc, g_loc, s_blk, a_blk)

def solve_kernel(np_in, np_out, n_dp, damp, cuts, early, quarter, fin, full, tmat, mat, linv, inv_all, lsp, lspt, xw, zin, pack, ssem, rsem, psem, osem):
    p = lax.axis_index('mp')
    d = lax.axis_index('dp')
    n_own = np_in * BW // n_dp
    n_in, n_out = PAIR * np_in, PAIR * np_out
    first, then = [[pltpu.make_async_copy(early.at[par, pl.ds(cuts[z], cuts[z + 1] - cuts[z])], full.at[par, pl.ds(cuts[z], cuts[z + 1] - cuts[z])], osem.at[z, par]) for par in HALVES] for z in HALVES]
    for c in first + then:
        c.start()
    entry_barrier()
    ms = pl.ds(cuts[-2], cuts[-1] - cuts[-2])
    def last(par, part, z, on):
        c = along(part, 0)
        ref = full.at[par, ms, part, turn(c, 3 - PAIR * z), pl.ds(z * HALF, HALF)] if on else full.at[par, ms, part, c]
        s = 30 + (par * 3 + part) * 4 + PAIR * on + z
        return remote(ref, ref, ssem.at[s], rsem.at[s], chip(part, 0, UPDOWN[z]))
    every = [(z, part, par) for z in HALVES for part in PARTS for par in HALVES]
    @pl.when(p == 1)
    def _():
        for part in PARTS:
            for par in HALVES:
                def put(m):
                    full[par, m, part, along(part, 0)] = quarter[par, m - cuts[-2], part]
                each(cuts[-2], cuts[-1], put)
        for z, part, par in every:
            last(par, part, z, 0).start()
    def wait_for(copies):
        for c in copies:
            c.wait()
    wait_for(first)
    @pl.when(p == 1)
    def _():
        wait_for(then)

    def block(par, b):
        return full[par, lax.div(b, GROUP), lax.div(lax.rem(b, GROUP), RING), lax.rem(b, RING)]

    base_g = np_out * (np_out + 1) + np_in * (np_in + 1)
    npan = np_out - (np_out - np_in) * p
    eye = jnp.where(lax.broadcasted_iota(jnp.int32, (BW, BW), 0) == lax.broadcasted_iota(jnp.int32, (BW, BW), 1), damp, 0.0)

    def load(q):
        base = block_at(q, np_in, np_out, 1 - p)
        slot = lax.rem(q, PAIR)
        for par in HALVES:
            cols = pl.ds(par * BW, BW)
            def rows(i):
                for h in HALVES:
                    tmat[slot, i, h * BW:h * BW + BW, cols] = block(par, base + PAIR * (i - q) + h)
            each(q, npan, rows)
            tmat[slot, q, cols, cols] = tmat[slot, q, cols, cols] + eye

    lsp_spare = lsp.shape[1] - 1
    def ltile(i, k):
        return lax.div(i * (i - 1), PAIR) + k

    def update(i, k, q, ok):
        slot = lax.rem(q, PAIR)
        at = ok * i + (1 - ok) * np_out
        prod = stack_dot(pieces(lsp, ok * ltile(i, k)), pieces(lspt, ok * ltile(q, k)), NN)
        tmat[slot, at] = tmat[slot, at] - prod

    def task(s, q):
        left = jnp.maximum(npan - 1 - q, 1)
        turn = lax.div(s, left)
        ok = (turn <= q).astype(jnp.int32) * jnp.minimum(q, 1) * jnp.minimum(npan - 1 - q, 1)
        k = turn - 1 + q * (1 - jnp.minimum(turn, 1))
        update(q + 1 + lax.rem(s, left), k, q + jnp.minimum(turn, 1), ok)

    load(0)

    def panel(k, *work):
        q = lax.div(k, PAIR)
        h = lax.rem(k, PAIR)
        slot = lax.rem(q, PAIR)
        @pl.when(h == 0)
        def _():
            mat[...] = tmat[slot, q, :BW, :BW]
        factor_block(mat, linv, lambda t: [fn(h * SUBL + t, q) for fn in work])
        @pl.when(h == 0)
        def _():
            inv0 = linv[...]
            inv0s = split3(inv0)
            l10 = dot6(split3(tmat[slot, q, BW:, :BW]), inv0s, NT)
            l10s = split3(l10)
            mat[...] = tmat[slot, q, BW:, BW:] - dot6(l10s, l10s, NT)
            inv_all[q, :BW, :BW] = inv0
            inv_all[q, :BW, BW:] = jnp.zeros((BW, BW), F32)
            inv_all[q, BW:, :BW] = dot6(l10s, inv0s, NN)
        @pl.when((h == 1) & (q < npan - 1))
        def _():
            each(MB, (npan - 1 - q) * (q + 1), lambda s: task(s, q))
        @pl.when(h == 1)
        def _():
            inv1 = linv[...]
            inv_all[q, BW:, BW:] = inv1
            inv_all[q, BW:, :BW] = -dot6(split3(inv1), split3(inv_all[q, BW:, :BW]), NN)
            invs = split3(inv_all[q].T)
            def below(s):
                i = q + 1 + PAIR * s
                ok = (i + 1 < npan).astype(jnp.int32)
                both = jnp.concatenate([tmat[slot, i], tmat[slot, ok * (i + 1) + (1 - ok) * np_out]], 0)
                low = stack_dot(split3(both), invs, NN)
                at = ltile(i, q), ok * ltile(i + 1, q) + (1 - ok) * lsp_spare
                for u in HALVES:
                    one = low[u * PW:(u + 1) * PW]
                    for ref, v in ((lsp, one), (lspt, one.T)):
                        for z, piece in enumerate(split3(v)):
                            ref[z, at[u]] = piece
            upto(lax.div(npan - q, PAIR), below)
        @pl.when((h == 1) & (q < npan - 1))
        def _():
            @pl.when(q == 0)
            def _():
                load(1)
            update(q + 1, q, q + 1, 1)
            @pl.when(q < npan - 2)
            def _():
                load(q + 2)
    upto(1, panel)
    @pl.when(p == 0)
    def _():
        wait_for(then)
    each(1, PAIR * npan, lambda k: panel(k, task))
    @pl.when(p == 1)
    def _():
        for z, part, par in every:
            last(par, part, z, 0).wait_recv()
            last(par, part, z, 1).start()

    zcopy = remote(zin.at[0], zin.at[1], *both_ends(psem, 1), partner())
    @pl.when(p == 1)
    def _():
        row = lax.broadcasted_iota(jnp.int32, (MB, PW), 0)
        lane = lax.broadcasted_iota(jnp.int32, (MB, PW), 1)
        par = lax.div(row, SUBL)
        idx = lax.rem(row, SUBL)
        col = d * n_own + idx
        for q in range(np_in):
            hit = (idx < n_own) & (lax.div(col, BW) == q) & (lane == par * BW + lax.rem(col, BW))
            xw[q] = jnp.where(hit, 1.0, 0.0)
    @pl.when(p == 0)
    def _():
        zcopy.wait_recv()
        def cp(q):
            xw[q] = zin[1, q]
        upto(np_out, cp)

    def spread(x, lo, hi, tile, ref):
        xs = split3(x)
        def some(i):
            for u in range(RING):
                j = lo + RING * i + u
                ok = (j < hi).astype(jnp.int32)
                at = ok * j + (1 - ok) * np_out
                xw[at] = xw[at] - stack_dot(xs, pieces(ref, ok * tile(j)), NN)
        upto(lax.div(hi - lo + RING - 1, RING), some)
    def fwd(q):
        y = stack_dot(split3(xw[q]), split3(inv_all[q]), NT)
        xw[q] = y
        spread(y, q + 1, npan, lambda j: ltile(j, q), lspt)
    upto(npan, fwd)
    def back(s):
        q = npan - 1 - s
        x = stack_dot(split3(xw[q]), split3(inv_all[q]), NN)
        xw[q] = x
        spread(x, 0, q, lambda j: ltile(q, j), lsp)
    upto(npan, back)

    xcopy = remote(pack.at[1], pack.at[0], *both_ends(psem, 2), partner())
    @pl.when(p == 1)
    def _():
        for z, part, par in every:
            last(par, part, z, 1).wait_recv()
        def zq(q):
            for par in HALVES:
                acc = jnp.zeros((MB, BW), F32)
                for i in range(n_in):
                    acc = acc + stack_dot(split3(xw[i // PAIR, :, (i % PAIR) * BW:(i % PAIR + 1) * BW]), split3(block(par, base_g + q * n_in + i)), NN)
                zin[0, q, :, par * BW:par * BW + BW] = acc
        upto(np_out, zq)
        zcopy.start()
        xcopy.wait_recv()
        zcopy.wait_send()
    @pl.when(p == 0)
    def _():
        for par in reversed(HALVES):
            pack[par, np_out * n_own:] = jnp.zeros((pack.shape[1] - np_out * n_own, PW), F32)
            for q in range(np_out):
                pack[par, q * n_own:(q + 1) * n_own] = xw[q, par * SUBL:par * SUBL + n_own]
            if par == 1:
                xcopy.start()
    n_t = fin.shape[4]
    for t in range(PAIR * (pack.shape[1] // SUBL)):
        part, z = divmod(t, n_t)
        half = t % PAIR
        fin[(part, *(along(part, ph) for ph in PARTS), z)] = pack[0, t // PAIR * SUBL:t // PAIR * SUBL + SUBL, half * BW:half * BW + BW]
    def fcopy(part, j):
        c1, e, f = (along(part, ph) for ph in PARTS)
        if j < 6:
            phase, step = 2 - j // 3, j % 3 + 1
            ref = fin.at[part, c1, e, f] if phase == 2 else fin.at[part, c1, e]
        else:
            z = j % PAIR
            phase, step = 0, UPDOWN[z]
            ref = fin.at[part, c1] if j < 8 else fin.at[part, turn(c1, 3 - PAIR * z), pl.ds(PAIR * z, 2)]
        s = part * 10 + j
        return remote(ref, ref, ssem.at[s], rsem.at[s], chip(part, phase, step))
    def fstep(came, js):
        def part_fn(part):
            for j in came:
                fcopy(part, j).wait_recv()
            for j in js:
                fcopy(part, j).start()
        for part in PARTS:
            part_fn(part)
    fstep((), (0, 1, 2))
    fstep((0, 1, 2), (3, 4, 5))
    fstep((3, 4, 5), (6, 7))
    def frelay(part):
        for z in HALVES:
            fcopy(part, 6 + z).wait_recv()
            fcopy(part, 8 + z).start()
    for part in PARTS:
        frelay(part)
    fstep((8, 9), ())
    for part in PARTS:
        for j in range(10):
            fcopy(part, j).wait_send()
    @pl.when(p == 1)
    def _():
        for z, part, par in every:
            last(par, part, z, 0).wait_send()
            last(par, part, z, 1).wait_send()
    @pl.when(p == 0)
    def _():
        xcopy.wait_send()

def solve(early, quarter, np_in, np_out, n_dp, damp, cuts):
    n_own = np_in * BW // n_dp
    n_row = -(-np_out * n_own // SUBL)
    n_t = -(-PAIR * n_row // 3)
    n_tile = np_out * (np_out - 1) // PAIR + 1
    V = lambda *s: pltpu.VMEM(s, F32)
    D = lambda *s: pltpu.SemaphoreType.DMA(s)
    hb = pl.BlockSpec(memory_space=pl.ANY)
    vb = pl.BlockSpec(memory_space=pltpu.VMEM)
    f32 = lambda *s: jax.ShapeDtypeStruct(s, F32)
    return pl.pallas_call(functools.partial(solve_kernel, np_in, np_out, n_dp, damp, cuts),
        out_shape=f32(3, RING, RING, RING, n_t, SUBL, BW), in_specs=[hb, vb], out_specs=vb,
        scratch_shapes=[V(2, cuts[-1], 3, RING, BW, BW), V(2, np_out + 1, PW, PW), V(BW, BW), V(BW, BW), V(np_out, PW, PW), *[pltpu.VMEM((3, n_tile, PW, PW), BF)] * 2, V(np_out + 1, MB, PW),
            V(2, np_out, MB, PW), V(2, n_row * SUBL, PW), D(54), D(54), D(2, 3), D(2, 2)],
        compiler_params=pltpu.CompilerParams(collective_id=1, has_side_effects=True, vmem_limit_bytes=67043328), name="solve")(early, quarter)

def finish_kernel(np_in, np_out, n_own, w_hbm, blocks, fin, w_out, a_out, s_out, wbuf, gath, cols_s, cols_a, up_s, up_a, isem, lsem, usem, wsem, csem):
    p = lax.axis_index('mp')
    wload = pltpu.make_async_copy(w_hbm, wbuf, isem)
    wload.start()
    sets = [(s_out, cols_s, up_s, np_out, 1), (a_out, cols_a, up_a, np_in, 0)]
    jobs, n = [], 0
    for out, cols, up, n_pan, of_s in sets:
        for q in range(n_pan):
            base = block_at(q, np_in, np_out, of_s) // PAIR
            low = pltpu.make_async_copy(blocks.at[p, pl.ds(base, n_pan - q)], cols.at[q, pl.ds(q, n_pan - q)], lsem.at[n])
            ups = [pltpu.make_async_copy(blocks.at[par, pl.ds(base + 1, n_pan - 1 - q), p], up.at[par, q, pl.ds(q + 1, n_pan - 1 - q)], usem.at[par, n]) for par in HALVES] if q < n_pan - 1 else []
            send = pltpu.make_async_copy(cols.at[q], out.at[q], csem.at[n])
            jobs.append((low, ups, send, cols, up, q))
            n += 1
    for low, ups, *_ in jobs:
        for c in (*ups, low):
            c.start()
    n_t = fin.shape[4]
    def tile(t, c):
        part, z = divmod(t, n_t)
        return fin[(part, *(c + c)[part:part + 3], z)]
    wload.wait()
    def weights(q):
        lo, hi = q * n_own // SUBL, ((q + 1) * n_own - 1) // SUBL
        for half in HALVES:
            def fill(z):
              for y in range(RING):
                vals = []
                for x in range(RING):
                    c = (x, y, z)
                    v = jnp.concatenate([tile(PAIR * r + half, c) for r in range(lo, hi + 1)], 0)
                    at = q * n_own - lo * SUBL
                    vals.append(v[at:at + n_own])
                gath[rows_at((z * RING + y) * RING * n_own, RING * n_own)] = jnp.concatenate(vals, 0)
            upto(RING, fill)
            for b in range(np_in):
                r = slice((PAIR * q + half) * BW, (PAIR * q + half + 1) * BW)
                wbuf[b, r] = wbuf[b, r] - LEARN_RATE * gath[b * BW:b * BW + BW].T
    for q in range(np_out // PAIR):
        weights(q)
    for low, ups, send, cols, up, q in jobs:
        low.wait()
        for c in ups:
            c.wait()
    for low, ups, send, cols, up, q in jobs:
        for q2 in range(q):
            for par in HALVES:
                cols[q, q2, par] = up[par, q2, q].T
        send.start()
    for q in range(np_out // PAIR, np_out):
        weights(q)
    wsend = pltpu.make_async_copy(wbuf, w_out, wsem)
    wsend.start()
    for low, ups, send, *_ in jobs:
        send.wait()
    wsend.wait()

def finish(w3, blocks, fin, np_in, np_out, n_dp):
    V = pltpu.VMEM
    D = pltpu.SemaphoreType.DMA
    hb = pl.BlockSpec(memory_space=pl.ANY)
    vb = pl.BlockSpec(memory_space=V)
    n_job = np_in + np_out
    square = lambda n: (n, n, 2, BW, BW)
    w_new, a_new, s_new = pl.pallas_call(functools.partial(finish_kernel, np_in, np_out, np_in * BW // n_dp),
        out_shape=(jax.ShapeDtypeStruct(w3.shape, F32), jax.ShapeDtypeStruct(square(np_in), F32), jax.ShapeDtypeStruct(square(np_out), F32)),
        in_specs=[hb, hb, vb], out_specs=(hb, hb, hb),
        scratch_shapes=[V(w3.shape, F32), V((np_in * BW, BW), F32), V(square(np_out), F32), V(square(np_in), F32), V((2, np_out, np_out, BW, BW), F32), V((2, np_in, np_in, BW, BW), F32),
            D, D((n_job,)), D((2, n_job)), D, D((n_job,))],
        compiler_params=pltpu.CompilerParams(vmem_limit_bytes=63 * 2**20), name="outputs")(w3, blocks.reshape(2, -1, 2, BW, BW), fin)
    return w_new, a_new.reshape(np_in, -1, BW), s_new.reshape(np_out, -1, BW)


def solution(mesh):
    n_dp = mesh.shape['dp']

    def local_step(a_loc, g_loc, w_loc, a_old_loc, s_old_loc):
        np_in = a_loc.shape[1] // PW
        np_out = g_loc.shape[1] // PW
        n_in, n_out = PAIR * np_in, PAIR * np_out
        early = np_in * (np_in + 1) + np_out * (np_out + 1)
        cuts = (0, 2, -(-early // GROUP), (early + n_in * np_out) // GROUP)
        panels = lambda x: x.transpose(1, 0, 2)
        blocks, quarter = front(a_loc, g_loc, panels(a_old_loc), panels(s_old_loc), n_dp, cuts)
        fin = solve(blocks, quarter, np_in, np_out, n_dp, DAMP_SHIFT, cuts)
        return tuple(panels(x) for x in finish(panels(w_loc), blocks, fin, np_in, np_out, n_dp))

    spec_rows = P('dp', None)
    spec_cyc = P(None, 'mp', None)
    return jax.shard_map(local_step, mesh=mesh, in_specs=(spec_rows, spec_rows, spec_cyc, spec_cyc, spec_cyc), out_specs=(spec_cyc, spec_cyc, spec_cyc), check_vma=False)
```
